1024 devices in a mesh: gx: 4 (over x_lo), gy: 8 (over y), gz: 32 (over z, x_hi, core).
Axes of the slice: x: 8 (x_hi: 2, x_lo: 4; x = x_hi * 4 + x_lo), y: 8, z: 8, core: 2. Of those that a mesh axis runs over, the one named last changes fastest.
Arguments:
- velocity_rhs: float32 [3, 256, 128, 512], P(None, 'gz', 'gy', 'gx'), may hold values from -48 to 48
- pressure_rhs: float32 [128, 64, 256], P('gz', 'gy', 'gx'), may hold values from -6 to 6
- viscosity: float32 [256, 128, 512], P('gz', 'gy', 'gx'), may hold values from 0.6 to 1.4
- velocity_mass: float32 [256, 128, 512], P('gz', 'gy', 'gx'), may hold values from 0.5 to 4
- pressure_scale: float32 [128, 64, 256], P('gz', 'gy', 'gx'), may hold values from 0.6 to 1.5
- velocity_bounds: float32 [2], replicated, may hold values from 4 to 72, as said below
- pressure_bounds: float32 [2], replicated, may hold values from 0.08 to 2.8, as said below
Outputs:
- velocity: float32 [3, 256, 128, 512], P(None, 'gz', 'gy', 'gx')
- pressure: float32 [128, 64, 256], P('gz', 'gy', 'gx')
The draws below stay inside these ranges and needn't reach their ends.
Inputs may be any that keep to these rules, and one draw needn't show every extreme that they name: velocity_bounds[0] is the lower bound and velocity_bounds[1] the upper one; the upper one exceeds the largest eigenvalue of A. pressure_bounds[0] is the lower bound and pressure_bounds[1] the upper one; the upper one exceeds the largest eigenvalue of M.
All inputs are finite; a program needn't handle non-finite values.
Results may differ from the reference program's by a relative error of at most 0.00002.
Values sent between devices are 32-bit elements; how exact they have to be, the bound alone decides.
No kernel may reach another device: no remote copies, remote signals or barrier semaphores. Data moves between devices by JAX's collectives and lax.ppermute only.
A program may use at most 32 MiB of HBM per device.

```python
import math
import jax
import jax.numpy as jnp
from jax import lax

SWEEPS = 2
PITERS = 2
NX = 512
NY = 128
NZ = 256
PX = 256
PY = 64
PZ = 128


def draw_velocity_bounds(key, part):
    values = jax.random.uniform(jax.random.fold_in(key, 11), (2,), jnp.float32)
    return jnp.stack([4.0 + 6.0 * values[0], 62.0 + 10.0 * values[1]]).astype(jnp.float32)


def draw_pressure_bounds(key, part):
    values = jax.random.uniform(jax.random.fold_in(key, 23), (2,), jnp.float32)
    return jnp.stack([0.08 + 0.22 * values[0], 2.4 + 0.4 * values[1]]).astype(jnp.float32)


def levels(key, shape, cuts, smallest, top_value):
    level, own = 1.0, jax.random.fold_in(key, 6)
    for axis_at, blocks in cuts:
        draws = jnp.exp(jax.random.uniform(jax.random.fold_in(own, axis_at), (blocks,), jnp.float32, smallest / len(cuts), top_value / len(cuts)))
        level = level * jnp.repeat(draws, shape[axis_at] // blocks).reshape([-1 if axis == axis_at else 1 for axis in range(len(shape))])
    return level


def centred(key, extent, scale, bound, split=(), kind=jnp.bfloat16):
    gain = levels(key, extent, split, -0.22, 0.18) if split else 1.0
    entries = jax.random.normal(key, extent, jnp.float32) * scale * gain
    return jnp.minimum(jnp.maximum(entries, -bound), bound).astype(kind)


def setup_inputs(seed: int = 0) -> dict:
    key_of = jax.random.split(jax.random.key(seed), 8)
    velocity_rhs = centred(key_of[0], (3, NZ, NY, NX), 8.0, 48.0, ((1, 32), (2, 8), (3, 4)), jnp.float32)
    pressure_rhs = centred(key_of[1], (PZ, PY, PX), 1.0, 6.0, ((0, 32), (1, 8), (2, 4)), jnp.float32)
    viscosity = jnp.clip(jnp.exp(math.log(1.4) - 0.8472978 * jax.random.uniform(key_of[2], (NZ, NY, NX), jnp.float32) ** levels(key_of[2], (NZ, NY, NX), ((0, 32), (1, 8), (2, 4)), -0.2, 0.2)), 0.6, 1.4)
    velocity_mass = jnp.clip(jnp.exp(math.log(4.0) - 2.0794415 * jax.random.uniform(key_of[3], (NZ, NY, NX), jnp.float32) ** levels(key_of[3], (NZ, NY, NX), ((0, 32), (1, 8), (2, 4)), -0.2, 0.2)), 0.5, 4.0)
    pressure_scale = jnp.clip(jnp.exp(math.log(1.5) - 0.9162907 * jax.random.uniform(key_of[4], (PZ, PY, PX), jnp.float32) ** levels(key_of[4], (PZ, PY, PX), ((0, 32), (1, 8), (2, 4)), -0.2, 0.2)), 0.6, 1.5)
    velocity_bounds = draw_velocity_bounds(jax.random.fold_in(key_of[7], 71), 0)
    pressure_bounds = draw_pressure_bounds(jax.random.fold_in(key_of[7], 71), 0)
    return {"velocity_rhs": velocity_rhs, "pressure_rhs": pressure_rhs, "viscosity": viscosity, "velocity_mass": velocity_mass, "pressure_scale": pressure_scale, "velocity_bounds": velocity_bounds, "pressure_bounds": pressure_bounds}


def pad_cells(field, width):
    return jnp.pad(field, [(0, 0)] * (field.ndim - 3) + [(width, width)] * 3)


def smooth_three(padded, outer_weight, centre):
    result = padded
    base = padded.ndim - 3
    for offset in range(3):
        dimension = base + offset
        length = result.shape[dimension] - 2
        result = (outer_weight * lax.slice_in_dim(result, 0, length, axis=dimension)
                  + centre * lax.slice_in_dim(result, 1, length + 1, axis=dimension)
                  + outer_weight * lax.slice_in_dim(result, 2, length + 2, axis=dimension))
    return result


def chebyshev(source, operator, bounds, count):
    low_end = bounds[0]
    high_end = bounds[1]
    centre_value = (high_end + low_end) / 2.0
    spread = (high_end - low_end) / 2.0
    sigma_ratio = centre_value / spread
    factor = 1.0 / sigma_ratio
    direction = source / centre_value
    iterate = direction
    residual = source
    for repeat in range(count):
        residual = residual - operator(direction)
        factor_next = 1.0 / (2.0 * sigma_ratio - factor)
        direction = factor_next * factor * direction + (2.0 * factor_next / spread) * residual
        iterate = iterate + direction
        factor = factor_next
    return iterate


def restrict_one(field, dimension):
    count = (field.shape[dimension] - 2) // 2
    return (0.25 * lax.slice_in_dim(field, 0, 2 * count, stride=2, axis=dimension)
            + 0.5 * lax.slice_in_dim(field, 1, 2 * count + 1, stride=2, axis=dimension)
            + 0.25 * lax.slice_in_dim(field, 2, 2 * count + 2, stride=2, axis=dimension))


def divergence_restricted(padded):
    along_x = 0.5 * (padded[0, 1:-1, 1:-1, 2:] - padded[0, 1:-1, 1:-1, :-2])
    along_y = 0.5 * (padded[1, 1:-1, 2:, 1:-1] - padded[1, 1:-1, :-2, 1:-1])
    along_z = 0.5 * (padded[2, 2:, 1:-1, 1:-1] - padded[2, :-2, 1:-1, 1:-1])
    diverge = along_x + along_y + along_z
    for dimension in range(3):
        diverge = restrict_one(diverge, dimension)
    return diverge


def reference(velocity_rhs, pressure_rhs, viscosity, velocity_mass, pressure_scale, velocity_bounds, pressure_bounds):
    def apply_velocity(direction):
        weighted = viscosity * direction
        laplace = 16.0 * weighted - 2.0 * smooth_three(pad_cells(weighted, 1), 0.5, 1.0)
        return viscosity * laplace + velocity_mass * direction

    def smooth_component(component):
        return chebyshev(component, apply_velocity, velocity_bounds, SWEEPS)

    velocity = lax.map(smooth_component, velocity_rhs)
    coupled = pressure_rhs - divergence_restricted(pad_cells(velocity, 2))

    def apply_pressure(direction):
        weighted = pressure_scale * direction
        return pressure_scale * smooth_three(pad_cells(weighted, 1), 1.0 / 6.0, 2.0 / 3.0)

    pressure = chebyshev(coupled, apply_pressure, pressure_bounds, PITERS)
    return velocity, pressure
```

```python
import jax
import jax.numpy as jnp
import ml_dtypes
import numpy as np
from jax import lax
from jax.experimental import pallas as pl
from jax.experimental.pallas import tpu as pltpu
from jax.sharding import PartitionSpec as P

Z, Y, X = 8, 16, 128
PZ, PY, PX = 4, 8, 64
F32 = jnp.float32

ZW = Z + 4
PLANES = 4 * ZW + Z + 2
S0, M0 = 3 * ZW, 4 * ZW
VT = 4 * PLANES
TILES = VT + 24
PACKED = TILES // 16


def parity(axis):
    return lax.rem(lax.axis_index(axis), 2)


def swap_neighbours(axis, first, second):
    size = lax.axis_size(axis)
    even = [(i, i ^ 1) for i in range(size)]
    odd = [(i, ((i + 1) ^ 1) - 1) for i in range(1, size - 1)]
    return lax.ppermute(first, axis, even), lax.ppermute(second, axis, odd)


def both_neighbours(axis, to_above, to_below):
    size = lax.axis_size(axis)
    up = [(i, i + 1) for i in range(size - 1)]
    down = [(i + 1, i) for i in range(size - 1)]
    return lax.ppermute(to_above, axis, up), lax.ppermute(to_below, axis, down)


def call(body, outs, scratch=(), smem=()):
    def run(*args):
        specs = [
            pl.BlockSpec(memory_space=pltpu.SMEM if i in smem else pltpu.VMEM)
            for i in range(len(args))
        ]
        return pl.pallas_call(
            body,
            in_specs=specs,
            out_specs=[pl.BlockSpec(memory_space=pltpu.VMEM) for _ in outs],
            out_shape=[jax.ShapeDtypeStruct(o, F32) for o in outs],
            scratch_shapes=list(scratch),
            name=body.__name__,
        )(*args)

    return run


def pack_z(rhs, visc, mass, msg_even, msg_odd):
    par = parity("gz")
    for out, up in ((msg_even, 1 - par), (msg_odd, par)):
        z0 = 6 * up
        for c in range(3):
            for j in range(2):
                out[2 * c + j] = rhs[c, z0 + j]
        for j in range(2):
            out[6 + j] = visc[z0 + j]
        out[8] = mass[7 * up]


def pack_y(rhs, visc, mass, got_even, got_odd, pscale, prhs, own, up, down, pt):
    even = parity("gz") == 0

    def put(plane, value):
        own[plane] = value
        down[plane] = value[:8]
        up[plane] = value[8:]

    def halo(i):
        a, b = got_even[i], got_odd[i]
        return jnp.where(even, b, a), jnp.where(even, a, b)

    for c in range(3):
        for j in range(2):
            below, above = halo(2 * c + j)
            put(c * ZW + j, below)
            put(c * ZW + 10 + j, above)
        for z in range(Z):
            put(c * ZW + 2 + z, rhs[c, z])
    for j in range(2):
        below, above = halo(6 + j)
        put(S0 + j, below)
        put(S0 + 10 + j, above)
    below, above = halo(8)
    put(M0, below)
    put(M0 + 9, above)
    for z in range(Z):
        put(S0 + 2 + z, visc[z])
        put(M0 + 1 + z, mass[z])
    for k in range(PZ):
        tile = jnp.concatenate([pscale[k], prhs[k]], axis=1)
        pt[k] = tile
        up[PLANES + k] = tile
        down[PLANES + k] = tile


def lanes():
    return lax.broadcasted_iota(jnp.int32, (8, X), 1)


def pack_x(own, below, above, pt, main, up, down):
    lane = lanes()
    for p in range(PLANES):
        main[4 * p] = below[p]
        main[4 * p + 1] = own[p, :8]
        main[4 * p + 2] = own[p, 8:]
        main[4 * p + 3] = above[p]
    for k in range(PZ):
        for t, src in enumerate((below[PLANES + k], pt[k], above[PLANES + k])):
            turned = pltpu.roll(src, 64, axis=1)
            main[VT + 3 * k + t] = jnp.where(lane < 64, src, turned)
            main[VT + 12 + 3 * k + t] = jnp.where(lane < 64, turned, src)
    low = (lane & 15) < 8

    def group(j):
        acc = pltpu.roll(main[8 * j], 8, axis=1)
        for k in range(1, 8):
            acc = jnp.where(lane >= 16 * k, pltpu.roll(main[8 * j + k], (8 + 16 * k) % X, axis=1), acc)
        return acc

    for i in range(PACKED):
        a, b = group(2 * i), group(2 * i + 1)
        up[i] = jnp.where(low, a, pltpu.roll(b, 8, axis=1))
        down[i] = jnp.where(low, pltpu.roll(a, 120, axis=1), b)


def coefficients(bounds):
    low = jnp.full((8, X), bounds[0], F32)
    high = jnp.full((8, X), bounds[1], F32)
    centre = (high + low) / 2.0
    spread = (high - low) / 2.0
    sigma = centre / spread
    rho0 = 1.0 / sigma
    rho1 = 1.0 / (2.0 * sigma - rho0)
    rho2 = 1.0 / (2.0 * sigma - rho1)
    return 1.0 / centre, rho1 * rho0, 2.0 * rho1 / spread, rho2 * rho1, 2.0 * rho2 / spread


def tall(coef, rows):
    return jnp.concatenate([coef] * (rows // 8), axis=0)


def restriction():
    table = np.zeros((4, X, X), np.float32)
    for half in range(2):
        for l in range(X):
            x = l if half == 0 else (X + l if l < 8 else l - X)
            if half and 8 <= l < 120:
                continue
            for node in range(-2, PX + 2):
                o = x - 2 * node
                table[half, l, node + 2] = {-1: 0.25, 0: 0.5, 1: 0.25}.get(o, 0.0)
                table[2 + half, l, node + 2] = {-2: -0.125, -1: -0.25, 1: 0.25, 2: 0.125}.get(o, 0.0)
    return table.reshape(4 * X, X).astype(ml_dtypes.bfloat16)


SMOOTH_Z = {-1: (), 0: ((0, 0.5), (1, 0.25)), 4: ((7, 0.25),)}
DERIVE_Z = {
    -1: ((0, 0.125),),
    0: ((1, 0.25), (2, 0.125)),
    1: ((0, -0.125), (1, -0.25), (3, 0.25), (4, 0.125)),
    2: ((2, -0.125), (3, -0.25), (5, 0.25), (6, 0.125)),
    3: ((4, -0.125), (5, -0.25), (7, 0.25)),
    4: ((6, -0.125), (7, -0.25)),
}
for _k in (1, 2, 3):
    SMOOTH_Z[_k] = ((2 * _k - 1, 0.25), (2 * _k, 0.5), (2 * _k + 1, 0.25))


def velocity_step(
    main, from_below, from_above, table, bounds, vel, coupled, pscale, msg_even, msg_odd,
    halo, w, d, r, u, t, g, q, ptmp,
):
    lane = lanes()
    low = (lane & 15) < 8
    edge = (lane < 8) | (lane >= 120)
    for i in range(PACKED):
        a, b = from_below[i], from_above[i]
        pair = (
            jnp.where(low, a, pltpu.roll(b, 8, axis=1)),
            jnp.where(low, pltpu.roll(a, 120, axis=1), b),
        )
        for e in range(2):
            for k in range(8):
                halo[16 * i + 8 * e + k] = jnp.where(
                    edge, pltpu.roll(pair[e], (120 - 16 * k) % X, axis=1), 0.0
                )

    inv, a1, g1, a2, g2 = (tall(v, 32) for v in coefficients(bounds))
    lane32 = lax.broadcasted_iota(jnp.int32, (32, X), 1)
    first, last = lane32 == 0, lane32 == X - 1
    t[...] = jnp.zeros_like(t)

    def planes(ref, p):
        return ref[pl.ds(4 * p, 4)].reshape(32, X)

    def smooth(src, z):
        out = []
        for h in range(2):
            v = src[h, z] + 0.5 * (src[h, z - 1] + src[h, z + 1])
            t[h, 8:40] = v
            out.append(v + 0.5 * (t[h, 7:39] + t[h, 9:41]))
        m, s = out
        ml, sl = pltpu.roll(m, 1, axis=1), pltpu.roll(s, 1, axis=1)
        mr, sr = pltpu.roll(m, X - 1, axis=1), pltpu.roll(s, X - 1, axis=1)
        return (
            m + 0.5 * (jnp.where(first, sl, ml) + jnp.where(last, sr, mr)),
            s + 0.5 * (jnp.where(first, ml, sl) + jnp.where(last, mr, sr)),
        )

    def component(c, _):
        base = c * ZW

        def weight(z, _):
            for h, src in enumerate((main, halo)):
                w[0, h, z] = planes(src, S0 + z) * (planes(src, base + z) * inv)
            return 0

        lax.fori_loop(0, ZW, weight, 0)

        def sweep1(z, _):
            s = smooth(w.at[0], z)
            for h, src in enumerate((main, halo)):
                b = planes(src, base + z)
                visc = planes(src, S0 + z)
                d0 = b * inv
                res = b - (visc * (16.0 * w[0, h, z] - 2.0 * s[h]) + planes(src, M0 + z - 1) * d0)
                d1 = a1 * d0 + g1 * res
                r[h, z] = res
                d[h, z] = d1
                w[1, h, z] = visc * d1
            return 0

        lax.fori_loop(1, ZW - 1, sweep1, 0)

        def sweep2(z, _):
            s = smooth(w.at[1], z)
            for h, src in enumerate((main, halo)):
                d1 = d[h, z]
                res = r[h, z] - (
                    planes(src, S0 + z) * (16.0 * w[1, h, z] - 2.0 * s[h]) + planes(src, M0 + z - 1) * d1
                )
                total = planes(src, base + z) * inv + d1 + (a2 * d1 + g2 * res)
                u[c, h, z - 2] = total
                if h == 0:
                    vel[c, z - 2] = total[8:24]
            return 0

        lax.fori_loop(2, ZW - 2, sweep2, 0)
        return 0

    lax.fori_loop(0, 3, component, 0)

    q[...] = jnp.zeros_like(q)
    for node in range(-1, 5):
        rows = slice(16 * (node + 1), 16 * (node + 1) + 12)

        def along_z(c, h, weights):
            acc = None
            for z, f in weights:
                term = f * u[c, h, z]
                acc = term if acc is None else acc + term
            return acc

        def at(k, start):
            return g[k, pl.ds(start, 12, stride=2), :]

        for h in range(2):
            cols = slice(X * h, X * (h + 1))
            g[2] = along_z(2, h, DERIVE_Z[node])
            total = 0.25 * (at(2, 3) + at(2, 5)) + 0.5 * at(2, 4)
            if SMOOTH_Z[node]:
                g[0] = along_z(0, h, SMOOTH_Z[node])
                g[1] = along_z(1, h, SMOOTH_Z[node])
                total = total + 0.25 * (at(1, 5) - at(1, 3)) + 0.125 * (at(1, 6) - at(1, 2))
                q[rows, 2 * X + X * h : 3 * X + X * h] = 0.25 * (at(0, 3) + at(0, 5)) + 0.5 * at(0, 4)
            q[rows, cols] = total

    full = q[...]
    hi = full.astype(jnp.bfloat16)
    rest = full - hi.astype(F32)
    mid = rest.astype(jnp.bfloat16)
    lo = (rest - mid.astype(F32)).astype(jnp.bfloat16)
    weights = table[...]
    div = sum(
        lax.dot_general(v, weights, (((1,), (0,)), ((), ())), preferred_element_type=F32)
        for v in (lo, mid, hi)
    )

    def nodes(base, k):
        for i in range(3):
            own = pltpu.roll(main[base + 3 * k + i], 2, axis=1)
            side = halo[base + 3 * k + i]
            left = pltpu.roll(side, 2, axis=1)
            right = pltpu.roll(side, 66, axis=1)
            value = jnp.where(lane < 66, own, jnp.where(lane < 68, right, 0.0))
            ptmp[8 * i : 8 * i + 8] = jnp.where(lane < 2, left, value)
        return ptmp[6:18]

    coupled[...] = -div.reshape(6, 16, X)
    pscale[...] = jnp.zeros_like(pscale)
    for k in range(PZ):
        pscale[k, :12] = nodes(VT, k)
        coupled[k + 1, :12] = nodes(VT + 12, k) - div[16 * (k + 1) : 16 * (k + 1) + 12]
    par = parity("gz")
    for out, up in ((msg_even, 1 - par), (msg_odd, par)):
        for j in range(3):
            out[j] = coupled[3 * up + j]
        for j in range(2):
            out[3 + j] = pscale[2 * up + j]


def pressure_step(coupled, pscale, got_even, got_odd, bounds, out):
    even = parity("gz") == 0
    below, above = [], []
    for i in range(5):
        a, b = got_even[i], got_odd[i]
        below.append(jnp.where(even, b, a))
        above.append(jnp.where(even, a, b))
    b = [
        below[0], below[1] + coupled[0], below[2] + coupled[1], coupled[2], coupled[3],
        coupled[4] + above[0], coupled[5] + above[1], above[2],
    ]
    s = [below[3], below[4], pscale[0], pscale[1], pscale[2], pscale[3], above[3], above[4]]
    inv, a1, g1, a2, g2 = (tall(v, 16) for v in coefficients(bounds))

    def operator(w, z):
        v = (1.0 / 6.0) * (w[z - 1] + w[z + 1]) + (2.0 / 3.0) * w[z]
        v = (1.0 / 6.0) * (pltpu.roll(v, 1, axis=0) + pltpu.roll(v, 15, axis=0)) + (2.0 / 3.0) * v
        v = (1.0 / 6.0) * (pltpu.roll(v, 1, axis=1) + pltpu.roll(v, X - 1, axis=1)) + (2.0 / 3.0) * v
        return s[z] * v

    d0 = [v * inv for v in b]
    w = [x * y for x, y in zip(s, d0)]
    r1, d1, w1 = [None] * 8, [None] * 8, [None] * 8
    for z in range(1, 7):
        r1[z] = b[z] - operator(w, z)
        d1[z] = a1 * d0[z] + g1 * r1[z]
        w1[z] = s[z] * d1[z]
    for z in range(2, 6):
        res = r1[z] - operator(w1, z)
        total = d0[z] + d1[z] + (a2 * d1[z] + g2 * res)
        total = pltpu.roll(pltpu.roll(total, 14, axis=0), X - 2, axis=1)
        out[z - 2] = total[:PY, :PX]


def per_device(rhs, prhs, visc, mass, pscale, vbounds, pbounds):
    plane = (Y, X)
    msg_even, msg_odd = call(pack_z, [(9, *plane)] * 2)(rhs, visc, mass)
    got_even, got_odd = swap_neighbours("gz", msg_even, msg_odd)
    own, up, down, pt = call(
        pack_y, [(PLANES, *plane), (PLANES + PZ, 8, X), (PLANES + PZ, 8, X), (PZ, 8, X)]
    )(rhs, visc, mass, got_even, got_odd, pscale, prhs)
    below, above = both_neighbours("gy", up, down)
    main, up, down = call(pack_x, [(TILES, 8, X), (PACKED, 8, X), (PACKED, 8, X)])(
        own, below, above, pt
    )
    below, above = both_neighbours("gx", up, down)
    vel, coupled, scale, msg_even, msg_odd = call(
        velocity_step,
        [(3, Z, Y, X), (6, *plane), (PZ, *plane), (5, *plane), (5, *plane)],
        scratch=[
            pltpu.VMEM((TILES, 8, X), F32),
            pltpu.VMEM((2, 2, ZW, 32, X), F32),
            pltpu.VMEM((2, ZW, 32, X), F32),
            pltpu.VMEM((2, ZW, 32, X), F32),
            pltpu.VMEM((3, 2, Z, 32, X), F32),
            pltpu.VMEM((2, 48, X), F32),
            pltpu.VMEM((3, 32, X), F32),
            pltpu.VMEM((96, 4 * X), F32),
            pltpu.VMEM((24, X), F32),
        ],
        smem=(4,),
    )(main, below, above, jnp.asarray(restriction()), vbounds)
    got_even, got_odd = swap_neighbours("gz", msg_even, msg_odd)
    (pressure,) = call(pressure_step, [(PZ, PY, PX)], smem=(4,))(
        coupled, scale, got_even, got_odd, pbounds
    )
    return vel, pressure


def solution(mesh):
    block = P("gz", "gy", "gx")
    field = P(None, "gz", "gy", "gx")
    return jax.shard_map(
        per_device,
        mesh=mesh,
        in_specs=(field, block, block, block, block, P(), P()),
        out_specs=(field, block),
        check_vma=False,
    )
```

```python
import jax
import jax.numpy as jnp
import ml_dtypes
import numpy as np
from jax import lax
from jax.experimental import pallas as pl
from jax.experimental.pallas import tpu as pltpu
from jax.sharding import PartitionSpec as P

Z, Y, X = 8, 16, 128
PZ, PY, PX = 4, 8, 64
F32 = jnp.float32
VMEM_LIMIT = 16 * 2**20

ZW = Z + 4
PLANES = 4 * ZW + Z + 2
S0, M0 = 3 * ZW, 4 * ZW
VT = 4 * PLANES
TILES = VT + 24
PACKED = TILES // 16


def parity(axis):
    return lax.rem(lax.axis_index(axis), 2)


def swap_neighbours(axis, first, second):
    size = lax.axis_size(axis)
    even = [(i, i ^ 1) for i in range(size)]
    odd = [(i, ((i + 1) ^ 1) - 1) for i in range(1, size - 1)]
    return lax.ppermute(first, axis, even), lax.ppermute(second, axis, odd)


def both_neighbours(axis, to_above, to_below):
    size = lax.axis_size(axis)
    up = [(i, i + 1) for i in range(size - 1)]
    down = [(i + 1, i) for i in range(size - 1)]
    return lax.ppermute(to_above, axis, up), lax.ppermute(to_below, axis, down)


def call(body, outs, scratch=(), smem=()):
    def run(*args):
        specs = [
            pl.BlockSpec(memory_space=pltpu.SMEM if i in smem else pltpu.VMEM)
            for i in range(len(args))
        ]
        return pl.pallas_call(
            body,
            in_specs=specs,
            out_specs=[pl.BlockSpec(memory_space=pltpu.VMEM) for _ in outs],
            out_shape=[jax.ShapeDtypeStruct(o, F32) for o in outs],
            scratch_shapes=list(scratch),
            name=body.__name__,
            compiler_params=pltpu.CompilerParams(vmem_limit_bytes=VMEM_LIMIT),
        )(*args)

    return run


def pack_z(rhs, visc, mass, msg_even, msg_odd):
    par = parity("gz")
    for out, up in ((msg_even, 1 - par), (msg_odd, par)):
        z0 = 6 * up
        for c in range(3):
            for j in range(2):
                out[2 * c + j] = rhs[c, z0 + j]
        for j in range(2):
            out[6 + j] = visc[z0 + j]
        out[8] = mass[7 * up]


def pack_y(rhs, visc, mass, got_even, got_odd, pscale, prhs, own, up, down, pt):
    even = parity("gz") == 0

    def put(plane, value):
        own[plane] = value
        down[plane] = value[:8]
        up[plane] = value[8:]

    def halo(i):
        a, b = got_even[i], got_odd[i]
        return jnp.where(even, b, a), jnp.where(even, a, b)

    for c in range(3):
        for j in range(2):
            below, above = halo(2 * c + j)
            put(c * ZW + j, below)
            put(c * ZW + 10 + j, above)
        for z in range(Z):
            put(c * ZW + 2 + z, rhs[c, z])
    for j in range(2):
        below, above = halo(6 + j)
        put(S0 + j, below)
        put(S0 + 10 + j, above)
    below, above = halo(8)
    put(M0, below)
    put(M0 + 9, above)
    for z in range(Z):
        put(S0 + 2 + z, visc[z])
        put(M0 + 1 + z, mass[z])
    for k in range(PZ):
        tile = jnp.concatenate([pscale[k], prhs[k]], axis=1)
        pt[k] = tile
        up[PLANES + k] = tile
        down[PLANES + k] = tile


def lanes():
    return lax.broadcasted_iota(jnp.int32, (8, X), 1)


def pack_x(own, below, above, pt, main, up, down):
    lane = lanes()
    for p in range(PLANES):
        main[4 * p] = below[p]
        main[4 * p + 1] = own[p, :8]
        main[4 * p + 2] = own[p, 8:]
        main[4 * p + 3] = above[p]
    for k in range(PZ):
        for t, src in enumerate((below[PLANES + k], pt[k], above[PLANES + k])):
            turned = pltpu.roll(src, 64, axis=1)
            main[VT + 3 * k + t] = jnp.where(lane < 64, src, turned)
            main[VT + 12 + 3 * k + t] = jnp.where(lane < 64, turned, src)
    low = (lane & 15) < 8

    def group(j):
        acc = pltpu.roll(main[8 * j], 8, axis=1)
        for k in range(1, 8):
            acc = jnp.where(lane >= 16 * k, pltpu.roll(main[8 * j + k], (8 + 16 * k) % X, axis=1), acc)
        return acc

    for i in range(PACKED):
        a, b = group(2 * i), group(2 * i + 1)
        up[i] = jnp.where(low, a, pltpu.roll(b, 8, axis=1))
        down[i] = jnp.where(low, pltpu.roll(a, 120, axis=1), b)


def coefficients(bounds):
    low = jnp.full((8, X), bounds[0], F32)
    high = jnp.full((8, X), bounds[1], F32)
    centre = (high + low) / 2.0
    spread = (high - low) / 2.0
    sigma = centre / spread
    rho0 = 1.0 / sigma
    rho1 = 1.0 / (2.0 * sigma - rho0)
    rho2 = 1.0 / (2.0 * sigma - rho1)
    return 1.0 / centre, rho1 * rho0, 2.0 * rho1 / spread, rho2 * rho1, 2.0 * rho2 / spread


def tall(coef, rows):
    return jnp.concatenate([coef] * (rows // 8), axis=0)


def restriction():
    table = np.zeros((4, X, X), np.float32)
    for half in range(2):
        for l in range(X):
            x = l if half == 0 else (X + l if l < 8 else l - X)
            if half and 8 <= l < 120:
                continue
            for node in range(-2, PX + 2):
                o = x - 2 * node
                table[half, l, node + 2] = {-1: 0.25, 0: 0.5, 1: 0.25}.get(o, 0.0)
                table[2 + half, l, node + 2] = {-2: -0.125, -1: -0.25, 1: 0.25, 2: 0.125}.get(o, 0.0)
    return table.reshape(4 * X, X).astype(ml_dtypes.bfloat16)


SMOOTH_Z = {-1: (), 0: ((0, 0.5), (1, 0.25)), 4: ((7, 0.25),)}
DERIVE_Z = {
    -1: ((0, 0.125),),
    0: ((1, 0.25), (2, 0.125)),
    1: ((0, -0.125), (1, -0.25), (3, 0.25), (4, 0.125)),
    2: ((2, -0.125), (3, -0.25), (5, 0.25), (6, 0.125)),
    3: ((4, -0.125), (5, -0.25), (7, 0.25)),
    4: ((6, -0.125), (7, -0.25)),
}
for _k in (1, 2, 3):
    SMOOTH_Z[_k] = ((2 * _k - 1, 0.25), (2 * _k, 0.5), (2 * _k + 1, 0.25))


def velocity_step(
    main, from_below, from_above, table, bounds, vel, coupled, pscale, msg_even, msg_odd,
    halo, w, d, r, u, t, g, q, ptmp,
):
    lane = lanes()
    low = (lane & 15) < 8
    edge = (lane < 8) | (lane >= 120)
    for i in range(PACKED):
        a, b = from_below[i], from_above[i]
        pair = (
            jnp.where(low, a, pltpu.roll(b, 8, axis=1)),
            jnp.where(low, pltpu.roll(a, 120, axis=1), b),
        )
        for e in range(2):
            for k in range(8):
                halo[16 * i + 8 * e + k] = jnp.where(
                    edge, pltpu.roll(pair[e], (120 - 16 * k) % X, axis=1), 0.0
                )

    inv, a1, g1, a2, g2 = (tall(v, 32) for v in coefficients(bounds))
    lane32 = lax.broadcasted_iota(jnp.int32, (32, X), 1)
    first, last = lane32 == 0, lane32 == X - 1
    t[...] = jnp.zeros_like(t)

    def planes(ref, p):
        return ref[pl.ds(4 * p, 4)].reshape(32, X)

    def smooth(src, z):
        out = []
        for h in range(2):
            v = src[h, z] + 0.5 * (src[h, z - 1] + src[h, z + 1])
            t[h, 8:40] = v
            out.append(v + 0.5 * (t[h, 7:39] + t[h, 9:41]))
        m, s = out
        ml, sl = pltpu.roll(m, 1, axis=1), pltpu.roll(s, 1, axis=1)
        mr, sr = pltpu.roll(m, X - 1, axis=1), pltpu.roll(s, X - 1, axis=1)
        return (
            m + 0.5 * (jnp.where(first, sl, ml) + jnp.where(last, sr, mr)),
            s + 0.5 * (jnp.where(first, ml, sl) + jnp.where(last, mr, sr)),
        )

    def component(c, _):
        base = c * ZW

        def weight(z, _):
            for h, src in enumerate((main, halo)):
                w[0, h, z] = planes(src, S0 + z) * (planes(src, base + z) * inv)
            return 0

        lax.fori_loop(0, ZW, weight, 0)

        def sweep1(z, _):
            s = smooth(w.at[0], z)
            for h, src in enumerate((main, halo)):
                b = planes(src, base + z)
                visc = planes(src, S0 + z)
                d0 = b * inv
                res = b - (visc * (16.0 * w[0, h, z] - 2.0 * s[h]) + planes(src, M0 + z - 1) * d0)
                d1 = a1 * d0 + g1 * res
                r[h, z] = res
                d[h, z] = d1
                w[1, h, z] = visc * d1
            return 0

        lax.fori_loop(1, ZW - 1, sweep1, 0)

        def sweep2(z, _):
            s = smooth(w.at[1], z)
            for h, src in enumerate((main, halo)):
                d1 = d[h, z]
                res = r[h, z] - (
                    planes(src, S0 + z) * (16.0 * w[1, h, z] - 2.0 * s[h]) + planes(src, M0 + z - 1) * d1
                )
                total = planes(src, base + z) * inv + d1 + (a2 * d1 + g2 * res)
                u[c, h, z - 2] = total
                if h == 0:
                    vel[c, z - 2] = total[8:24]
            return 0

        lax.fori_loop(2, ZW - 2, sweep2, 0)
        return 0

    lax.fori_loop(0, 3, component, 0)

    q[...] = jnp.zeros_like(q)
    for node in range(-1, 5):
        rows = slice(16 * (node + 1), 16 * (node + 1) + 12)

        def along_z(c, h, weights):
            acc = None
            for z, f in weights:
                term = f * u[c, h, z]
                acc = term if acc is None else acc + term
            return acc

        def at(k, start):
            return g[k, pl.ds(start, 12, stride=2), :]

        for h in range(2):
            cols = slice(X * h, X * (h + 1))
            g[2] = along_z(2, h, DERIVE_Z[node])
            total = 0.25 * (at(2, 3) + at(2, 5)) + 0.5 * at(2, 4)
            if SMOOTH_Z[node]:
                g[0] = along_z(0, h, SMOOTH_Z[node])
                g[1] = along_z(1, h, SMOOTH_Z[node])
                total = total + 0.25 * (at(1, 5) - at(1, 3)) + 0.125 * (at(1, 6) - at(1, 2))
                q[rows, 2 * X + X * h : 3 * X + X * h] = 0.25 * (at(0, 3) + at(0, 5)) + 0.5 * at(0, 4)
            q[rows, cols] = total

    full = q[...]
    hi = full.astype(jnp.bfloat16)
    rest = full - hi.astype(F32)
    mid = rest.astype(jnp.bfloat16)
    lo = (rest - mid.astype(F32)).astype(jnp.bfloat16)
    weights = table[...]
    div = sum(
        lax.dot_general(v, weights, (((1,), (0,)), ((), ())), preferred_element_type=F32)
        for v in (lo, mid, hi)
    )

    def nodes(base, k):
        for i in range(3):
            own = pltpu.roll(main[base + 3 * k + i], 2, axis=1)
            side = halo[base + 3 * k + i]
            left = pltpu.roll(side, 2, axis=1)
            right = pltpu.roll(side, 66, axis=1)
            value = jnp.where(lane < 66, own, jnp.where(lane < 68, right, 0.0))
            ptmp[8 * i : 8 * i + 8] = jnp.where(lane < 2, left, value)
        return ptmp[6:18]

    coupled[...] = -div.reshape(6, 16, X)
    pscale[...] = jnp.zeros_like(pscale)
    for k in range(PZ):
        pscale[k, :12] = nodes(VT, k)
        coupled[k + 1, :12] = nodes(VT + 12, k) - div[16 * (k + 1) : 16 * (k + 1) + 12]
    par = parity("gz")
    for out, up in ((msg_even, 1 - par), (msg_odd, par)):
        for j in range(3):
            out[j] = coupled[3 * up + j]
        for j in range(2):
            out[3 + j] = pscale[2 * up + j]


def pressure_step(coupled, pscale, got_even, got_odd, bounds, out):
    even = parity("gz") == 0
    below, above = [], []
    for i in range(5):
        a, b = got_even[i], got_odd[i]
        below.append(jnp.where(even, b, a))
        above.append(jnp.where(even, a, b))
    b = [
        below[0], below[1] + coupled[0], below[2] + coupled[1], coupled[2], coupled[3],
        coupled[4] + above[0], coupled[5] + above[1], above[2],
    ]
    s = [below[3], below[4], pscale[0], pscale[1], pscale[2], pscale[3], above[3], above[4]]
    inv, a1, g1, a2, g2 = (tall(v, 16) for v in coefficients(bounds))

    def operator(w, z):
        v = (1.0 / 6.0) * (w[z - 1] + w[z + 1]) + (2.0 / 3.0) * w[z]
        v = (1.0 / 6.0) * (pltpu.roll(v, 1, axis=0) + pltpu.roll(v, 15, axis=0)) + (2.0 / 3.0) * v
        v = (1.0 / 6.0) * (pltpu.roll(v, 1, axis=1) + pltpu.roll(v, X - 1, axis=1)) + (2.0 / 3.0) * v
        return s[z] * v

    d0 = [v * inv for v in b]
    w = [x * y for x, y in zip(s, d0)]
    r1, d1, w1 = [None] * 8, [None] * 8, [None] * 8
    for z in range(1, 7):
        r1[z] = b[z] - operator(w, z)
        d1[z] = a1 * d0[z] + g1 * r1[z]
        w1[z] = s[z] * d1[z]
    for z in range(2, 6):
        res = r1[z] - operator(w1, z)
        total = d0[z] + d1[z] + (a2 * d1[z] + g2 * res)
        total = pltpu.roll(pltpu.roll(total, 14, axis=0), X - 2, axis=1)
        out[z - 2] = total[:PY, :PX]


def per_device(rhs, prhs, visc, mass, pscale, vbounds, pbounds):
    plane = (Y, X)
    msg_even, msg_odd = call(pack_z, [(9, *plane)] * 2)(rhs, visc, mass)
    got_even, got_odd = swap_neighbours("gz", msg_even, msg_odd)
    own, up, down, pt = call(
        pack_y, [(PLANES, *plane), (PLANES + PZ, 8, X), (PLANES + PZ, 8, X), (PZ, 8, X)]
    )(rhs, visc, mass, got_even, got_odd, pscale, prhs)
    below, above = both_neighbours("gy", up, down)
    main, up, down = call(pack_x, [(TILES, 8, X), (PACKED, 8, X), (PACKED, 8, X)])(
        own, below, above, pt
    )
    below, above = both_neighbours("gx", up, down)
    vel, coupled, scale, msg_even, msg_odd = call(
        velocity_step,
        [(3, Z, Y, X), (6, *plane), (PZ, *plane), (5, *plane), (5, *plane)],
        scratch=[
            pltpu.VMEM((TILES, 8, X), F32),
            pltpu.VMEM((2, 2, ZW, 32, X), F32),
            pltpu.VMEM((2, ZW, 32, X), F32),
            pltpu.VMEM((2, ZW, 32, X), F32),
            pltpu.VMEM((3, 2, Z, 32, X), F32),
            pltpu.VMEM((2, 48, X), F32),
            pltpu.VMEM((3, 32, X), F32),
            pltpu.VMEM((96, 4 * X), F32),
            pltpu.VMEM((24, X), F32),
        ],
        smem=(4,),
    )(main, below, above, jnp.asarray(restriction()), vbounds)
    got_even, got_odd = swap_neighbours("gz", msg_even, msg_odd)
    (pressure,) = call(pressure_step, [(PZ, PY, PX)], smem=(4,))(
        coupled, scale, got_even, got_odd, pbounds
    )
    return vel, pressure


def solution(mesh):
    block = P("gz", "gy", "gx")
    field = P(None, "gz", "gy", "gx")
    return jax.shard_map(
        per_device,
        mesh=mesh,
        in_specs=(field, block, block, block, block, P(), P()),
        out_specs=(field, block),
        check_vma=False,
    )
```

```python
import jax
import jax.numpy as jnp
import ml_dtypes
import numpy as np
from jax import lax
from jax.experimental import pallas as pl
from jax.experimental.pallas import tpu as pltpu
from jax.sharding import PartitionSpec as P


Z, Y, X = 8, 16, 128
PZ, PY, PX = 4, 8, 64
F32 = jnp.float32
VMEM_LIMIT = 16 * 2**20

ZW = Z + 4
PLANES = 4 * ZW + Z + 2
S0, M0 = 3 * ZW, 4 * ZW
VT = 4 * PLANES
TILES = VT + 24
PACKED = TILES // 16


def parity(axis):
    return lax.rem(lax.axis_index(axis), 2)


def swap_neighbours(axis, first, second):
    size = lax.axis_size(axis)
    even = [(i, i ^ 1) for i in range(size)]
    odd = [(i, ((i + 1) ^ 1) - 1) for i in range(1, size - 1)]
    inner = lax.ppermute(first, axis, even)
    outer = lax.ppermute(second, axis, odd)
    return inner, outer


def both_neighbours(axis, to_above, to_below):
    size = lax.axis_size(axis)
    up = [(i, i + 1) for i in range(size - 1)]
    down = [(i + 1, i) for i in range(size - 1)]
    from_below = lax.ppermute(to_above, axis, up)
    from_above = lax.ppermute(to_below, axis, down)
    return from_below, from_above


def call(body, outs, scratch=(), smem=(), hbm=()):
    def run(*args):
        space = {i: pltpu.SMEM for i in smem} | {i: pltpu.HBM for i in hbm}
        args = [
            pltpu.with_memory_space_constraint(x, pltpu.HBM) if i in hbm else x
            for i, x in enumerate(args)
        ]
        return pl.pallas_call(
            body,
            in_specs=[
                pl.BlockSpec(memory_space=space.get(i, pltpu.VMEM)) for i in range(len(args))
            ],
            out_specs=[pl.BlockSpec(memory_space=pltpu.VMEM) for _ in outs],
            out_shape=[jax.ShapeDtypeStruct(o, F32) for o in outs],
            scratch_shapes=list(scratch),
            compiler_params=pltpu.CompilerParams(vmem_limit_bytes=VMEM_LIMIT),
        )(*args)

    return run


def pack_z(rhs, visc, mass, msg_even, msg_odd, sems):
    par = parity("gz")
    copies = []
    for out, up in ((msg_even, 1 - par), (msg_odd, par)):
        z = pl.ds(6 * up, 2)
        for c in range(3):
            copies.append((rhs.at[c, z], out.at[pl.ds(2 * c, 2)]))
        copies.append((visc.at[z], out.at[pl.ds(6, 2)]))
        copies.append((mass.at[pl.ds(7 * up, 1)], out.at[pl.ds(8, 1)]))
    copies = [pltpu.make_async_copy(*c, sems.at[i]) for i, c in enumerate(copies)]
    for c in copies:
        c.start()
    for c in copies:
        c.wait()


def pack_y_own(rhs, visc, mass, pscale, prhs, vbounds, pbounds, up, down, pt, coefs):
    def put(plane, value):
        down[plane] = value[:8]
        up[plane] = value[8:]

    for z in range(Z):
        for c in range(3):
            put(c * Z + z, rhs[c, z])
        put(3 * Z + z, visc[z])
        put(4 * Z + z, mass[z])
    for k in range(PZ):
        tile = jnp.concatenate([pscale[k], prhs[k]], axis=1)
        pt[k] = tile
        up[5 * Z + k] = tile
        down[5 * Z + k] = tile
    for i, bounds in enumerate((vbounds, pbounds)):
        for j, value in enumerate(coefficients(bounds)):
            coefs[5 * i + j] = value


def z_halo(got_even, got_odd, i):
    even = parity("gz") == 0
    a, b = got_even[i], got_odd[i]
    return jnp.where(even, b, a), jnp.where(even, a, b)


def pack_y_halo(got_even, got_odd, up, down):
    for i in range(9):
        for side, value in enumerate(z_halo(got_even, got_odd, i)):
            down[9 * side + i] = value[:8]
            up[9 * side + i] = value[8:]


def pack_x(
    rhs, visc, mass, got_even, got_odd, below_own, above_own, below_halo, above_halo, pt,
    main, up, down,
):
    def put(p, value, below, above):
        main[4 * p] = below
        main[4 * p + 1] = value[:8]
        main[4 * p + 2] = value[8:]
        main[4 * p + 3] = above

    for z in range(Z):
        for c in range(3):
            i = c * Z + z
            put(c * ZW + 2 + z, rhs[c, z], below_own[i], above_own[i])
        put(S0 + 2 + z, visc[z], below_own[3 * Z + z], above_own[3 * Z + z])
        put(M0 + 1 + z, mass[z], below_own[4 * Z + z], above_own[4 * Z + z])
    for i in range(9):
        field, j = divmod(i, 2)
        places = (field * ZW + j, field * ZW + ZW - 2 + j) if i < 8 else (M0, M0 + Z + 1)
        for side, value in enumerate(z_halo(got_even, got_odd, i)):
            put(places[side], value, below_halo[9 * side + i], above_halo[9 * side + i])
    lane = lanes()
    for k in range(PZ):
        tiles = (below_own[5 * Z + k], pt[k], above_own[5 * Z + k])
        for t, src in enumerate(tiles):
            turned = pltpu.roll(src, 64, axis=1)
            main[VT + 3 * k + t] = jnp.where(lane < 64, src, turned)
            main[VT + 12 + 3 * k + t] = jnp.where(lane < 64, turned, src)
    for i in range(PACKED):
        turned = main[16 * i : 16 * i + 16].reshape(X, X).T
        down[i] = turned[:8]
        up[i] = turned[X - 8 :]


def lanes():
    return lax.broadcasted_iota(jnp.int32, (8, X), 1)


def coefficients(bounds):
    low = jnp.full((8, X), bounds[0], F32)
    high = jnp.full((8, X), bounds[1], F32)
    centre = (high + low) / 2.0
    spread = (high - low) / 2.0
    sigma = centre / spread
    rho0 = 1.0 / sigma
    rho1 = 1.0 / (2.0 * sigma - rho0)
    rho2 = 1.0 / (2.0 * sigma - rho1)
    return 1.0 / centre, rho1 * rho0, 2.0 * rho1 / spread, rho2 * rho1, 2.0 * rho2 / spread


def tall(coef, rows):
    return jnp.concatenate([coef] * (rows // 8), axis=0)


def restriction():
    table = np.zeros((4, X, X), np.float32)
    for half in range(2):
        for l in range(X):
            x = l if half == 0 else (X + l if l < 8 else l - X)
            if half and 8 <= l < 120:
                continue
            for node in range(-2, PX + 2):
                o = x - 2 * node
                table[half, l, node + 2] = {-1: 0.25, 0: 0.5, 1: 0.25}.get(o, 0.0)
                table[2 + half, l, node + 2] = {-2: -0.125, -1: -0.25, 1: 0.25, 2: 0.125}.get(o, 0.0)
    return table.reshape(4 * X, X).astype(ml_dtypes.bfloat16)


SMOOTH_Z = {-1: (), 0: ((0, 0.5), (1, 0.25)), 4: ((7, 0.25),)}
DERIVE_Z = {
    -1: ((0, 0.125),),
    0: ((1, 0.25), (2, 0.125)),
    1: ((0, -0.125), (1, -0.25), (3, 0.25), (4, 0.125)),
    2: ((2, -0.125), (3, -0.25), (5, 0.25), (6, 0.125)),
    3: ((4, -0.125), (5, -0.25), (7, 0.25)),
    4: ((6, -0.125), (7, -0.25)),
}
for _k in (1, 2, 3):
    SMOOTH_Z[_k] = ((2 * _k - 1, 0.25), (2 * _k, 0.5), (2 * _k + 1, 0.25))


def smoothing():
    ring = np.eye(2 * X, dtype=np.float32)
    ring += 0.5 * (np.roll(ring, 1, axis=0) + np.roll(ring, -1, axis=0))
    return np.concatenate([ring, ring]).astype(ml_dtypes.bfloat16)


def split(value, parts):
    out = []
    for _ in range(parts):
        out.append(value.astype(jnp.bfloat16))
        value = value - out[-1].astype(F32)
    return out


def dot(a, b):
    return lax.dot_general(a, b, (((1,), (0,)), ((), ())), preferred_element_type=F32)


def velocity_step(
    main, from_below, from_above, table, ring, coefs, vel, coupled, pscale, msg_even, msg_odd,
    halo, w, d, r, u, t, lhs, s, g, q, ptmp,
):
    lane = lanes()
    gap = jnp.zeros((X - 16, X), F32)
    for i in range(PACKED):
        strips = jnp.concatenate([from_above[i], gap, from_below[i]], axis=0)
        halo[16 * i : 16 * i + 16] = strips.T.reshape(16, 8, X)

    inv, a1, g1, a2, g2 = (tall(coefs[i], 32) for i in range(5))
    t[...] = jnp.zeros_like(t)

    def planes(ref, p):
        return ref[pl.ds(4 * p, 4)].reshape(32, X)

    def smooth(k, z0, count):
        for c in range(3):
            def rows(z, _):
                for h in range(2):
                    src = w.at[k, c, h]
                    v = src[z] + 0.5 * (src[z - 1] + src[z + 1])
                    t[h, 8:40] = v
                    v = v + 0.5 * (t[h, 7:39] + t[h, 9:41])
                    at = pl.ds((c * count + z - z0) * 32, 32)
                    for part, value in enumerate(split(v, 2)):
                        lhs[at, (2 * part + h) * X : (2 * part + h + 1) * X] = value
                return 0

            lax.fori_loop(z0, z0 + count, rows, 0)
        total = 3 * count * 32
        s[:total] = dot(lhs[:total], ring[...])

    for c in range(3):
        def weight(z, _):
            for h, src in enumerate((main, halo)):
                w[0, c, h, z] = planes(src, S0 + z) * (planes(src, c * ZW + z) * inv)
            return 0

        lax.fori_loop(0, ZW, weight, 0)

    smooth(0, 1, Z + 2)
    for c in range(3):
        def sweep1(z, _):
            at = pl.ds((c * (Z + 2) + z - 1) * 32, 32)
            for h, src in enumerate((main, halo)):
                b = planes(src, c * ZW + z)
                visc = planes(src, S0 + z)
                d0 = b * inv
                lap = 16.0 * w[0, c, h, z] - 2.0 * s[at, h * X : (h + 1) * X]
                res = b - (visc * lap + planes(src, M0 + z - 1) * d0)
                d1 = a1 * d0 + g1 * res
                r[c, h, z] = res
                d[c, h, z] = d1
                w[1, c, h, z] = visc * d1
            return 0

        lax.fori_loop(1, ZW - 1, sweep1, 0)

    smooth(1, 2, Z)
    for c in range(3):
        def sweep2(z, _):
            at = pl.ds((c * Z + z - 2) * 32, 32)
            for h, src in enumerate((main, halo)):
                d1 = d[c, h, z]
                lap = 16.0 * w[1, c, h, z] - 2.0 * s[at, h * X : (h + 1) * X]
                res = r[c, h, z] - (planes(src, S0 + z) * lap + planes(src, M0 + z - 1) * d1)
                total = planes(src, c * ZW + z) * inv + d1 + (a2 * d1 + g2 * res)
                u[c, h, z - 2] = total
                if h == 0:
                    vel[c, z - 2] = total[8:24]
            return 0

        lax.fori_loop(2, ZW - 2, sweep2, 0)

    q[...] = jnp.zeros_like(q)
    for node in range(-1, 5):
        rows = slice(16 * (node + 1), 16 * (node + 1) + 12)

        def along_z(c, h, weights):
            acc = None
            for z, f in weights:
                term = f * u[c, h, z]
                acc = term if acc is None else acc + term
            return acc

        def at(k, start):
            return g[k, pl.ds(start, 12, stride=2), :]

        for h in range(2):
            cols = slice(X * h, X * (h + 1))
            g[2] = along_z(2, h, DERIVE_Z[node])
            total = 0.25 * (at(2, 3) + at(2, 5)) + 0.5 * at(2, 4)
            if SMOOTH_Z[node]:
                g[0] = along_z(0, h, SMOOTH_Z[node])
                g[1] = along_z(1, h, SMOOTH_Z[node])
                total = total + 0.25 * (at(1, 5) - at(1, 3)) + 0.125 * (at(1, 6) - at(1, 2))
                q[rows, 2 * X + X * h : 3 * X + X * h] = 0.25 * (at(0, 3) + at(0, 5)) + 0.5 * at(0, 4)
            q[rows, cols] = total

    div = sum(dot(v, table[...]) for v in reversed(split(q[...], 3)))

    def nodes(base, k):
        for i in range(3):
            own = pltpu.roll(main[base + 3 * k + i], 2, axis=1)
            side = halo[base + 3 * k + i]
            left = pltpu.roll(side, 2, axis=1)
            right = pltpu.roll(side, 66, axis=1)
            value = jnp.where(lane < 66, own, jnp.where(lane < 68, right, 0.0))
            ptmp[8 * i : 8 * i + 8] = jnp.where(lane < 2, left, value)
        return ptmp[6:18]

    coupled[...] = -div.reshape(6, 16, X)
    pscale[...] = jnp.zeros_like(pscale)
    for k in range(PZ):
        pscale[k, :12] = nodes(VT, k)
        coupled[k + 1, :12] = nodes(VT + 12, k) - div[16 * (k + 1) : 16 * (k + 1) + 12]
    par = parity("gz")
    for out, up in ((msg_even, 1 - par), (msg_odd, par)):
        for j in range(3):
            out[j] = coupled[3 * up + j]
        for j in range(2):
            out[3 + j] = pscale[2 * up + j]


def pressure_step(coupled, pscale, got_even, got_odd, coefs, out):
    below, above = [], []
    for i in range(5):
        low, high = z_halo(got_even, got_odd, i)
        below.append(low)
        above.append(high)
    b = [
        below[0], below[1] + coupled[0], below[2] + coupled[1], coupled[2], coupled[3],
        coupled[4] + above[0], coupled[5] + above[1], above[2],
    ]
    s = [below[3], below[4], pscale[0], pscale[1], pscale[2], pscale[3], above[3], above[4]]
    inv, a1, g1, a2, g2 = (tall(coefs[5 + i], 16) for i in range(5))

    def operator(w, z):
        v = (1.0 / 6.0) * (w[z - 1] + w[z + 1]) + (2.0 / 3.0) * w[z]
        v = (1.0 / 6.0) * (pltpu.roll(v, 1, axis=0) + pltpu.roll(v, 15, axis=0)) + (2.0 / 3.0) * v
        v = (1.0 / 6.0) * (pltpu.roll(v, 1, axis=1) + pltpu.roll(v, X - 1, axis=1)) + (2.0 / 3.0) * v
        return s[z] * v

    d0 = [v * inv for v in b]
    w = [x * y for x, y in zip(s, d0)]
    r1, d1, w1 = [None] * 8, [None] * 8, [None] * 8
    for z in range(1, 7):
        r1[z] = b[z] - operator(w, z)
        d1[z] = a1 * d0[z] + g1 * r1[z]
        w1[z] = s[z] * d1[z]
    for z in range(2, 6):
        res = r1[z] - operator(w1, z)
        total = d0[z] + d1[z] + (a2 * d1[z] + g2 * res)
        total = pltpu.roll(pltpu.roll(total, 14, axis=0), X - 2, axis=1)
        out[z - 2] = total[:PY, :PX]


def per_device(rhs, prhs, visc, mass, pscale, vbounds, pbounds):
    plane, tile = (Y, X), (8, X)
    msg_even, msg_odd = call(
        pack_z, [(9, *plane)] * 2, scratch=[pltpu.SemaphoreType.DMA((10,))], hbm=(0, 1, 2)
    )(rhs, visc, mass)
    z_halos = swap_neighbours("gz", msg_even, msg_odd)
    up, down, pt, coefs = call(
        pack_y_own, [(5 * Z + PZ, *tile)] * 2 + [(PZ, *tile), (10, *tile)], smem=(5, 6)
    )(rhs, visc, mass, pscale, prhs, vbounds, pbounds)
    y_own = both_neighbours("gy", up, down)
    up, down = call(pack_y_halo, [(18, *tile)] * 2)(*z_halos)
    y_halos = both_neighbours("gy", up, down)
    main, up, down = call(pack_x, [(TILES, *tile), (PACKED, *tile), (PACKED, *tile)])(
        rhs, visc, mass, *z_halos, *y_own, *y_halos, pt
    )
    below, above = both_neighbours("gx", up, down)
    vel, coupled, scale, msg_even, msg_odd = call(
        velocity_step,
        [(3, Z, Y, X), (6, *plane), (PZ, *plane), (5, *plane), (5, *plane)],
        scratch=[
            pltpu.VMEM((TILES, 8, X), F32),
            pltpu.VMEM((2, 3, 2, ZW, 32, X), F32),
            pltpu.VMEM((3, 2, ZW, 32, X), F32),
            pltpu.VMEM((3, 2, ZW, 32, X), F32),
            pltpu.VMEM((3, 2, Z, 32, X), F32),
            pltpu.VMEM((2, 48, X), F32),
            pltpu.VMEM((3 * (Z + 2) * 32, 4 * X), jnp.bfloat16),
            pltpu.VMEM((3 * (Z + 2) * 32, 2 * X), F32),
            pltpu.VMEM((3, 32, X), F32),
            pltpu.VMEM((96, 4 * X), F32),
            pltpu.VMEM((24, X), F32),
        ],
    )(main, below, above, jnp.asarray(restriction()), jnp.asarray(smoothing()), coefs)
    z_halos = swap_neighbours("gz", msg_even, msg_odd)
    (pressure,) = call(pressure_step, [(PZ, PY, PX)])(coupled, scale, *z_halos, coefs)
    return vel, pressure


def solution(mesh):
    block = P("gz", "gy", "gx")
    field = P(None, "gz", "gy", "gx")
    return jax.shard_map(
        per_device,
        mesh=mesh,
        in_specs=(field, block, block, block, block, P(), P()),
        out_specs=(field, block),
        check_vma=False,
    )
```

```python
import jax
import jax.numpy as jnp
import ml_dtypes
import numpy as np
from jax import lax
from jax.experimental import pallas as pl
from jax.experimental.pallas import tpu as pltpu
from jax.sharding import PartitionSpec as P


Z, Y, X = 8, 16, 128
PZ, PY, PX = 4, 8, 64
F32 = jnp.float32
VMEM_LIMIT = 16 * 2**20

ZW = Z + 4
PLANES = 4 * ZW + Z + 2
S0, M0 = 3 * ZW, 4 * ZW
VT = 4 * PLANES
TILES = VT + 24
PACKED = TILES // 16


def parity(axis):
    return lax.rem(lax.axis_index(axis), 2)


def swap_neighbours(axis, first, second):
    size = lax.axis_size(axis)
    even = [(i, i ^ 1) for i in range(size)]
    odd = [(i, ((i + 1) ^ 1) - 1) for i in range(1, size - 1)]
    inner = lax.ppermute(first, axis, even)
    outer = lax.ppermute(second, axis, odd)
    return inner, outer


def both_neighbours(axis, to_above, to_below):
    size = lax.axis_size(axis)
    up = [(i, i + 1) for i in range(size - 1)]
    down = [(i + 1, i) for i in range(size - 1)]
    from_below = lax.ppermute(to_above, axis, up)
    from_above = lax.ppermute(to_below, axis, down)
    return from_below, from_above


def call(body, outs, scratch=(), smem=(), hbm=()):
    def run(*args):
        space = {i: pltpu.SMEM for i in smem} | {i: pltpu.HBM for i in hbm}
        args = [
            pltpu.with_memory_space_constraint(x, pltpu.HBM) if i in hbm else x
            for i, x in enumerate(args)
        ]
        return pl.pallas_call(
            body,
            in_specs=[
                pl.BlockSpec(memory_space=space.get(i, pltpu.VMEM)) for i in range(len(args))
            ],
            out_specs=[pl.BlockSpec(memory_space=pltpu.VMEM) for _ in outs],
            out_shape=[jax.ShapeDtypeStruct(o, F32) for o in outs],
            scratch_shapes=list(scratch),
            compiler_params=pltpu.CompilerParams(vmem_limit_bytes=VMEM_LIMIT),
        )(*args)

    return run


def pack_z(rhs, visc, mass, msg_even, msg_odd, sems):
    par = parity("gz")
    copies = []
    for out, up in ((msg_even, 1 - par), (msg_odd, par)):
        z = pl.ds(6 * up, 2)
        for c in range(3):
            copies.append((rhs.at[c, z], out.at[pl.ds(2 * c, 2)]))
        copies.append((visc.at[z], out.at[pl.ds(6, 2)]))
        copies.append((mass.at[pl.ds(7 * up, 1)], out.at[pl.ds(8, 1)]))
    copies = [pltpu.make_async_copy(*c, sems.at[i]) for i, c in enumerate(copies)]
    for c in copies:
        c.start()
    for c in copies:
        c.wait()


def scalars(vbounds, pbounds, coefs):
    for i, bounds in enumerate((vbounds, pbounds)):
        for j, value in enumerate(coefficients(bounds)):
            coefs[5 * i + j] = value


def z_halo(got_even, got_odd, i):
    even = parity("gz") == 0
    a, b = got_even[i], got_odd[i]
    return jnp.where(even, b, a), jnp.where(even, a, b)


def pack_y(rhs, visc, mass, got_even, got_odd, pscale, prhs, up, down):
    def put(plane, value):
        down[plane] = value[:8]
        up[plane] = value[8:]

    for z in range(Z):
        for c in range(3):
            put(c * ZW + 2 + z, rhs[c, z])
        put(S0 + 2 + z, visc[z])
        put(M0 + 1 + z, mass[z])
    for i in range(9):
        field, j = divmod(i, 2)
        places = (field * ZW + j, field * ZW + ZW - 2 + j) if i < 8 else (M0, M0 + Z + 1)
        for place, value in zip(places, z_halo(got_even, got_odd, i)):
            put(place, value)
    for k in range(PZ):
        tile = jnp.concatenate([pscale[k], prhs[k]], axis=1)
        up[PLANES + k] = tile
        down[PLANES + k] = tile


def pack_x(low_rows, high_rows, below, above, main, up, down):
    for p in range(PLANES):
        for i, src in enumerate((below, low_rows, high_rows, above)):
            main[4 * p + i] = src[p]
    lane = lanes()
    for k in range(PZ):
        for t, src in enumerate((below, low_rows, above)):
            tile = src[PLANES + k]
            turned = pltpu.roll(tile, 64, axis=1)
            main[VT + 3 * k + t] = jnp.where(lane < 64, tile, turned)
            main[VT + 12 + 3 * k + t] = jnp.where(lane < 64, turned, tile)
    for i in range(PACKED):
        turned = main[16 * i : 16 * i + 16].reshape(X, X).T
        down[i] = turned[:8]
        up[i] = turned[X - 8 :]


def lanes():
    return lax.broadcasted_iota(jnp.int32, (8, X), 1)


def coefficients(bounds):
    low = jnp.full((8, X), bounds[0], F32)
    high = jnp.full((8, X), bounds[1], F32)
    centre = (high + low) / 2.0
    spread = (high - low) / 2.0
    sigma = centre / spread
    rho0 = 1.0 / sigma
    rho1 = 1.0 / (2.0 * sigma - rho0)
    rho2 = 1.0 / (2.0 * sigma - rho1)
    return 1.0 / centre, rho1 * rho0, 2.0 * rho1 / spread, rho2 * rho1, 2.0 * rho2 / spread


def tall(coef, rows):
    return jnp.concatenate([coef] * (rows // 8), axis=0)


def restriction():
    table = np.zeros((4, X, X), np.float32)
    for half in range(2):
        for l in range(X):
            x = l if half == 0 else (X + l if l < 8 else l - X)
            if half and 8 <= l < 120:
                continue
            for node in range(-2, PX + 2):
                o = x - 2 * node
                table[half, l, node + 2] = {-1: 0.25, 0: 0.5, 1: 0.25}.get(o, 0.0)
                table[2 + half, l, node + 2] = {-2: -0.125, -1: -0.25, 1: 0.25, 2: 0.125}.get(o, 0.0)
    return table.reshape(4 * X, X).astype(ml_dtypes.bfloat16)


SMOOTH_Z = {-1: (), 0: ((0, 0.5), (1, 0.25)), 4: ((7, 0.25),)}
DERIVE_Z = {
    -1: ((0, 0.125),),
    0: ((1, 0.25), (2, 0.125)),
    1: ((0, -0.125), (1, -0.25), (3, 0.25), (4, 0.125)),
    2: ((2, -0.125), (3, -0.25), (5, 0.25), (6, 0.125)),
    3: ((4, -0.125), (5, -0.25), (7, 0.25)),
    4: ((6, -0.125), (7, -0.25)),
}
for _k in (1, 2, 3):
    SMOOTH_Z[_k] = ((2 * _k - 1, 0.25), (2 * _k, 0.5), (2 * _k + 1, 0.25))


def smoothing():
    ring = np.eye(2 * X, dtype=np.float32)
    ring += 0.5 * (np.roll(ring, 1, axis=0) + np.roll(ring, -1, axis=0))
    return np.concatenate([ring, ring]).astype(ml_dtypes.bfloat16)


def split(value, parts):
    out = []
    for _ in range(parts):
        out.append(value.astype(jnp.bfloat16))
        value = value - out[-1].astype(F32)
    return out


def dot(a, b):
    return lax.dot_general(a, b, (((1,), (0,)), ((), ())), preferred_element_type=F32)


def velocity_step(
    main, from_below, from_above, table, ring, coefs, vel, coupled, pscale, msg_even, msg_odd,
    halo, w, d, r, u, t, lhs, s, g, q, ptmp,
):
    lane = lanes()
    gap = jnp.zeros((X - 16, X), F32)
    for i in range(PACKED):
        strips = jnp.concatenate([from_above[i], gap, from_below[i]], axis=0)
        halo[16 * i : 16 * i + 16] = strips.T.reshape(16, 8, X)

    inv, a1, g1, a2, g2 = (tall(coefs[i], 32) for i in range(5))
    t[...] = jnp.zeros_like(t)

    def planes(ref, p):
        return ref[pl.ds(4 * p, 4)].reshape(32, X)

    def smooth(k, z0, count):
        for c in range(3):
            def rows(z, _):
                for h in range(2):
                    src = w.at[k, c, h]
                    v = src[z] + 0.5 * (src[z - 1] + src[z + 1])
                    t[h, 8:40] = v
                    v = v + 0.5 * (t[h, 7:39] + t[h, 9:41])
                    at = pl.ds((c * count + z - z0) * 32, 32)
                    for part, value in enumerate(split(v, 2)):
                        lhs[at, (2 * part + h) * X : (2 * part + h + 1) * X] = value
                return 0

            lax.fori_loop(z0, z0 + count, rows, 0)
        total = 3 * count * 32
        s[:total] = dot(lhs[:total], ring[...])

    for c in range(3):
        def weight(z, _):
            for h, src in enumerate((main, halo)):
                w[0, c, h, z] = planes(src, S0 + z) * (planes(src, c * ZW + z) * inv)
            return 0

        lax.fori_loop(0, ZW, weight, 0)

    smooth(0, 1, Z + 2)
    for c in range(3):
        def sweep1(z, _):
            at = pl.ds((c * (Z + 2) + z - 1) * 32, 32)
            for h, src in enumerate((main, halo)):
                b = planes(src, c * ZW + z)
                visc = planes(src, S0 + z)
                d0 = b * inv
                lap = 16.0 * w[0, c, h, z] - 2.0 * s[at, h * X : (h + 1) * X]
                res = b - (visc * lap + planes(src, M0 + z - 1) * d0)
                d1 = a1 * d0 + g1 * res
                r[c, h, z] = res
                d[c, h, z] = d1
                w[1, c, h, z] = visc * d1
            return 0

        lax.fori_loop(1, ZW - 1, sweep1, 0)

    smooth(1, 2, Z)
    for c in range(3):
        def sweep2(z, _):
            at = pl.ds((c * Z + z - 2) * 32, 32)
            for h, src in enumerate((main, halo)):
                d1 = d[c, h, z]
                lap = 16.0 * w[1, c, h, z] - 2.0 * s[at, h * X : (h + 1) * X]
                res = r[c, h, z] - (planes(src, S0 + z) * lap + planes(src, M0 + z - 1) * d1)
                total = planes(src, c * ZW + z) * inv + d1 + (a2 * d1 + g2 * res)
                u[c, h, z - 2] = total
                if h == 0:
                    vel[c, z - 2] = total[8:24]
            return 0

        lax.fori_loop(2, ZW - 2, sweep2, 0)

    q[...] = jnp.zeros_like(q)
    for node in range(-1, 5):
        rows = slice(16 * (node + 1), 16 * (node + 1) + 12)

        def along_z(c, h, weights):
            acc = None
            for z, f in weights:
                term = f * u[c, h, z]
                acc = term if acc is None else acc + term
            return acc

        def at(k, start):
            return g[k, pl.ds(start, 12, stride=2), :]

        for h in range(2):
            cols = slice(X * h, X * (h + 1))
            g[2] = along_z(2, h, DERIVE_Z[node])
            total = 0.25 * (at(2, 3) + at(2, 5)) + 0.5 * at(2, 4)
            if SMOOTH_Z[node]:
                g[0] = along_z(0, h, SMOOTH_Z[node])
                g[1] = along_z(1, h, SMOOTH_Z[node])
                total = total + 0.25 * (at(1, 5) - at(1, 3)) + 0.125 * (at(1, 6) - at(1, 2))
                q[rows, 2 * X + X * h : 3 * X + X * h] = 0.25 * (at(0, 3) + at(0, 5)) + 0.5 * at(0, 4)
            q[rows, cols] = total

    div = sum(dot(v, table[...]) for v in reversed(split(q[...], 3)))

    def nodes(base, k):
        for i in range(3):
            own = pltpu.roll(main[base + 3 * k + i], 2, axis=1)
            side = halo[base + 3 * k + i]
            left = pltpu.roll(side, 2, axis=1)
            right = pltpu.roll(side, 66, axis=1)
            value = jnp.where(lane < 66, own, jnp.where(lane < 68, right, 0.0))
            ptmp[8 * i : 8 * i + 8] = jnp.where(lane < 2, left, value)
        return ptmp[6:18]

    coupled[...] = -div.reshape(6, 16, X)
    pscale[...] = jnp.zeros_like(pscale)
    for k in range(PZ):
        pscale[k, :12] = nodes(VT, k)
        coupled[k + 1, :12] = nodes(VT + 12, k) - div[16 * (k + 1) : 16 * (k + 1) + 12]
    par = parity("gz")
    for out, up in ((msg_even, 1 - par), (msg_odd, par)):
        for j in range(3):
            out[j] = coupled[3 * up + j]
        for j in range(2):
            out[3 + j] = pscale[2 * up + j]


def pressure_step(coupled, pscale, got_even, got_odd, coefs, out):
    below, above = [], []
    for i in range(5):
        low, high = z_halo(got_even, got_odd, i)
        below.append(low)
        above.append(high)
    b = [
        below[0], below[1] + coupled[0], below[2] + coupled[1], coupled[2], coupled[3],
        coupled[4] + above[0], coupled[5] + above[1], above[2],
    ]
    s = [below[3], below[4], pscale[0], pscale[1], pscale[2], pscale[3], above[3], above[4]]
    inv, a1, g1, a2, g2 = (tall(coefs[5 + i], 16) for i in range(5))

    def operator(w, z):
        v = (1.0 / 6.0) * (w[z - 1] + w[z + 1]) + (2.0 / 3.0) * w[z]
        v = (1.0 / 6.0) * (pltpu.roll(v, 1, axis=0) + pltpu.roll(v, 15, axis=0)) + (2.0 / 3.0) * v
        v = (1.0 / 6.0) * (pltpu.roll(v, 1, axis=1) + pltpu.roll(v, X - 1, axis=1)) + (2.0 / 3.0) * v
        return s[z] * v

    d0 = [v * inv for v in b]
    w = [x * y for x, y in zip(s, d0)]
    r1, d1, w1 = [None] * 8, [None] * 8, [None] * 8
    for z in range(1, 7):
        r1[z] = b[z] - operator(w, z)
        d1[z] = a1 * d0[z] + g1 * r1[z]
        w1[z] = s[z] * d1[z]
    for z in range(2, 6):
        res = r1[z] - operator(w1, z)
        total = d0[z] + d1[z] + (a2 * d1[z] + g2 * res)
        total = pltpu.roll(pltpu.roll(total, 14, axis=0), X - 2, axis=1)
        out[z - 2] = total[:PY, :PX]


def per_device(rhs, prhs, visc, mass, pscale, vbounds, pbounds):
    plane, tile = (Y, X), (8, X)
    msg_even, msg_odd = call(
        pack_z, [(9, *plane)] * 2, scratch=[pltpu.SemaphoreType.DMA((10,))], hbm=(0, 1, 2)
    )(rhs, visc, mass)
    z_halos = swap_neighbours("gz", msg_even, msg_odd)
    (coefs,) = call(scalars, [(10, *tile)], smem=(0, 1))(vbounds, pbounds)
    up, down = call(pack_y, [(PLANES + PZ, *tile)] * 2)(rhs, visc, mass, *z_halos, pscale, prhs)
    below, above = both_neighbours("gy", up, down)
    main, up, down = call(pack_x, [(TILES, *tile), (PACKED, *tile), (PACKED, *tile)])(
        down, up, below, above
    )
    below, above = both_neighbours("gx", up, down)
    vel, coupled, scale, msg_even, msg_odd = call(
        velocity_step,
        [(3, Z, Y, X), (6, *plane), (PZ, *plane), (5, *plane), (5, *plane)],
        scratch=[
            pltpu.VMEM((TILES, 8, X), F32),
            pltpu.VMEM((2, 3, 2, ZW, 32, X), F32),
            pltpu.VMEM((3, 2, ZW, 32, X), F32),
            pltpu.VMEM((3, 2, ZW, 32, X), F32),
            pltpu.VMEM((3, 2, Z, 32, X), F32),
            pltpu.VMEM((2, 48, X), F32),
            pltpu.VMEM((3 * (Z + 2) * 32, 4 * X), jnp.bfloat16),
            pltpu.VMEM((3 * (Z + 2) * 32, 2 * X), F32),
            pltpu.VMEM((3, 32, X), F32),
            pltpu.VMEM((96, 4 * X), F32),
            pltpu.VMEM((24, X), F32),
        ],
    )(main, below, above, jnp.asarray(restriction()), jnp.asarray(smoothing()), coefs)
    z_halos = swap_neighbours("gz", msg_even, msg_odd)
    (pressure,) = call(pressure_step, [(PZ, PY, PX)])(coupled, scale, *z_halos, coefs)
    return vel, pressure


def solution(mesh):
    block = P("gz", "gy", "gx")
    field = P(None, "gz", "gy", "gx")
    return jax.shard_map(
        per_device,
        mesh=mesh,
        in_specs=(field, block, block, block, block, P(), P()),
        out_specs=(field, block),
        check_vma=False,
    )
```

```python
import jax
import jax.numpy as jnp
import ml_dtypes
import numpy as np
from jax import lax
from jax.experimental import pallas as pl
from jax.experimental.pallas import tpu as pltpu
from jax.sharding import PartitionSpec as P


Z, Y, X = 8, 16, 128
PZ, PY, PX = 4, 8, 64
F32 = jnp.float32
VMEM_LIMIT = 16 * 2**20

ZW = Z + 4
PLANES = 4 * ZW + Z + 2
S0, M0 = 3 * ZW, 4 * ZW
VT = 4 * PLANES
TILES = VT + 24
PACKED = TILES // 16


def parity(axis):
    return lax.rem(lax.axis_index(axis), 2)


def swap_neighbours(axis, first, second):
    size = lax.axis_size(axis)
    even = [(i, i ^ 1) for i in range(size)]
    odd = [(i, ((i + 1) ^ 1) - 1) for i in range(1, size - 1)]
    inner = lax.ppermute(first, axis, even)
    outer = lax.ppermute(second, axis, odd)
    return inner, outer


def both_neighbours(axis, to_above, to_below):
    size = lax.axis_size(axis)
    up = [(i, i + 1) for i in range(size - 1)]
    down = [(i + 1, i) for i in range(size - 1)]
    from_below = lax.ppermute(to_above, axis, up)
    from_above = lax.ppermute(to_below, axis, down)
    return from_below, from_above


def call(body, outs, scratch=(), smem=(), hbm=(), vmem=()):
    def run(*args):
        space = {i: pltpu.SMEM for i in smem} | {i: pltpu.HBM for i in hbm}
        args = [
            pltpu.with_memory_space_constraint(x, pltpu.HBM) if i in hbm else x
            for i, x in enumerate(args)
        ]
        return pl.pallas_call(
            body,
            in_specs=[
                pl.BlockSpec(memory_space=space.get(i, pltpu.VMEM)) for i in range(len(args))
            ],
            out_specs=[pl.BlockSpec(memory_space=pltpu.VMEM) for _ in outs],
            out_shape=[
                pltpu.VMEM(o, F32) if i in vmem else jax.ShapeDtypeStruct(o, F32)
                for i, o in enumerate(outs)
            ],
            scratch_shapes=list(scratch),
            compiler_params=pltpu.CompilerParams(vmem_limit_bytes=VMEM_LIMIT),
        )(*args)

    return run


def pack_z(rhs, visc, mass, msg_even, msg_odd, far, sems):
    par = parity("gz")
    copies = []
    for i, (out, up) in enumerate(((msg_even, 1 - par), (msg_odd, par))):
        near, deep = 7 * up, 1 + 5 * up
        copies += [
            (rhs.at[:, near], out.at[3:6]),
            (visc.at[near], out.at[6]),
            (mass.at[near], out.at[7]),
            (rhs.at[:, deep], far.at[i, :3]),
            (visc.at[deep], far.at[i, 3]),
        ]
    copies = [pltpu.make_async_copy(*c, sems.at[i]) for i, c in enumerate(copies)]
    for c in copies:
        c.start()
    for c in copies:
        c.wait()
    for i, out in enumerate((msg_even, msg_odd)):
        for c in range(3):
            out[c] = far[i, c] * far[i, 3]


def scalars(vbounds, pbounds, coefs):
    for i, bounds in enumerate((vbounds, pbounds)):
        for j, value in enumerate(coefficients(bounds)):
            coefs[5 * i + j] = value


def z_halo(got_even, got_odd, i):
    even = parity("gz") == 0
    a, b = got_even[i], got_odd[i]
    return jnp.where(even, b, a), jnp.where(even, a, b)


def y_rows():
    out = []
    for p in range(PLANES):
        if p not in (S0, S0 + ZW - 1):
            out.append((p, 8, 7) if p // ZW == 1 else (p, 7, 6))
    return out


UP_ROWS = sum(r[1] for r in y_rows())
DOWN_ROWS = sum(r[2] for r in y_rows())


def padded(rows):
    return -(-rows // 8) * 8


def pack_nodes(pscale, prhs, pt):
    for k in range(PZ):
        pt[k] = jnp.concatenate([pscale[k], prhs[k]], axis=1)


def pack_y(rhs, visc, mass, got_even, got_odd, pt, own, up, down):
    for z in range(Z):
        for c in range(3):
            own[c * ZW + 2 + z] = rhs[c, z]
        own[S0 + 2 + z] = visc[z]
        own[M0 + 1 + z] = mass[z]
    for side, (deep, near) in enumerate(((0, 1), (ZW - 1, ZW - 2))):
        for c in range(3):
            own[c * ZW + deep] = z_halo(got_even, got_odd, c)[side]
            own[c * ZW + near] = z_halo(got_even, got_odd, 3 + c)[side]
        own[S0 + deep] = jnp.ones((Y, X), F32)
        own[S0 + near] = z_halo(got_even, got_odd, 6)[side]
        own[M0 + near - 1] = z_halo(got_even, got_odd, 7)[side]
    row = lax.broadcasted_iota(jnp.int32, (8, X), 0)
    at_up = at_down = 0
    for p, n_up, n_down in y_rows():
        if p // ZW == 1:
            z = p - ZW
            up[at_up : at_up + 8] = own[p, 8:] * jnp.where(row == 0, own[S0 + z, 8:], 1.0)
            part = own[p, :8] * jnp.where(row == 6, own[S0 + z, :8], 1.0)
            down[at_down : at_down + 7] = part[:7]
        else:
            up[at_up : at_up + n_up] = own[p, Y - n_up :]
            down[at_down : at_down + n_down] = own[p, :n_down]
        at_up, at_down = at_up + n_up, at_down + n_down
    for k in range(PZ):
        up[at_up + 2 * k : at_up + 2 * k + 2] = pt[k, 6:]
        down[at_down + 2 * k : at_down + 2 * k + 2] = pt[k, :2]


def pack_x(own, pt, below, above, main, up, down):
    at_up = at_down = 0
    rows = {r[0]: r[1:] for r in y_rows()}
    for p in range(PLANES):
        rest = jnp.full((8, X), 1.0 if S0 <= p < M0 else 0.0, F32)
        main[4 * p] = rest
        main[4 * p + 1] = own[p, :8]
        main[4 * p + 2] = own[p, 8:]
        main[4 * p + 3] = rest
        n_up, n_down = rows.get(p, (0, 0))
        if n_up:
            main[4 * p, 8 - n_up :] = below[at_up : at_up + n_up]
            main[4 * p + 3, :n_down] = above[at_down : at_down + n_down]
        at_up, at_down = at_up + n_up, at_down + n_down
    for k in range(PZ):
        for t in (0, 2):
            main[VT + 3 * k + t] = jnp.zeros((8, X), F32)
        main[VT + 3 * k, 6:] = below[at_up + 2 * k : at_up + 2 * k + 2]
        main[VT + 3 * k + 1] = pt[k]
        main[VT + 3 * k + 2, :2] = above[at_down + 2 * k : at_down + 2 * k + 2]
    lane = lanes()
    for k in range(PZ):
        for t in range(3):
            tile = main[VT + 3 * k + t]
            turned = pltpu.roll(tile, 64, axis=1)
            main[VT + 3 * k + t] = jnp.where(lane < 64, tile, turned)
            main[VT + 12 + 3 * k + t] = jnp.where(lane < 64, turned, tile)
    for i in range(PACKED):
        turned = main[16 * i : 16 * i + 16].reshape(X, X).T
        down[i] = turned[:8]
        up[i] = turned[X - 8 :]


def lanes():
    return lax.broadcasted_iota(jnp.int32, (8, X), 1)


def coefficients(bounds):
    low = jnp.full((8, X), bounds[0], F32)
    high = jnp.full((8, X), bounds[1], F32)
    centre = (high + low) / 2.0
    spread = (high - low) / 2.0
    sigma = centre / spread
    rho0 = 1.0 / sigma
    rho1 = 1.0 / (2.0 * sigma - rho0)
    rho2 = 1.0 / (2.0 * sigma - rho1)
    return 1.0 / centre, rho1 * rho0, 2.0 * rho1 / spread, rho2 * rho1, 2.0 * rho2 / spread


def tall(coef, rows):
    return jnp.concatenate([coef] * (rows // 8), axis=0)


def restriction():
    table = np.zeros((4, X, X), np.float32)
    for half in range(2):
        for l in range(X):
            x = l if half == 0 else (X + l if l < 8 else l - X)
            if half and 8 <= l < 120:
                continue
            for node in range(-2, PX + 2):
                o = x - 2 * node
                table[half, l, node + 2] = {-1: 0.25, 0: 0.5, 1: 0.25}.get(o, 0.0)
                table[2 + half, l, node + 2] = {-2: -0.125, -1: -0.25, 1: 0.25, 2: 0.125}.get(o, 0.0)
    return table.reshape(4 * X, X).astype(ml_dtypes.bfloat16)


SMOOTH_Z = {-1: (), 0: ((0, 0.5), (1, 0.25)), 4: ((7, 0.25),)}
DERIVE_Z = {
    -1: ((0, 0.125),),
    0: ((1, 0.25), (2, 0.125)),
    1: ((0, -0.125), (1, -0.25), (3, 0.25), (4, 0.125)),
    2: ((2, -0.125), (3, -0.25), (5, 0.25), (6, 0.125)),
    3: ((4, -0.125), (5, -0.25), (7, 0.25)),
    4: ((6, -0.125), (7, -0.25)),
}
for _k in (1, 2, 3):
    SMOOTH_Z[_k] = ((2 * _k - 1, 0.25), (2 * _k, 0.5), (2 * _k + 1, 0.25))


def smoothing():
    ring = np.eye(2 * X, dtype=np.float32)
    ring += 0.5 * (np.roll(ring, 1, axis=0) + np.roll(ring, -1, axis=0))
    return np.concatenate([ring, ring]).astype(ml_dtypes.bfloat16)


def split(value, parts):
    out = []
    for _ in range(parts):
        out.append(value.astype(jnp.bfloat16))
        value = value - out[-1].astype(F32)
    return out


def dot(a, b):
    return lax.dot_general(a, b, (((1,), (0,)), ((), ())), preferred_element_type=F32)


def velocity_step(
    main, from_below, from_above, table, ring, coefs, vel, coupled, pscale, msg_even, msg_odd,
    halo, w, d, r, u, t, lhs, s, g, q, ptmp,
):
    lane = lanes()
    gap = jnp.zeros((X - 16, X), F32)
    for i in range(PACKED):
        strips = jnp.concatenate([from_above[i], gap, from_below[i]], axis=0)
        halo[16 * i : 16 * i + 16] = strips.T.reshape(16, 8, X)

    inv, a1, g1, a2, g2 = (tall(coefs[i], 32) for i in range(5))
    t[...] = jnp.zeros_like(t)

    def planes(ref, p):
        return ref[pl.ds(4 * p, 4)].reshape(32, X)

    def smooth(k, z0, count):
        for c in range(3):
            def rows(z, _):
                for h in range(2):
                    src = w.at[k, c, h]
                    v = src[z] + 0.5 * (src[z - 1] + src[z + 1])
                    t[h, 8:40] = v
                    v = v + 0.5 * (t[h, 7:39] + t[h, 9:41])
                    at = pl.ds((c * count + z - z0) * 32, 32)
                    for part, value in enumerate(split(v, 2)):
                        lhs[at, (2 * part + h) * X : (2 * part + h + 1) * X] = value
                return 0

            lax.fori_loop(z0, z0 + count, rows, 0)
        total = 3 * count * 32
        s[:total] = dot(lhs[:total], ring[...])

    for c in range(3):
        def weight(z, _):
            for h, src in enumerate((main, halo)):
                w[0, c, h, z] = planes(src, S0 + z) * (planes(src, c * ZW + z) * inv)
            return 0

        lax.fori_loop(0, ZW, weight, 0)

    smooth(0, 1, Z + 2)
    for c in range(3):
        def sweep1(z, _):
            at = pl.ds((c * (Z + 2) + z - 1) * 32, 32)
            for h, src in enumerate((main, halo)):
                b = planes(src, c * ZW + z)
                visc = planes(src, S0 + z)
                d0 = b * inv
                lap = 16.0 * w[0, c, h, z] - 2.0 * s[at, h * X : (h + 1) * X]
                res = b - (visc * lap + planes(src, M0 + z - 1) * d0)
                d1 = a1 * d0 + g1 * res
                r[c, h, z] = res
                d[c, h, z] = d1
                w[1, c, h, z] = visc * d1
            return 0

        lax.fori_loop(1, ZW - 1, sweep1, 0)

    smooth(1, 2, Z)
    for c in range(3):
        def sweep2(z, _):
            at = pl.ds((c * Z + z - 2) * 32, 32)
            for h, src in enumerate((main, halo)):
                d1 = d[c, h, z]
                lap = 16.0 * w[1, c, h, z] - 2.0 * s[at, h * X : (h + 1) * X]
                res = r[c, h, z] - (planes(src, S0 + z) * lap + planes(src, M0 + z - 1) * d1)
                total = planes(src, c * ZW + z) * inv + d1 + (a2 * d1 + g2 * res)
                u[c, h, z - 2] = total
                if h == 0:
                    vel[c, z - 2] = total[8:24]
            return 0

        lax.fori_loop(2, ZW - 2, sweep2, 0)

    q[...] = jnp.zeros_like(q)
    for node in range(-1, 5):
        rows = slice(16 * (node + 1), 16 * (node + 1) + 12)

        def along_z(c, h, weights):
            acc = None
            for z, f in weights:
                term = f * u[c, h, z]
                acc = term if acc is None else acc + term
            return acc

        def at(k, start):
            return g[k, pl.ds(start, 12, stride=2), :]

        for h in range(2):
            cols = slice(X * h, X * (h + 1))
            g[2] = along_z(2, h, DERIVE_Z[node])
            total = 0.25 * (at(2, 3) + at(2, 5)) + 0.5 * at(2, 4)
            if SMOOTH_Z[node]:
                g[0] = along_z(0, h, SMOOTH_Z[node])
                g[1] = along_z(1, h, SMOOTH_Z[node])
                total = total + 0.25 * (at(1, 5) - at(1, 3)) + 0.125 * (at(1, 6) - at(1, 2))
                q[rows, 2 * X + X * h : 3 * X + X * h] = 0.25 * (at(0, 3) + at(0, 5)) + 0.5 * at(0, 4)
            q[rows, cols] = total

    div = sum(dot(v, table[...]) for v in reversed(split(q[...], 3)))

    def nodes(base, k):
        for i in range(3):
            own = pltpu.roll(main[base + 3 * k + i], 2, axis=1)
            side = halo[base + 3 * k + i]
            left = pltpu.roll(side, 2, axis=1)
            right = pltpu.roll(side, 66, axis=1)
            value = jnp.where(lane < 66, own, jnp.where(lane < 68, right, 0.0))
            ptmp[8 * i : 8 * i + 8] = jnp.where(lane < 2, left, value)
        return ptmp[6:18]

    coupled[...] = -div.reshape(6, 16, X)
    pscale[...] = jnp.zeros_like(pscale)
    for k in range(PZ):
        pscale[k, :12] = nodes(VT, k)
        coupled[k + 1, :12] = nodes(VT + 12, k) - div[16 * (k + 1) : 16 * (k + 1) + 12]
    par = parity("gz")
    for out, up in ((msg_even, 1 - par), (msg_odd, par)):
        parts = (
            coupled[2 + up] * pscale[1 + up], coupled[1 + 3 * up], coupled[5 * up], pscale[3 * up],
        )
        for j, part in enumerate(parts):
            out[12 * j : 12 * j + 12] = part[:12]


def pressure_step(coupled, pscale, got_even, got_odd, coefs, out, halo):
    even = parity("gz") == 0
    halo[...] = jnp.zeros_like(halo)
    for i in range(4):
        rows = slice(12 * i, 12 * i + 12)
        a, b = got_even[rows], got_odd[rows]
        halo[0, i, :12] = jnp.where(even, b, a)
        halo[1, i, :12] = jnp.where(even, a, b)
    b = [
        halo[0, 0], halo[0, 1] + coupled[0], halo[0, 2] + coupled[1], coupled[2],
        coupled[3], coupled[4] + halo[1, 2], coupled[5] + halo[1, 1], halo[1, 0],
    ]
    one = jnp.ones((16, X), F32)
    s = [one, halo[0, 3], pscale[0], pscale[1], pscale[2], pscale[3], halo[1, 3], one]
    inv, a1, g1, a2, g2 = (tall(coefs[5 + i], 16) for i in range(5))

    def operator(w, z):
        v = (1.0 / 6.0) * (w[z - 1] + w[z + 1]) + (2.0 / 3.0) * w[z]
        v = (1.0 / 6.0) * (pltpu.roll(v, 1, axis=0) + pltpu.roll(v, 15, axis=0)) + (2.0 / 3.0) * v
        v = (1.0 / 6.0) * (pltpu.roll(v, 1, axis=1) + pltpu.roll(v, X - 1, axis=1)) + (2.0 / 3.0) * v
        return s[z] * v

    d0 = [v * inv for v in b]
    w = [x * y for x, y in zip(s, d0)]
    r1, d1, w1 = [None] * 8, [None] * 8, [None] * 8
    for z in range(1, 7):
        r1[z] = b[z] - operator(w, z)
        d1[z] = a1 * d0[z] + g1 * r1[z]
        w1[z] = s[z] * d1[z]
    for z in range(2, 6):
        res = r1[z] - operator(w1, z)
        total = d0[z] + d1[z] + (a2 * d1[z] + g2 * res)
        total = pltpu.roll(pltpu.roll(total, 14, axis=0), X - 2, axis=1)
        out[z - 2] = total[:PY, :PX]


def per_device(rhs, prhs, visc, mass, pscale, vbounds, pbounds):
    plane, tile = (Y, X), (8, X)
    msg_even, msg_odd = call(
        pack_z,
        [(8, *plane)] * 2,
        scratch=[pltpu.VMEM((2, 4, *plane), F32), pltpu.SemaphoreType.DMA((10,))],
        hbm=(0, 1, 2),
    )(rhs, visc, mass)
    z_halos = swap_neighbours("gz", msg_even, msg_odd)
    (coefs,) = call(scalars, [(10, *tile)], smem=(0, 1))(vbounds, pbounds)
    (pt,) = call(pack_nodes, [(PZ, *tile)])(pscale, prhs)
    own, up, down = call(
        pack_y, [(PLANES, *plane), (padded(UP_ROWS + 8), X), (padded(DOWN_ROWS + 8), X)]
    )(rhs, visc, mass, *z_halos, pt)
    below, above = both_neighbours("gy", up, down)
    main, up, down = call(pack_x, [(TILES, *tile), (PACKED, *tile), (PACKED, *tile)])(
        own, pt, below, above
    )
    below, above = both_neighbours("gx", up, down)
    vel, coupled, scale, msg_even, msg_odd = call(
        velocity_step,
        [(3, Z, Y, X), (6, *plane), (PZ, *plane), (48, X), (48, X)],
        vmem=(0,),
        scratch=[
            pltpu.VMEM((TILES, 8, X), F32),
            pltpu.VMEM((2, 3, 2, ZW, 32, X), F32),
            pltpu.VMEM((3, 2, ZW, 32, X), F32),
            pltpu.VMEM((3, 2, ZW, 32, X), F32),
            pltpu.VMEM((3, 2, Z, 32, X), F32),
            pltpu.VMEM((2, 48, X), F32),
            pltpu.VMEM((3 * (Z + 2) * 32, 4 * X), jnp.bfloat16),
            pltpu.VMEM((3 * (Z + 2) * 32, 2 * X), F32),
            pltpu.VMEM((3, 32, X), F32),
            pltpu.VMEM((96, 4 * X), F32),
            pltpu.VMEM((24, X), F32),
        ],
    )(main, below, above, jnp.asarray(restriction()), jnp.asarray(smoothing()), coefs)
    z_halos = swap_neighbours("gz", msg_even, msg_odd)
    (pressure,) = call(
        pressure_step, [(PZ, PY, PX)], scratch=[pltpu.VMEM((2, 4, *plane), F32)]
    )(coupled, scale, *z_halos, coefs)
    return vel, pressure


def solution(mesh):
    block = P("gz", "gy", "gx")
    field = P(None, "gz", "gy", "gx")
    return jax.shard_map(
        per_device,
        mesh=mesh,
        in_specs=(field, block, block, block, block, P(), P()),
        out_specs=(field, block),
        check_vma=False,
    )
```

```python
import jax
import jax.numpy as jnp
import ml_dtypes
import numpy as np
from jax import lax
from jax.experimental import pallas as pl
from jax.experimental.pallas import tpu as pltpu
from jax.sharding import PartitionSpec as P


Z, Y, X = 8, 16, 128
PZ, PY, PX = 4, 8, 64
F32 = jnp.float32
VMEM_LIMIT = 16 * 2**20

ZW = Z + 4
PLANES = 4 * ZW + Z + 2
S0, M0 = 3 * ZW, 4 * ZW
VT = 4 * PLANES
TILES = VT + 24
PACKED = TILES // 16


def parity(axis):
    return lax.rem(lax.axis_index(axis), 2)


def swap_neighbours(axis, first, second):
    size = lax.axis_size(axis)
    even = [(i, i ^ 1) for i in range(size)]
    odd = [(i, ((i + 1) ^ 1) - 1) for i in range(1, size - 1)]
    inner = lax.ppermute(first, axis, even)
    outer = lax.ppermute(second, axis, odd)
    return inner, outer


def both_neighbours(axis, to_above, to_below):
    size = lax.axis_size(axis)
    up = [(i, i + 1) for i in range(size - 1)]
    down = [(i + 1, i) for i in range(size - 1)]
    from_below = lax.ppermute(to_above, axis, up)
    from_above = lax.ppermute(to_below, axis, down)
    return from_below, from_above


def call(body, outs, scratch=(), smem=(), hbm=(), vmem=(), hbm_out=()):
    def run(*args):
        space = {i: pltpu.SMEM for i in smem} | {i: pltpu.HBM for i in hbm}
        args = [
            pltpu.with_memory_space_constraint(x, pltpu.HBM) if i in hbm else x
            for i, x in enumerate(args)
        ]
        return pl.pallas_call(
            body,
            in_specs=[
                pl.BlockSpec(memory_space=space.get(i, pltpu.VMEM)) for i in range(len(args))
            ],
            out_specs=[
                pl.BlockSpec(memory_space=pltpu.HBM if i in hbm_out else pltpu.VMEM)
                for i in range(len(outs))
            ],
            out_shape=[
                pltpu.VMEM(o, F32) if i in vmem else jax.ShapeDtypeStruct(o, F32)
                for i, o in enumerate(outs)
            ],
            scratch_shapes=list(scratch),
            compiler_params=pltpu.CompilerParams(vmem_limit_bytes=VMEM_LIMIT),
        )(*args)

    return run


def pack_z(rhs, visc, mass, msg_even, msg_odd, far, sems):
    par = parity("gz")
    copies = []
    for i, (out, up) in enumerate(((msg_even, 1 - par), (msg_odd, par))):
        near, deep = 7 * up, 1 + 5 * up
        copies += [
            (rhs.at[:, near], out.at[3:6]),
            (visc.at[near], out.at[6]),
            (mass.at[near], out.at[7]),
            (rhs.at[:, deep], far.at[i, :3]),
            (visc.at[deep], far.at[i, 3]),
        ]
    copies = [pltpu.make_async_copy(*c, sems.at[i]) for i, c in enumerate(copies)]
    for c in copies:
        c.start()
    for c in copies:
        c.wait()
    for i, out in enumerate((msg_even, msg_odd)):
        for c in range(3):
            out[c] = far[i, c] * far[i, 3]


def scalars(vbounds, pbounds, coefs):
    for i, bounds in enumerate((vbounds, pbounds)):
        for j, value in enumerate(coefficients(bounds)):
            coefs[5 * i + j] = value


def z_halo(got_even, got_odd, i):
    even = parity("gz") == 0
    a, b = got_even[i], got_odd[i]
    return jnp.where(even, b, a), jnp.where(even, a, b)


def y_rows():
    out = []
    for p in range(PLANES):
        if p not in (S0, S0 + ZW - 1):
            out.append((p, 8, 7) if p // ZW == 1 else (p, 7, 6))
    return out


UP_ROWS = sum(r[1] for r in y_rows())
DOWN_ROWS = sum(r[2] for r in y_rows())


def padded(rows):
    return -(-rows // 8) * 8


def pack_nodes(pscale, prhs, pt):
    for k in range(PZ):
        pt[k] = jnp.concatenate([pscale[k], prhs[k]], axis=1)


def pack_y(rhs, visc, mass, got_even, got_odd, pt, own, up, down):
    for z in range(Z):
        for c in range(3):
            own[c * ZW + 2 + z] = rhs[c, z]
        own[S0 + 2 + z] = visc[z]
        own[M0 + 1 + z] = mass[z]
    for side, (deep, near) in enumerate(((0, 1), (ZW - 1, ZW - 2))):
        for c in range(3):
            own[c * ZW + deep] = z_halo(got_even, got_odd, c)[side]
            own[c * ZW + near] = z_halo(got_even, got_odd, 3 + c)[side]
        own[S0 + deep] = jnp.ones((Y, X), F32)
        own[S0 + near] = z_halo(got_even, got_odd, 6)[side]
        own[M0 + near - 1] = z_halo(got_even, got_odd, 7)[side]
    row = lax.broadcasted_iota(jnp.int32, (8, X), 0)
    at_up = at_down = 0
    for p, n_up, n_down in y_rows():
        if p // ZW == 1:
            z = p - ZW
            up[at_up : at_up + 8] = own[p, 8:] * jnp.where(row == 0, own[S0 + z, 8:], 1.0)
            part = own[p, :8] * jnp.where(row == 6, own[S0 + z, :8], 1.0)
            down[at_down : at_down + 7] = part[:7]
        else:
            up[at_up : at_up + n_up] = own[p, Y - n_up :]
            down[at_down : at_down + n_down] = own[p, :n_down]
        at_up, at_down = at_up + n_up, at_down + n_down
    for k in range(PZ):
        up[at_up + 2 * k : at_up + 2 * k + 2] = pt[k, 6:]
        down[at_down + 2 * k : at_down + 2 * k + 2] = pt[k, :2]


def pack_x(own, pt, below, above, main, up, down):
    at_up = at_down = 0
    rows = {r[0]: r[1:] for r in y_rows()}
    for p in range(PLANES):
        rest = jnp.full((8, X), 1.0 if S0 <= p < M0 else 0.0, F32)
        main[4 * p] = rest
        main[4 * p + 1] = own[p, :8]
        main[4 * p + 2] = own[p, 8:]
        main[4 * p + 3] = rest
        n_up, n_down = rows.get(p, (0, 0))
        if n_up:
            main[4 * p, 8 - n_up :] = below[at_up : at_up + n_up]
            main[4 * p + 3, :n_down] = above[at_down : at_down + n_down]
        at_up, at_down = at_up + n_up, at_down + n_down
    for k in range(PZ):
        for t in (0, 2):
            main[VT + 3 * k + t] = jnp.zeros((8, X), F32)
        main[VT + 3 * k, 6:] = below[at_up + 2 * k : at_up + 2 * k + 2]
        main[VT + 3 * k + 1] = pt[k]
        main[VT + 3 * k + 2, :2] = above[at_down + 2 * k : at_down + 2 * k + 2]
    lane = lanes()
    for k in range(PZ):
        for t in range(3):
            tile = main[VT + 3 * k + t]
            turned = pltpu.roll(tile, 64, axis=1)
            main[VT + 3 * k + t] = jnp.where(lane < 64, tile, turned)
            main[VT + 12 + 3 * k + t] = jnp.where(lane < 64, turned, tile)
    for i in range(PACKED):
        turned = main[16 * i : 16 * i + 16].reshape(X, X).T
        down[i] = turned[:8]
        up[i] = turned[X - 8 :]


def lanes():
    return lax.broadcasted_iota(jnp.int32, (8, X), 1)


def coefficients(bounds):
    low = jnp.full((8, X), bounds[0], F32)
    high = jnp.full((8, X), bounds[1], F32)
    centre = (high + low) / 2.0
    spread = (high - low) / 2.0
    sigma = centre / spread
    rho0 = 1.0 / sigma
    rho1 = 1.0 / (2.0 * sigma - rho0)
    rho2 = 1.0 / (2.0 * sigma - rho1)
    return 1.0 / centre, rho1 * rho0, 2.0 * rho1 / spread, rho2 * rho1, 2.0 * rho2 / spread


def tall(coef, rows):
    return jnp.concatenate([coef] * (rows // 8), axis=0)


def restriction():
    table = np.zeros((4, X, X), np.float32)
    for half in range(2):
        for l in range(X):
            x = l if half == 0 else (X + l if l < 8 else l - X)
            if half and 8 <= l < 120:
                continue
            for node in range(-2, PX + 2):
                o = x - 2 * node
                table[half, l, node + 2] = {-1: 0.25, 0: 0.5, 1: 0.25}.get(o, 0.0)
                table[2 + half, l, node + 2] = {-2: -0.125, -1: -0.25, 1: 0.25, 2: 0.125}.get(o, 0.0)
    return table.reshape(4 * X, X).astype(ml_dtypes.bfloat16)


SMOOTH_Z = {-1: (), 0: ((0, 0.5), (1, 0.25)), 4: ((7, 0.25),)}
DERIVE_Z = {
    -1: ((0, 0.125),),
    0: ((1, 0.25), (2, 0.125)),
    1: ((0, -0.125), (1, -0.25), (3, 0.25), (4, 0.125)),
    2: ((2, -0.125), (3, -0.25), (5, 0.25), (6, 0.125)),
    3: ((4, -0.125), (5, -0.25), (7, 0.25)),
    4: ((6, -0.125), (7, -0.25)),
}
for _k in (1, 2, 3):
    SMOOTH_Z[_k] = ((2 * _k - 1, 0.25), (2 * _k, 0.5), (2 * _k + 1, 0.25))


def smoothing():
    ring = np.eye(2 * X, dtype=np.float32)
    ring += 0.5 * (np.roll(ring, 1, axis=0) + np.roll(ring, -1, axis=0))
    return np.concatenate([ring[:X], ring[:X], ring[X:], ring[X:]]).astype(ml_dtypes.bfloat16)


def split(value, parts):
    out = []
    for _ in range(parts):
        out.append(value.astype(jnp.bfloat16))
        value = value - out[-1].astype(F32)
    return out


def dot(a, b):
    return lax.dot_general(a, b, (((1,), (0,)), ((), ())), preferred_element_type=F32)


def planes(ref, p):
    return ref[pl.ds(4 * p, 4)].reshape(32, X)


def loop(start, count, body):
    def step(z, _):
        body(z)
        return 0

    lax.fori_loop(start, start + count, step, 0)


def weigh(src, w, c):
    def body(z):
        w[z] = planes(src, S0 + z) * planes(src, c * ZW + z)

    loop(0, ZW, body)


def sum_rows(w, t, lhs, first_row, col, z0, count):
    def body(z):
        v = w[z] + 0.5 * (w[z - 1] + w[z + 1])
        t[8:40] = v
        v = v + 0.5 * (t[7:39] + t[9:41])
        at = pl.ds(first_row + (z - z0) * 32, 32)
        for part, value in enumerate(split(v, 2)):
            lhs[at, col + part * X : col + (part + 1) * X] = value

    loop(z0, count, body)


def first_sums(main, ring, sums, w, t, lhs):
    t[...] = jnp.zeros_like(t)
    for c in range(3):
        weigh(main, w, c)
        sum_rows(w, t, lhs, c * (Z + 2) * 32, 0, 1, Z + 2)
    sums[...] = dot(lhs[...], ring[: 2 * X])


def velocity_step(
    main, from_below, from_above, table, ring, sums, coefs, vel, coupled, pscale, msg_even, msg_odd,
    halo, w, d, r, u, t, lhs, s, g, q, ptmp,
):
    lane = lanes()
    gap = jnp.zeros((X - 16, X), F32)
    for i in range(PACKED):
        strips = jnp.concatenate([from_above[i], gap, from_below[i]], axis=0)
        halo[16 * i : 16 * i + 16] = strips.T.reshape(16, 8, X)

    inv, a1, g1, a2, g2 = (tall(coefs[i], 32) for i in range(5))
    t[...] = jnp.zeros_like(t)
    both = (main, halo)

    for c in range(3):
        weigh(halo, w.at[c, 1], c)
        sum_rows(w.at[c, 1], t.at[1], lhs, c * (Z + 2) * 32, 2 * X, 1, Z + 2)
    s[...] = dot(lhs[:, 2 * X :], ring[2 * X :])

    for c in range(3):
        def sweep1(z):
            at = pl.ds((c * (Z + 2) + z - 1) * 32, 32)
            for h, src in enumerate(both):
                cols = slice(h * X, (h + 1) * X)
                b = planes(src, c * ZW + z)
                visc = planes(src, S0 + z)
                d0 = b * inv
                lap = 16.0 * (visc * d0) - (2.0 * inv) * (sums[at, cols] + s[at, cols])
                res = b - (visc * lap + planes(src, M0 + z - 1) * d0)
                d1 = a1 * d0 + g1 * res
                r[c, h, z] = res
                d[c, h, z] = d1
                w[c, h, z] = visc * d1

        loop(1, Z + 2, sweep1)

    for c in range(3):
        for h in range(2):
            sum_rows(w.at[c, h], t.at[h], lhs, c * Z * 32, 2 * h * X, 2, Z)
    total = 3 * Z * 32
    s[:total] = dot(lhs[:total], ring[...])

    for c in range(3):
        def sweep2(z):
            at = pl.ds((c * Z + z - 2) * 32, 32)
            for h, src in enumerate(both):
                d1 = d[c, h, z]
                lap = 16.0 * w[c, h, z] - 2.0 * s[at, h * X : (h + 1) * X]
                res = r[c, h, z] - (planes(src, S0 + z) * lap + planes(src, M0 + z - 1) * d1)
                value = planes(src, c * ZW + z) * inv + d1 + (a2 * d1 + g2 * res)
                u[c, h, z - 2] = value
                if h == 0:
                    vel[c, z - 2] = value[8:24]

        loop(2, Z, sweep2)

    q[...] = jnp.zeros_like(q)
    for node in range(-1, 5):
        rows = slice(16 * (node + 1), 16 * (node + 1) + 12)

        def along_z(c, h, weights):
            acc = None
            for z, f in weights:
                term = f * u[c, h, z]
                acc = term if acc is None else acc + term
            return acc

        def at(k, start):
            return g[k, pl.ds(start, 12, stride=2), :]

        for h in range(2):
            cols = slice(X * h, X * (h + 1))
            g[2] = along_z(2, h, DERIVE_Z[node])
            total = 0.25 * (at(2, 3) + at(2, 5)) + 0.5 * at(2, 4)
            if SMOOTH_Z[node]:
                g[0] = along_z(0, h, SMOOTH_Z[node])
                g[1] = along_z(1, h, SMOOTH_Z[node])
                total = total + 0.25 * (at(1, 5) - at(1, 3)) + 0.125 * (at(1, 6) - at(1, 2))
                q[rows, 2 * X + X * h : 3 * X + X * h] = 0.25 * (at(0, 3) + at(0, 5)) + 0.5 * at(0, 4)
            q[rows, cols] = total

    div = sum(dot(v, table[...]) for v in reversed(split(q[...], 3)))

    def nodes(base, k):
        for i in range(3):
            own = pltpu.roll(main[base + 3 * k + i], 2, axis=1)
            side = halo[base + 3 * k + i]
            left = pltpu.roll(side, 2, axis=1)
            right = pltpu.roll(side, 66, axis=1)
            value = jnp.where(lane < 66, own, jnp.where(lane < 68, right, 0.0))
            ptmp[8 * i : 8 * i + 8] = jnp.where(lane < 2, left, value)
        return ptmp[6:18]

    coupled[...] = -div.reshape(6, 16, X)
    pscale[...] = jnp.zeros_like(pscale)
    for k in range(PZ):
        pscale[k, :12] = nodes(VT, k)
        coupled[k + 1, :12] = nodes(VT + 12, k) - div[16 * (k + 1) : 16 * (k + 1) + 12]
    par = parity("gz")
    for out, up in ((msg_even, 1 - par), (msg_odd, par)):
        parts = (
            coupled[2 + up] * pscale[1 + up], coupled[1 + 3 * up], coupled[5 * up], pscale[3 * up],
        )
        for j, part in enumerate(parts):
            out[12 * j : 12 * j + 12] = part[:12]


def pressure_step(coupled, pscale, got_even, got_odd, coefs, vel, vel_out, out, halo, sem):
    write = pltpu.make_async_copy(vel, vel_out, sem)
    write.start()
    even = parity("gz") == 0
    halo[...] = jnp.zeros_like(halo)
    for i in range(4):
        rows = slice(12 * i, 12 * i + 12)
        a, b = got_even[rows], got_odd[rows]
        halo[0, i, :12] = jnp.where(even, b, a)
        halo[1, i, :12] = jnp.where(even, a, b)
    b = [
        halo[0, 0], halo[0, 1] + coupled[0], halo[0, 2] + coupled[1], coupled[2],
        coupled[3], coupled[4] + halo[1, 2], coupled[5] + halo[1, 1], halo[1, 0],
    ]
    one = jnp.ones((16, X), F32)
    s = [one, halo[0, 3], pscale[0], pscale[1], pscale[2], pscale[3], halo[1, 3], one]
    inv, a1, g1, a2, g2 = (tall(coefs[5 + i], 16) for i in range(5))

    def operator(w, z):
        v = (1.0 / 6.0) * (w[z - 1] + w[z + 1]) + (2.0 / 3.0) * w[z]
        v = (1.0 / 6.0) * (pltpu.roll(v, 1, axis=0) + pltpu.roll(v, 15, axis=0)) + (2.0 / 3.0) * v
        v = (1.0 / 6.0) * (pltpu.roll(v, 1, axis=1) + pltpu.roll(v, X - 1, axis=1)) + (2.0 / 3.0) * v
        return s[z] * v

    d0 = [v * inv for v in b]
    w = [x * y for x, y in zip(s, d0)]
    r1, d1, w1 = [None] * 8, [None] * 8, [None] * 8
    for z in range(1, 7):
        r1[z] = b[z] - operator(w, z)
        d1[z] = a1 * d0[z] + g1 * r1[z]
        w1[z] = s[z] * d1[z]
    for z in range(2, 6):
        res = r1[z] - operator(w1, z)
        total = d0[z] + d1[z] + (a2 * d1[z] + g2 * res)
        total = pltpu.roll(pltpu.roll(total, 14, axis=0), X - 2, axis=1)
        out[z - 2] = total[:PY, :PX]
    write.wait()


def per_device(rhs, prhs, visc, mass, pscale, vbounds, pbounds):
    plane, tile = (Y, X), (8, X)
    msg_even, msg_odd = call(
        pack_z,
        [(8, *plane)] * 2,
        scratch=[pltpu.VMEM((2, 4, *plane), F32), pltpu.SemaphoreType.DMA((10,))],
        hbm=(0, 1, 2),
    )(rhs, visc, mass)
    z_halos = swap_neighbours("gz", msg_even, msg_odd)
    (coefs,) = call(scalars, [(10, *tile)], smem=(0, 1))(vbounds, pbounds)
    (pt,) = call(pack_nodes, [(PZ, *tile)])(pscale, prhs)
    own, up, down = call(
        pack_y, [(PLANES, *plane), (padded(UP_ROWS + 8), X), (padded(DOWN_ROWS + 8), X)]
    )(rhs, visc, mass, *z_halos, pt)
    below, above = both_neighbours("gy", up, down)
    main, up, down = call(pack_x, [(TILES, *tile), (PACKED, *tile), (PACKED, *tile)])(
        own, pt, below, above
    )
    below, above = both_neighbours("gx", up, down)
    ring = jnp.asarray(smoothing())
    rows = 3 * (Z + 2) * 32
    (sums,) = call(
        first_sums,
        [(rows, 2 * X)],
        scratch=[
            pltpu.VMEM((ZW, 32, X), F32),
            pltpu.VMEM((48, X), F32),
            pltpu.VMEM((rows, 2 * X), jnp.bfloat16),
        ],
    )(main, ring)
    vel, coupled, scale, msg_even, msg_odd = call(
        velocity_step,
        [(3, Z, Y, X), (6, *plane), (PZ, *plane), (48, X), (48, X)],
        vmem=(0,),
        scratch=[
            pltpu.VMEM((TILES, 8, X), F32),
            pltpu.VMEM((3, 2, ZW, 32, X), F32),
            pltpu.VMEM((3, 2, ZW, 32, X), F32),
            pltpu.VMEM((3, 2, ZW, 32, X), F32),
            pltpu.VMEM((3, 2, Z, 32, X), F32),
            pltpu.VMEM((2, 48, X), F32),
            pltpu.VMEM((rows, 4 * X), jnp.bfloat16),
            pltpu.VMEM((rows, 2 * X), F32),
            pltpu.VMEM((3, 32, X), F32),
            pltpu.VMEM((96, 4 * X), F32),
            pltpu.VMEM((24, X), F32),
        ],
    )(main, below, above, jnp.asarray(restriction()), ring, sums, coefs)
    z_halos = swap_neighbours("gz", msg_even, msg_odd)
    return call(
        pressure_step,
        [(3, Z, Y, X), (PZ, PY, PX)],
        scratch=[pltpu.VMEM((2, 4, *plane), F32), pltpu.SemaphoreType.DMA],
        hbm_out=(0,),
    )(coupled, scale, *z_halos, coefs, vel)


def solution(mesh):
    block = P("gz", "gy", "gx")
    field = P(None, "gz", "gy", "gx")
    return jax.shard_map(
        per_device,
        mesh=mesh,
        in_specs=(field, block, block, block, block, P(), P()),
        out_specs=(field, block),
        check_vma=False,
    )
```

```python
import jax
import jax.numpy as jnp
import ml_dtypes
import numpy as np
from jax import lax
from jax.experimental import pallas as pl
from jax.experimental.pallas import tpu as pltpu
from jax.sharding import PartitionSpec as P


Z, Y, X = 8, 16, 128
PZ, PY, PX = 4, 8, 64
F32 = jnp.float32
VMEM_LIMIT = 16 * 2**20

ZW = Z + 4
PLANES = 4 * ZW + Z + 2
S0, M0 = 3 * ZW, 4 * ZW
VT = 4 * PLANES
TILES = VT + 24
PACKED = TILES // 16


def parity(axis):
    return lax.rem(lax.axis_index(axis), 2)


def swap_neighbours(axis, first, second):
    size = lax.axis_size(axis)
    even = [(i, i ^ 1) for i in range(size)]
    odd = [(i, ((i + 1) ^ 1) - 1) for i in range(1, size - 1)]
    inner = lax.ppermute(first, axis, even)
    outer = lax.ppermute(second, axis, odd)
    return inner, outer


def both_neighbours(axis, to_above, to_below):
    size = lax.axis_size(axis)
    up = [(i, i + 1) for i in range(size - 1)]
    down = [(i + 1, i) for i in range(size - 1)]
    from_below = lax.ppermute(to_above, axis, up)
    from_above = lax.ppermute(to_below, axis, down)
    return from_below, from_above


def call(body, outs, scratch=(), smem=(), hbm=(), vmem=()):
    def run(*args):
        space = {i: pltpu.SMEM for i in smem} | {i: pltpu.HBM for i in hbm}
        args = [
            pltpu.with_memory_space_constraint(x, pltpu.HBM) if i in hbm else x
            for i, x in enumerate(args)
        ]
        return pl.pallas_call(
            body,
            in_specs=[
                pl.BlockSpec(memory_space=space.get(i, pltpu.VMEM)) for i in range(len(args))
            ],
            out_specs=[pl.BlockSpec(memory_space=pltpu.VMEM) for _ in outs],
            out_shape=[
                pltpu.VMEM(o, F32) if i in vmem else jax.ShapeDtypeStruct(o, F32)
                for i, o in enumerate(outs)
            ],
            scratch_shapes=list(scratch),
            compiler_params=pltpu.CompilerParams(vmem_limit_bytes=VMEM_LIMIT),
        )(*args)

    return run


def pack_z(rhs, visc, mass, msg_even, msg_odd, far, sems):
    par = parity("gz")
    copies = []
    for i, (out, up) in enumerate(((msg_even, 1 - par), (msg_odd, par))):
        near, deep = 7 * up, 1 + 5 * up
        copies += [
            (rhs.at[:, near], out.at[3:6]),
            (visc.at[near], out.at[6]),
            (mass.at[near], out.at[7]),
            (rhs.at[:, deep], far.at[i, :3]),
            (visc.at[deep], far.at[i, 3]),
        ]
    copies = [pltpu.make_async_copy(*c, sems.at[i]) for i, c in enumerate(copies)]
    for c in copies:
        c.start()
    for c in copies:
        c.wait()
    for i, out in enumerate((msg_even, msg_odd)):
        for c in range(3):
            out[c] = far[i, c] * far[i, 3]


def scalars(vbounds, pbounds, coefs):
    for i, bounds in enumerate((vbounds, pbounds)):
        for j, value in enumerate(coefficients(bounds)):
            coefs[5 * i + j] = value


def z_halo(got_even, got_odd, i):
    even = parity("gz") == 0
    a, b = got_even[i], got_odd[i]
    return jnp.where(even, b, a), jnp.where(even, a, b)


def y_rows():
    out = []
    for p in range(PLANES):
        if p not in (S0, S0 + ZW - 1):
            out.append((p, 8, 7) if p // ZW == 1 else (p, 7, 6))
    return out


UP_ROWS = sum(r[1] for r in y_rows())
DOWN_ROWS = sum(r[2] for r in y_rows())


def padded(rows):
    return -(-rows // 8) * 8


def pack_nodes(pscale, prhs, pt):
    for k in range(PZ):
        pt[k] = jnp.concatenate([pscale[k], prhs[k]], axis=1)


def pack_y(rhs, visc, mass, got_even, got_odd, pt, own, up, down):
    for z in range(Z):
        for c in range(3):
            own[c * ZW + 2 + z] = rhs[c, z]
        own[S0 + 2 + z] = visc[z]
        own[M0 + 1 + z] = mass[z]
    for side, (deep, near) in enumerate(((0, 1), (ZW - 1, ZW - 2))):
        for c in range(3):
            own[c * ZW + deep] = z_halo(got_even, got_odd, c)[side]
            own[c * ZW + near] = z_halo(got_even, got_odd, 3 + c)[side]
        own[S0 + deep] = jnp.ones((Y, X), F32)
        own[S0 + near] = z_halo(got_even, got_odd, 6)[side]
        own[M0 + near - 1] = z_halo(got_even, got_odd, 7)[side]
    row = lax.broadcasted_iota(jnp.int32, (8, X), 0)
    at_up = at_down = 0
    for p, n_up, n_down in y_rows():
        if p // ZW == 1:
            z = p - ZW
            up[at_up : at_up + 8] = own[p, 8:] * jnp.where(row == 0, own[S0 + z, 8:], 1.0)
            part = own[p, :8] * jnp.where(row == 6, own[S0 + z, :8], 1.0)
            down[at_down : at_down + 7] = part[:7]
        else:
            up[at_up : at_up + n_up] = own[p, Y - n_up :]
            down[at_down : at_down + n_down] = own[p, :n_down]
        at_up, at_down = at_up + n_up, at_down + n_down
    for k in range(PZ):
        up[at_up + 2 * k : at_up + 2 * k + 2] = pt[k, 6:]
        down[at_down + 2 * k : at_down + 2 * k + 2] = pt[k, :2]


def pack_x(own, pt, below, above, main, up, down):
    at_up = at_down = 0
    rows = {r[0]: r[1:] for r in y_rows()}
    for p in range(PLANES):
        rest = jnp.full((8, X), 1.0 if S0 <= p < M0 else 0.0, F32)
        main[4 * p] = rest
        main[4 * p + 1] = own[p, :8]
        main[4 * p + 2] = own[p, 8:]
        main[4 * p + 3] = rest
        n_up, n_down = rows.get(p, (0, 0))
        if n_up:
            main[4 * p, 8 - n_up :] = below[at_up : at_up + n_up]
            main[4 * p + 3, :n_down] = above[at_down : at_down + n_down]
        at_up, at_down = at_up + n_up, at_down + n_down
    for k in range(PZ):
        for t in (0, 2):
            main[VT + 3 * k + t] = jnp.zeros((8, X), F32)
        main[VT + 3 * k, 6:] = below[at_up + 2 * k : at_up + 2 * k + 2]
        main[VT + 3 * k + 1] = pt[k]
        main[VT + 3 * k + 2, :2] = above[at_down + 2 * k : at_down + 2 * k + 2]
    lane = lanes()
    for k in range(PZ):
        for t in range(3):
            tile = main[VT + 3 * k + t]
            turned = pltpu.roll(tile, 64, axis=1)
            main[VT + 3 * k + t] = jnp.where(lane < 64, tile, turned)
            main[VT + 12 + 3 * k + t] = jnp.where(lane < 64, turned, tile)
    for i in range(PACKED):
        turned = main[16 * i : 16 * i + 16].reshape(X, X).T
        down[i] = turned[:8]
        up[i] = turned[X - 8 :]


def lanes():
    return lax.broadcasted_iota(jnp.int32, (8, X), 1)


def coefficients(bounds):
    low = jnp.full((8, X), bounds[0], F32)
    high = jnp.full((8, X), bounds[1], F32)
    centre = (high + low) / 2.0
    spread = (high - low) / 2.0
    sigma = centre / spread
    rho0 = 1.0 / sigma
    rho1 = 1.0 / (2.0 * sigma - rho0)
    rho2 = 1.0 / (2.0 * sigma - rho1)
    return 1.0 / centre, rho1 * rho0, 2.0 * rho1 / spread, rho2 * rho1, 2.0 * rho2 / spread


def tall(coef, rows):
    return jnp.concatenate([coef] * (rows // 8), axis=0)


def restriction():
    table = np.zeros((4, X, X), np.float32)
    for half in range(2):
        for l in range(X):
            x = l if half == 0 else (X + l if l < 8 else l - X)
            if half and 8 <= l < 120:
                continue
            for node in range(-2, PX + 2):
                o = x - 2 * node
                table[half, l, node + 2] = {-1: 0.25, 0: 0.5, 1: 0.25}.get(o, 0.0)
                table[2 + half, l, node + 2] = {-2: -0.125, -1: -0.25, 1: 0.25, 2: 0.125}.get(o, 0.0)
    return table.reshape(4 * X, X).astype(ml_dtypes.bfloat16)


SMOOTH_Z = {-1: (), 0: ((0, 0.5), (1, 0.25)), 4: ((7, 0.25),)}
DERIVE_Z = {
    -1: ((0, 0.125),),
    0: ((1, 0.25), (2, 0.125)),
    1: ((0, -0.125), (1, -0.25), (3, 0.25), (4, 0.125)),
    2: ((2, -0.125), (3, -0.25), (5, 0.25), (6, 0.125)),
    3: ((4, -0.125), (5, -0.25), (7, 0.25)),
    4: ((6, -0.125), (7, -0.25)),
}
for _k in (1, 2, 3):
    SMOOTH_Z[_k] = ((2 * _k - 1, 0.25), (2 * _k, 0.5), (2 * _k + 1, 0.25))


def smoothing():
    ring = np.eye(2 * X, dtype=np.float32)
    ring += 0.5 * (np.roll(ring, 1, axis=0) + np.roll(ring, -1, axis=0))
    return np.concatenate([ring[:X], ring[:X], ring[X:], ring[X:]]).astype(ml_dtypes.bfloat16)


def split(value, parts):
    out = []
    for _ in range(parts):
        out.append(value.astype(jnp.bfloat16))
        value = value - out[-1].astype(F32)
    return out


def dot(a, b):
    return lax.dot_general(a, b, (((1,), (0,)), ((), ())), preferred_element_type=F32)


def planes(ref, p):
    return ref[pl.ds(4 * p, 4)].reshape(32, X)


def loop(start, count, body, each=1):
    def step(i, _):
        body([start + each * i + j for j in range(each)])
        return 0

    lax.fori_loop(0, count // each, step, 0)


def weigh(src, w):
    def body(zs):
        for z in zs:
            visc = planes(src, S0 + z)
            for c in range(3):
                w[c, z] = visc * planes(src, c * ZW + z)

    loop(0, ZW, body, 3)


def sum_rows(chains, t, lhs, z0, count):
    def body(zs):
        work = [(z, *chain) for z in zs for chain in chains]
        first = []
        for i, (z, c, w, col) in enumerate(work):
            v = w[z] + 0.5 * (w[z - 1] + w[z + 1])
            t[i, 8:40] = v
            first.append(v)
        for i, (z, c, w, col) in enumerate(work):
            v = first[i] + 0.5 * (t[i, 7:39] + t[i, 9:41])
            at = pl.ds((c * count + z - z0) * 32, 32)
            for part, value in enumerate(split(v, 2)):
                lhs[at, col + part * X : col + (part + 1) * X] = value

    loop(z0, count, body, 6 // len(chains))


def first_sums(main, ring, sums, w, t, lhs):
    t[...] = jnp.zeros_like(t)
    weigh(main, w)
    sum_rows([(c, w.at[c], 0) for c in range(3)], t, lhs, 1, Z + 2)
    sums[...] = dot(lhs[...], ring[: 2 * X])


def velocity_step(
    main, from_below, from_above, table, ring, sums, coefs, vel, coupled, pscale, msg_even, msg_odd,
    halo, w, d, r, u, t, lhs, s, g, q, ptmp,
):
    lane = lanes()
    gap = jnp.zeros((X - 16, X), F32)
    for i in range(PACKED):
        strips = jnp.concatenate([from_above[i], gap, from_below[i]], axis=0)
        halo[16 * i : 16 * i + 16] = strips.T.reshape(16, 8, X)

    inv, a1, g1, a2, g2 = (tall(coefs[i], 32) for i in range(5))
    t[...] = jnp.zeros_like(t)
    both = (main, halo)

    weigh(halo, w.at[1])
    sum_rows([(c, w.at[1, c], 2 * X) for c in range(3)], t, lhs, 1, Z + 2)
    s[...] = dot(lhs[:, 2 * X :], ring[2 * X :])

    def sweep1(zs):
        (z,) = zs
        for h, src in enumerate(both):
            visc, mass = planes(src, S0 + z), planes(src, M0 + z - 1)
            cols = slice(h * X, (h + 1) * X)
            for c in range(3):
                at = pl.ds((c * (Z + 2) + z - 1) * 32, 32)
                b = planes(src, c * ZW + z)
                d0 = b * inv
                lap = 16.0 * (visc * d0) - (2.0 * inv) * (sums[at, cols] + s[at, cols])
                res = b - (visc * lap + mass * d0)
                d1 = a1 * d0 + g1 * res
                r[h, c, z] = res
                d[h, c, z] = d1
                w[h, c, z] = visc * d1

    loop(1, Z + 2, sweep1)

    sum_rows([(c, w.at[h, c], 2 * h * X) for h in range(2) for c in range(3)], t, lhs, 2, Z)
    total = 3 * Z * 32
    s[:total] = dot(lhs[:total], ring[...])

    def sweep2(zs):
        (z,) = zs
        for h, src in enumerate(both):
            visc, mass = planes(src, S0 + z), planes(src, M0 + z - 1)
            for c in range(3):
                at = pl.ds((c * Z + z - 2) * 32, 32)
                d1 = d[h, c, z]
                lap = 16.0 * w[h, c, z] - 2.0 * s[at, h * X : (h + 1) * X]
                res = r[h, c, z] - (visc * lap + mass * d1)
                value = planes(src, c * ZW + z) * inv + d1 + (a2 * d1 + g2 * res)
                u[c, h, z - 2] = value
                if h == 0:
                    vel[c, z - 2] = value[8:24]

    loop(2, Z, sweep2)

    q[...] = jnp.zeros_like(q)
    for node in range(-1, 5):
        rows = slice(16 * (node + 1), 16 * (node + 1) + 12)

        def along_z(c, h, weights):
            acc = None
            for z, f in weights:
                term = f * u[c, h, z]
                acc = term if acc is None else acc + term
            return acc

        def at(k, start):
            return g[k, pl.ds(start, 12, stride=2), :]

        for h in range(2):
            cols = slice(X * h, X * (h + 1))
            g[2] = along_z(2, h, DERIVE_Z[node])
            total = 0.25 * (at(2, 3) + at(2, 5)) + 0.5 * at(2, 4)
            if SMOOTH_Z[node]:
                g[0] = along_z(0, h, SMOOTH_Z[node])
                g[1] = along_z(1, h, SMOOTH_Z[node])
                total = total + 0.25 * (at(1, 5) - at(1, 3)) + 0.125 * (at(1, 6) - at(1, 2))
                q[rows, 2 * X + X * h : 3 * X + X * h] = 0.25 * (at(0, 3) + at(0, 5)) + 0.5 * at(0, 4)
            q[rows, cols] = total

    div = sum(dot(v, table[...]) for v in reversed(split(q[...], 3)))

    def nodes(base, k):
        for i in range(3):
            own = pltpu.roll(main[base + 3 * k + i], 2, axis=1)
            side = halo[base + 3 * k + i]
            left = pltpu.roll(side, 2, axis=1)
            right = pltpu.roll(side, 66, axis=1)
            value = jnp.where(lane < 66, own, jnp.where(lane < 68, right, 0.0))
            ptmp[8 * i : 8 * i + 8] = jnp.where(lane < 2, left, value)
        return ptmp[6:18]

    coupled[...] = -div.reshape(6, 16, X)
    pscale[...] = jnp.zeros_like(pscale)
    for k in range(PZ):
        pscale[k, :12] = nodes(VT, k)
        coupled[k + 1, :12] = nodes(VT + 12, k) - div[16 * (k + 1) : 16 * (k + 1) + 12]
    par = parity("gz")
    for out, up in ((msg_even, 1 - par), (msg_odd, par)):
        parts = (
            coupled[2 + up] * pscale[1 + up], coupled[1 + 3 * up], coupled[5 * up], pscale[3 * up],
        )
        for j, part in enumerate(parts):
            out[12 * j : 12 * j + 12] = part[:12]


def pressure_step(coupled, pscale, got_even, got_odd, coefs, out, halo):
    even = parity("gz") == 0
    halo[...] = jnp.zeros_like(halo)
    for i in range(4):
        rows = slice(12 * i, 12 * i + 12)
        a, b = got_even[rows], got_odd[rows]
        halo[0, i, :12] = jnp.where(even, b, a)
        halo[1, i, :12] = jnp.where(even, a, b)
    b = [
        halo[0, 0], halo[0, 1] + coupled[0], halo[0, 2] + coupled[1], coupled[2],
        coupled[3], coupled[4] + halo[1, 2], coupled[5] + halo[1, 1], halo[1, 0],
    ]
    one = jnp.ones((16, X), F32)
    s = [one, halo[0, 3], pscale[0], pscale[1], pscale[2], pscale[3], halo[1, 3], one]
    inv, a1, g1, a2, g2 = (tall(coefs[5 + i], 16) for i in range(5))

    def operator(w, z):
        v = (1.0 / 6.0) * (w[z - 1] + w[z + 1]) + (2.0 / 3.0) * w[z]
        v = (1.0 / 6.0) * (pltpu.roll(v, 1, axis=0) + pltpu.roll(v, 15, axis=0)) + (2.0 / 3.0) * v
        v = (1.0 / 6.0) * (pltpu.roll(v, 1, axis=1) + pltpu.roll(v, X - 1, axis=1)) + (2.0 / 3.0) * v
        return s[z] * v

    d0 = [v * inv for v in b]
    w = [x * y for x, y in zip(s, d0)]
    r1, d1, w1 = [None] * 8, [None] * 8, [None] * 8
    for z in range(1, 7):
        r1[z] = b[z] - operator(w, z)
        d1[z] = a1 * d0[z] + g1 * r1[z]
        w1[z] = s[z] * d1[z]
    for z in range(2, 6):
        res = r1[z] - operator(w1, z)
        total = d0[z] + d1[z] + (a2 * d1[z] + g2 * res)
        total = pltpu.roll(pltpu.roll(total, 14, axis=0), X - 2, axis=1)
        out[z - 2] = total[:PY, :PX]


def per_device(rhs, prhs, visc, mass, pscale, vbounds, pbounds):
    plane, tile = (Y, X), (8, X)
    msg_even, msg_odd = call(
        pack_z,
        [(8, *plane)] * 2,
        scratch=[pltpu.VMEM((2, 4, *plane), F32), pltpu.SemaphoreType.DMA((10,))],
        hbm=(0, 1, 2),
    )(rhs, visc, mass)
    z_halos = swap_neighbours("gz", msg_even, msg_odd)
    (coefs,) = call(scalars, [(10, *tile)], smem=(0, 1))(vbounds, pbounds)
    (pt,) = call(pack_nodes, [(PZ, *tile)])(pscale, prhs)
    own, up, down = call(
        pack_y, [(PLANES, *plane), (padded(UP_ROWS + 8), X), (padded(DOWN_ROWS + 8), X)]
    )(rhs, visc, mass, *z_halos, pt)
    below, above = both_neighbours("gy", up, down)
    main, up, down = call(pack_x, [(TILES, *tile), (PACKED, *tile), (PACKED, *tile)])(
        own, pt, below, above
    )
    below, above = both_neighbours("gx", up, down)
    ring = jnp.asarray(smoothing())
    rows = 3 * (Z + 2) * 32
    (sums,) = call(
        first_sums,
        [(rows, 2 * X)],
        scratch=[
            pltpu.VMEM((3, ZW, 32, X), F32),
            pltpu.VMEM((6, 48, X), F32),
            pltpu.VMEM((rows, 2 * X), jnp.bfloat16),
        ],
    )(main, ring)
    vel, coupled, scale, msg_even, msg_odd = call(
        velocity_step,
        [(3, Z, Y, X), (6, *plane), (PZ, *plane), (48, X), (48, X)],
        vmem=(0,),
        scratch=[
            pltpu.VMEM((TILES, 8, X), F32),
            pltpu.VMEM((2, 3, ZW, 32, X), F32),
            pltpu.VMEM((2, 3, ZW, 32, X), F32),
            pltpu.VMEM((2, 3, ZW, 32, X), F32),
            pltpu.VMEM((3, 2, Z, 32, X), F32),
            pltpu.VMEM((6, 48, X), F32),
            pltpu.VMEM((rows, 4 * X), jnp.bfloat16),
            pltpu.VMEM((rows, 2 * X), F32),
            pltpu.VMEM((3, 32, X), F32),
            pltpu.VMEM((96, 4 * X), F32),
            pltpu.VMEM((24, X), F32),
        ],
    )(main, below, above, jnp.asarray(restriction()), ring, sums, coefs)
    z_halos = swap_neighbours("gz", msg_even, msg_odd)
    (pressure,) = call(
        pressure_step, [(PZ, PY, PX)], scratch=[pltpu.VMEM((2, 4, *plane), F32)]
    )(coupled, scale, *z_halos, coefs)
    return vel, pressure


def solution(mesh):
    block = P("gz", "gy", "gx")
    field = P(None, "gz", "gy", "gx")
    return jax.shard_map(
        per_device,
        mesh=mesh,
        in_specs=(field, block, block, block, block, P(), P()),
        out_specs=(field, block),
        check_vma=False,
    )
```

```python
import jax
import jax.numpy as jnp
import ml_dtypes
import numpy as np
from jax import lax
from jax.experimental import pallas as pl
from jax.experimental.pallas import tpu as pltpu
from jax.sharding import PartitionSpec as P


Z, Y, X = 8, 16, 128
PZ, PY, PX = 4, 8, 64
F32 = jnp.float32
VMEM_LIMIT = 16 * 2**20

ZW = Z + 4
PLANES = 4 * ZW + Z + 2
S0, M0 = 3 * ZW, 4 * ZW
VT = 4 * PLANES
TILES = VT + 24
PACKED = TILES // 16


def parity(axis):
    return lax.rem(lax.axis_index(axis), 2)


def swap_neighbours(axis, first, second):
    size = lax.axis_size(axis)
    even = [(i, i ^ 1) for i in range(size)]
    odd = [(i, ((i + 1) ^ 1) - 1) for i in range(1, size - 1)]
    inner = lax.ppermute(first, axis, even)
    outer = lax.ppermute(second, axis, odd)
    return inner, outer


def both_neighbours(axis, to_above, to_below):
    size = lax.axis_size(axis)
    up = [(i, i + 1) for i in range(size - 1)]
    down = [(i + 1, i) for i in range(size - 1)]
    from_below = lax.ppermute(to_above, axis, up)
    from_above = lax.ppermute(to_below, axis, down)
    return from_below, from_above


def call(body, outs, scratch=(), smem=(), hbm=(), vmem=()):
    def run(*args):
        space = {i: pltpu.SMEM for i in smem} | {i: pltpu.HBM for i in hbm}
        args = [
            pltpu.with_memory_space_constraint(x, pltpu.HBM) if i in hbm else x
            for i, x in enumerate(args)
        ]
        return pl.pallas_call(
            body,
            in_specs=[
                pl.BlockSpec(memory_space=space.get(i, pltpu.VMEM)) for i in range(len(args))
            ],
            out_specs=[pl.BlockSpec(memory_space=pltpu.VMEM) for _ in outs],
            out_shape=[
                pltpu.VMEM(o, F32) if i in vmem else jax.ShapeDtypeStruct(o, F32)
                for i, o in enumerate(outs)
            ],
            scratch_shapes=list(scratch),
            compiler_params=pltpu.CompilerParams(vmem_limit_bytes=VMEM_LIMIT),
        )(*args)

    return run


def pack_z(rhs, visc, mass, msg_even, msg_odd, far, sems):
    par = parity("gz")
    copies = []
    for i, (out, up) in enumerate(((msg_even, 1 - par), (msg_odd, par))):
        near, deep = 7 * up, 1 + 5 * up
        copies += [
            (rhs.at[:, near], out.at[3:6]),
            (visc.at[near], out.at[6]),
            (mass.at[near], out.at[7]),
            (rhs.at[:, deep], far.at[i, :3]),
            (visc.at[deep], far.at[i, 3]),
        ]
    copies = [pltpu.make_async_copy(*c, sems.at[i]) for i, c in enumerate(copies)]
    for c in copies:
        c.start()
    for c in copies:
        c.wait()
    for i, out in enumerate((msg_even, msg_odd)):
        for c in range(3):
            out[c] = far[i, c] * far[i, 3]


def scalars(vbounds, pbounds, coefs):
    for i, bounds in enumerate((vbounds, pbounds)):
        for j, value in enumerate(coefficients(bounds)):
            coefs[5 * i + j] = value


def z_halo(got_even, got_odd, i):
    even = parity("gz") == 0
    a, b = got_even[i], got_odd[i]
    return jnp.where(even, b, a), jnp.where(even, a, b)


def y_rows():
    out = []
    for p in range(PLANES):
        if p not in (S0, S0 + ZW - 1):
            out.append((p, 8, 7) if p // ZW == 1 else (p, 7, 6))
    return out


UP_ROWS = sum(r[1] for r in y_rows())
DOWN_ROWS = sum(r[2] for r in y_rows())


def padded(rows):
    return -(-rows // 8) * 8


def pack_nodes(pscale, prhs, pt):
    for k in range(PZ):
        pt[k] = jnp.concatenate([pscale[k], prhs[k]], axis=1)


def pack_y(rhs, visc, mass, got_even, got_odd, pt, own, up, down):
    for z in range(Z):
        for c in range(3):
            own[c * ZW + 2 + z] = rhs[c, z]
        own[S0 + 2 + z] = visc[z]
        own[M0 + 1 + z] = mass[z]
    for side, (deep, near) in enumerate(((0, 1), (ZW - 1, ZW - 2))):
        for c in range(3):
            own[c * ZW + deep] = z_halo(got_even, got_odd, c)[side]
            own[c * ZW + near] = z_halo(got_even, got_odd, 3 + c)[side]
        own[S0 + deep] = jnp.ones((Y, X), F32)
        own[S0 + near] = z_halo(got_even, got_odd, 6)[side]
        own[M0 + near - 1] = z_halo(got_even, got_odd, 7)[side]
    row = lax.broadcasted_iota(jnp.int32, (8, X), 0)
    at_up = at_down = 0
    for p, n_up, n_down in y_rows():
        if p // ZW == 1:
            z = p - ZW
            up[at_up : at_up + 8] = own[p, 8:] * jnp.where(row == 0, own[S0 + z, 8:], 1.0)
            part = own[p, :8] * jnp.where(row == 6, own[S0 + z, :8], 1.0)
            down[at_down : at_down + 7] = part[:7]
        else:
            up[at_up : at_up + n_up] = own[p, Y - n_up :]
            down[at_down : at_down + n_down] = own[p, :n_down]
        at_up, at_down = at_up + n_up, at_down + n_down
    for k in range(PZ):
        up[at_up + 2 * k : at_up + 2 * k + 2] = pt[k, 6:]
        down[at_down + 2 * k : at_down + 2 * k + 2] = pt[k, :2]


def pack_x(own, pt, below, above, main, up, down):
    at_up = at_down = 0
    rows = {r[0]: r[1:] for r in y_rows()}
    for p in range(PLANES):
        rest = jnp.full((8, X), 1.0 if S0 <= p < M0 else 0.0, F32)
        main[4 * p] = rest
        main[4 * p + 1] = own[p, :8]
        main[4 * p + 2] = own[p, 8:]
        main[4 * p + 3] = rest
        n_up, n_down = rows.get(p, (0, 0))
        if n_up:
            main[4 * p, 8 - n_up :] = below[at_up : at_up + n_up]
            main[4 * p + 3, :n_down] = above[at_down : at_down + n_down]
        at_up, at_down = at_up + n_up, at_down + n_down
    for k in range(PZ):
        for t in (0, 2):
            main[VT + 3 * k + t] = jnp.zeros((8, X), F32)
        main[VT + 3 * k, 6:] = below[at_up + 2 * k : at_up + 2 * k + 2]
        main[VT + 3 * k + 1] = pt[k]
        main[VT + 3 * k + 2, :2] = above[at_down + 2 * k : at_down + 2 * k + 2]
    lane = lanes()
    for k in range(PZ):
        for t in range(3):
            tile = main[VT + 3 * k + t]
            turned = pltpu.roll(tile, 64, axis=1)
            main[VT + 3 * k + t] = jnp.where(lane < 64, tile, turned)
            main[VT + 12 + 3 * k + t] = jnp.where(lane < 64, turned, tile)
    for i in range(PACKED):
        turned = main[16 * i : 16 * i + 16].reshape(X, X).T
        down[i] = turned[:8]
        up[i] = turned[X - 8 :]


def lanes():
    return lax.broadcasted_iota(jnp.int32, (8, X), 1)


def coefficients(bounds):
    low = jnp.full((8, X), bounds[0], F32)
    high = jnp.full((8, X), bounds[1], F32)
    centre = (high + low) / 2.0
    spread = (high - low) / 2.0
    sigma = centre / spread
    rho0 = 1.0 / sigma
    rho1 = 1.0 / (2.0 * sigma - rho0)
    rho2 = 1.0 / (2.0 * sigma - rho1)
    return 1.0 / centre, rho1 * rho0, 2.0 * rho1 / spread, rho2 * rho1, 2.0 * rho2 / spread


def tall(coef, rows):
    return jnp.concatenate([coef] * (rows // 8), axis=0)


def restriction():
    table = np.zeros((4, X, X), np.float32)
    for half in range(2):
        for l in range(X):
            x = l if half == 0 else (X + l if l < 8 else l - X)
            if half and 8 <= l < 120:
                continue
            for node in range(-2, PX + 2):
                o = x - 2 * node
                table[half, l, node + 2] = {-1: 0.25, 0: 0.5, 1: 0.25}.get(o, 0.0)
                table[2 + half, l, node + 2] = {-2: -0.125, -1: -0.25, 1: 0.25, 2: 0.125}.get(o, 0.0)
    return table.reshape(4 * X, X).astype(ml_dtypes.bfloat16)


SMOOTH_Z = {-1: (), 0: ((0, 0.5), (1, 0.25)), 4: ((7, 0.25),)}
DERIVE_Z = {
    -1: ((0, 0.125),),
    0: ((1, 0.25), (2, 0.125)),
    1: ((0, -0.125), (1, -0.25), (3, 0.25), (4, 0.125)),
    2: ((2, -0.125), (3, -0.25), (5, 0.25), (6, 0.125)),
    3: ((4, -0.125), (5, -0.25), (7, 0.25)),
    4: ((6, -0.125), (7, -0.25)),
}
for _k in (1, 2, 3):
    SMOOTH_Z[_k] = ((2 * _k - 1, 0.25), (2 * _k, 0.5), (2 * _k + 1, 0.25))


def smoothing():
    ring = np.eye(2 * X, dtype=np.float32)
    ring += 0.5 * (np.roll(ring, 1, axis=0) + np.roll(ring, -1, axis=0))
    return np.concatenate([ring[:X], ring[:X], ring[X:], ring[X:]]).astype(ml_dtypes.bfloat16)


def split(value, parts):
    out = []
    for _ in range(parts):
        out.append(value.astype(jnp.bfloat16))
        value = value - out[-1].astype(F32)
    return out


def dot(a, b):
    return lax.dot_general(a, b, (((1,), (0,)), ((), ())), preferred_element_type=F32)


def planes(ref, p):
    return ref[pl.ds(4 * p, 4)].reshape(32, X)


def loop(start, count, body, each=1):
    for z in range(start, start + count, each):
        body(list(range(z, min(z + each, start + count))))


def weigh(src, w):
    def body(zs):
        for z in zs:
            visc = planes(src, S0 + z)
            for c in range(3):
                w[c, z] = visc * planes(src, c * ZW + z)

    loop(0, ZW, body, 3)


def sum_rows(chains, t, lhs, z0, count):
    def body(zs):
        work = [(z, *chain) for z in zs for chain in chains]
        first = []
        for i, (z, c, w, col) in enumerate(work):
            v = w[z] + 0.5 * (w[z - 1] + w[z + 1])
            t[i, 8:40] = v
            first.append(v)
        for i, (z, c, w, col) in enumerate(work):
            v = first[i] + 0.5 * (t[i, 7:39] + t[i, 9:41])
            at = pl.ds((c * count + z - z0) * 32, 32)
            for part, value in enumerate(split(v, 2)):
                lhs[at, col + part * X : col + (part + 1) * X] = value

    loop(z0, count, body, 6 // len(chains))


def first_sums(main, ring, sums, w, t, lhs):
    t[...] = jnp.zeros_like(t)
    weigh(main, w)
    sum_rows([(c, w.at[c], 0) for c in range(3)], t, lhs, 1, Z + 2)
    sums[...] = dot(lhs[...], ring[: 2 * X])


def velocity_step(
    main, from_below, from_above, table, ring, sums, coefs, vel, coupled, pscale, msg_even, msg_odd,
    halo, w, d, r, u, t, lhs, s, g, q, ptmp,
):
    lane = lanes()
    gap = jnp.zeros((X - 16, X), F32)
    for i in range(PACKED):
        strips = jnp.concatenate([from_above[i], gap, from_below[i]], axis=0)
        halo[16 * i : 16 * i + 16] = strips.T.reshape(16, 8, X)

    inv, a1, g1, a2, g2 = (tall(coefs[i], 32) for i in range(5))
    t[...] = jnp.zeros_like(t)
    both = (main, halo)

    weigh(halo, w.at[1])
    sum_rows([(c, w.at[1, c], 2 * X) for c in range(3)], t, lhs, 1, Z + 2)
    s[...] = dot(lhs[:, 2 * X :], ring[2 * X :])

    def sweep1(zs):
        (z,) = zs
        for h, src in enumerate(both):
            visc, mass = planes(src, S0 + z), planes(src, M0 + z - 1)
            cols = slice(h * X, (h + 1) * X)
            for c in range(3):
                at = pl.ds((c * (Z + 2) + z - 1) * 32, 32)
                b = planes(src, c * ZW + z)
                d0 = b * inv
                lap = 16.0 * (visc * d0) - (2.0 * inv) * (sums[at, cols] + s[at, cols])
                res = b - (visc * lap + mass * d0)
                d1 = a1 * d0 + g1 * res
                r[h, c, z] = res
                d[h, c, z] = d1
                w[h, c, z] = visc * d1

    loop(1, Z + 2, sweep1)

    for c in range(3):
        sum_rows([(c, w.at[h, c], 2 * h * X) for h in range(2)], t, lhs, 2, Z)
        at = slice(c * Z * 32, (c + 1) * Z * 32)
        s[at] = dot(lhs[at], ring[...])

    def sweep2(zs):
        (z,) = zs
        for h, src in enumerate(both):
            visc, mass = planes(src, S0 + z), planes(src, M0 + z - 1)
            for c in range(3):
                at = pl.ds((c * Z + z - 2) * 32, 32)
                d1 = d[h, c, z]
                lap = 16.0 * w[h, c, z] - 2.0 * s[at, h * X : (h + 1) * X]
                res = r[h, c, z] - (visc * lap + mass * d1)
                value = planes(src, c * ZW + z) * inv + d1 + (a2 * d1 + g2 * res)
                u[c, h, z - 2] = value
                if h == 0:
                    vel[c, z - 2] = value[8:24]

    loop(2, Z, sweep2)

    q[...] = jnp.zeros_like(q)
    for node in range(-1, 5):
        rows = slice(16 * (node + 1), 16 * (node + 1) + 12)

        def along_z(c, h, weights):
            acc = None
            for z, f in weights:
                term = f * u[c, h, z]
                acc = term if acc is None else acc + term
            return acc

        def at(k, start):
            return g[k, pl.ds(start, 12, stride=2), :]

        for h in range(2):
            cols = slice(X * h, X * (h + 1))
            g[2] = along_z(2, h, DERIVE_Z[node])
            total = 0.25 * (at(2, 3) + at(2, 5)) + 0.5 * at(2, 4)
            if SMOOTH_Z[node]:
                g[0] = along_z(0, h, SMOOTH_Z[node])
                g[1] = along_z(1, h, SMOOTH_Z[node])
                total = total + 0.25 * (at(1, 5) - at(1, 3)) + 0.125 * (at(1, 6) - at(1, 2))
                q[rows, 2 * X + X * h : 3 * X + X * h] = 0.25 * (at(0, 3) + at(0, 5)) + 0.5 * at(0, 4)
            q[rows, cols] = total

    div = sum(dot(v, table[...]) for v in reversed(split(q[...], 3)))

    def nodes(base, k):
        for i in range(3):
            own = pltpu.roll(main[base + 3 * k + i], 2, axis=1)
            side = halo[base + 3 * k + i]
            left = pltpu.roll(side, 2, axis=1)
            right = pltpu.roll(side, 66, axis=1)
            value = jnp.where(lane < 66, own, jnp.where(lane < 68, right, 0.0))
            ptmp[8 * i : 8 * i + 8] = jnp.where(lane < 2, left, value)
        return ptmp[6:18]

    coupled[...] = -div.reshape(6, 16, X)
    pscale[...] = jnp.zeros_like(pscale)
    for k in range(PZ):
        pscale[k, :12] = nodes(VT, k)
        coupled[k + 1, :12] = nodes(VT + 12, k) - div[16 * (k + 1) : 16 * (k + 1) + 12]
    par = parity("gz")
    for out, up in ((msg_even, 1 - par), (msg_odd, par)):
        parts = (
            coupled[2 + up] * pscale[1 + up], coupled[1 + 3 * up], coupled[5 * up], pscale[3 * up],
        )
        for j, part in enumerate(parts):
            out[12 * j : 12 * j + 12] = part[:12]


def pressure_step(coupled, pscale, got_even, got_odd, coefs, out, halo):
    even = parity("gz") == 0
    halo[...] = jnp.zeros_like(halo)
    for i in range(4):
        rows = slice(12 * i, 12 * i + 12)
        a, b = got_even[rows], got_odd[rows]
        halo[0, i, :12] = jnp.where(even, b, a)
        halo[1, i, :12] = jnp.where(even, a, b)
    b = [
        halo[0, 0], halo[0, 1] + coupled[0], halo[0, 2] + coupled[1], coupled[2],
        coupled[3], coupled[4] + halo[1, 2], coupled[5] + halo[1, 1], halo[1, 0],
    ]
    one = jnp.ones((16, X), F32)
    s = [one, halo[0, 3], pscale[0], pscale[1], pscale[2], pscale[3], halo[1, 3], one]
    inv, a1, g1, a2, g2 = (tall(coefs[5 + i], 16) for i in range(5))

    def operator(w, z):
        v = (1.0 / 6.0) * (w[z - 1] + w[z + 1]) + (2.0 / 3.0) * w[z]
        v = (1.0 / 6.0) * (pltpu.roll(v, 1, axis=0) + pltpu.roll(v, 15, axis=0)) + (2.0 / 3.0) * v
        v = (1.0 / 6.0) * (pltpu.roll(v, 1, axis=1) + pltpu.roll(v, X - 1, axis=1)) + (2.0 / 3.0) * v
        return s[z] * v

    d0 = [v * inv for v in b]
    w = [x * y for x, y in zip(s, d0)]
    r1, d1, w1 = [None] * 8, [None] * 8, [None] * 8
    for z in range(1, 7):
        r1[z] = b[z] - operator(w, z)
        d1[z] = a1 * d0[z] + g1 * r1[z]
        w1[z] = s[z] * d1[z]
    for z in range(2, 6):
        res = r1[z] - operator(w1, z)
        total = d0[z] + d1[z] + (a2 * d1[z] + g2 * res)
        total = pltpu.roll(pltpu.roll(total, 14, axis=0), X - 2, axis=1)
        out[z - 2] = total[:PY, :PX]


def per_device(rhs, prhs, visc, mass, pscale, vbounds, pbounds):
    plane, tile = (Y, X), (8, X)
    msg_even, msg_odd = call(
        pack_z,
        [(8, *plane)] * 2,
        scratch=[pltpu.VMEM((2, 4, *plane), F32), pltpu.SemaphoreType.DMA((10,))],
        hbm=(0, 1, 2),
    )(rhs, visc, mass)
    z_halos = swap_neighbours("gz", msg_even, msg_odd)
    (coefs,) = call(scalars, [(10, *tile)], smem=(0, 1))(vbounds, pbounds)
    (pt,) = call(pack_nodes, [(PZ, *tile)])(pscale, prhs)
    own, up, down = call(
        pack_y, [(PLANES, *plane), (padded(UP_ROWS + 8), X), (padded(DOWN_ROWS + 8), X)]
    )(rhs, visc, mass, *z_halos, pt)
    below, above = both_neighbours("gy", up, down)
    main, up, down = call(pack_x, [(TILES, *tile), (PACKED, *tile), (PACKED, *tile)])(
        own, pt, below, above
    )
    below, above = both_neighbours("gx", up, down)
    ring = jnp.asarray(smoothing())
    rows = 3 * (Z + 2) * 32
    (sums,) = call(
        first_sums,
        [(rows, 2 * X)],
        scratch=[
            pltpu.VMEM((3, ZW, 32, X), F32),
            pltpu.VMEM((6, 48, X), F32),
            pltpu.VMEM((rows, 2 * X), jnp.bfloat16),
        ],
    )(main, ring)
    vel, coupled, scale, msg_even, msg_odd = call(
        velocity_step,
        [(3, Z, Y, X), (6, *plane), (PZ, *plane), (48, X), (48, X)],
        vmem=(0,),
        scratch=[
            pltpu.VMEM((TILES, 8, X), F32),
            pltpu.VMEM((2, 3, ZW, 32, X), F32),
            pltpu.VMEM((2, 3, ZW, 32, X), F32),
            pltpu.VMEM((2, 3, ZW, 32, X), F32),
            pltpu.VMEM((3, 2, Z, 32, X), F32),
            pltpu.VMEM((6, 48, X), F32),
            pltpu.VMEM((rows, 4 * X), jnp.bfloat16),
            pltpu.VMEM((rows, 2 * X), F32),
            pltpu.VMEM((3, 32, X), F32),
            pltpu.VMEM((96, 4 * X), F32),
            pltpu.VMEM((24, X), F32),
        ],
    )(main, below, above, jnp.asarray(restriction()), ring, sums, coefs)
    z_halos = swap_neighbours("gz", msg_even, msg_odd)
    (pressure,) = call(
        pressure_step, [(PZ, PY, PX)], scratch=[pltpu.VMEM((2, 4, *plane), F32)]
    )(coupled, scale, *z_halos, coefs)
    return vel, pressure


def solution(mesh):
    block = P("gz", "gy", "gx")
    field = P(None, "gz", "gy", "gx")
    return jax.shard_map(
        per_device,
        mesh=mesh,
        in_specs=(field, block, block, block, block, P(), P()),
        out_specs=(field, block),
        check_vma=False,
    )
```

```python
import jax
import jax.numpy as jnp
import ml_dtypes
import numpy as np
from jax import lax
from jax.experimental import pallas as pl
from jax.experimental.pallas import tpu as pltpu
from jax.sharding import PartitionSpec as P


Z, Y, X = 8, 16, 128
PZ, PY, PX = 4, 8, 64
F32 = jnp.float32
VMEM_LIMIT = 16 * 2**20

ZW = Z + 4
PLANES = 4 * ZW + Z + 2
S0, M0 = 3 * ZW, 4 * ZW
VT = 4 * PLANES
TILES = VT + 24
PACKED = TILES // 16


def parity(axis):
    return lax.rem(lax.axis_index(axis), 2)


def swap_neighbours(axis, first, second):
    size = lax.axis_size(axis)
    even = [(i, i ^ 1) for i in range(size)]
    odd = [(i, ((i + 1) ^ 1) - 1) for i in range(1, size - 1)]
    inner = lax.ppermute(first, axis, even)
    outer = lax.ppermute(second, axis, odd)
    return inner, outer


def both_neighbours(axis, to_above, to_below):
    size = lax.axis_size(axis)
    up = [(i, i + 1) for i in range(size - 1)]
    down = [(i + 1, i) for i in range(size - 1)]
    from_below = lax.ppermute(to_above, axis, up)
    from_above = lax.ppermute(to_below, axis, down)
    return from_below, from_above


def call(body, outs, scratch=(), smem=(), hbm=(), vmem=()):
    def run(*args):
        space = {i: pltpu.SMEM for i in smem} | {i: pltpu.HBM for i in hbm}
        args = [
            pltpu.with_memory_space_constraint(x, pltpu.HBM) if i in hbm else x
            for i, x in enumerate(args)
        ]
        return pl.pallas_call(
            body,
            in_specs=[
                pl.BlockSpec(memory_space=space.get(i, pltpu.VMEM)) for i in range(len(args))
            ],
            out_specs=[pl.BlockSpec(memory_space=pltpu.VMEM) for _ in outs],
            out_shape=[
                pltpu.VMEM(o, F32) if i in vmem else jax.ShapeDtypeStruct(o, F32)
                for i, o in enumerate(outs)
            ],
            scratch_shapes=list(scratch),
            compiler_params=pltpu.CompilerParams(vmem_limit_bytes=VMEM_LIMIT),
        )(*args)

    return run


def pack_z(rhs, visc, mass, msg_even, msg_odd, far, sems):
    par = parity("gz")
    copies = []
    for i, (out, up) in enumerate(((msg_even, 1 - par), (msg_odd, par))):
        near, deep = 7 * up, 1 + 5 * up
        copies += [
            (rhs.at[:, near], out.at[3:6]),
            (visc.at[near], out.at[6]),
            (mass.at[near], out.at[7]),
            (rhs.at[:, deep], far.at[i, :3]),
            (visc.at[deep], far.at[i, 3]),
        ]
    copies = [pltpu.make_async_copy(*c, sems.at[i]) for i, c in enumerate(copies)]
    for c in copies:
        c.start()
    for c in copies:
        c.wait()
    for i, out in enumerate((msg_even, msg_odd)):
        for c in range(3):
            out[c] = far[i, c] * far[i, 3]


def scalars(vbounds, pbounds, coefs):
    for i, bounds in enumerate((vbounds, pbounds)):
        for j, value in enumerate(coefficients(bounds)):
            coefs[5 * i + j] = value


def z_halo(got_even, got_odd, i):
    even = parity("gz") == 0
    a, b = got_even[i], got_odd[i]
    return jnp.where(even, b, a), jnp.where(even, a, b)


def y_rows():
    out = []
    for p in range(PLANES):
        if p not in (S0, S0 + ZW - 1):
            out.append((p, 8, 7) if p // ZW == 1 else (p, 7, 6))
    return out


UP_ROWS = sum(r[1] for r in y_rows())
DOWN_ROWS = sum(r[2] for r in y_rows())


def padded(rows):
    return -(-rows // 8) * 8


def pack_nodes(pscale, prhs, pt):
    for k in range(PZ):
        pt[k] = jnp.concatenate([pscale[k], prhs[k]], axis=1)


def pack_y(rhs, visc, mass, got_even, got_odd, pt, own, up, down):
    for z in range(Z):
        for c in range(3):
            own[c * ZW + 2 + z] = rhs[c, z]
        own[S0 + 2 + z] = visc[z]
        own[M0 + 1 + z] = mass[z]
    for side, (deep, near) in enumerate(((0, 1), (ZW - 1, ZW - 2))):
        for c in range(3):
            own[c * ZW + deep] = z_halo(got_even, got_odd, c)[side]
            own[c * ZW + near] = z_halo(got_even, got_odd, 3 + c)[side]
        own[S0 + deep] = jnp.ones((Y, X), F32)
        own[S0 + near] = z_halo(got_even, got_odd, 6)[side]
        own[M0 + near - 1] = z_halo(got_even, got_odd, 7)[side]
    row = lax.broadcasted_iota(jnp.int32, (8, X), 0)
    at_up = at_down = 0
    for p, n_up, n_down in y_rows():
        if p // ZW == 1:
            z = p - ZW
            up[at_up : at_up + 8] = own[p, 8:] * jnp.where(row == 0, own[S0 + z, 8:], 1.0)
            part = own[p, :8] * jnp.where(row == 6, own[S0 + z, :8], 1.0)
            down[at_down : at_down + 7] = part[:7]
        else:
            up[at_up : at_up + n_up] = own[p, Y - n_up :]
            down[at_down : at_down + n_down] = own[p, :n_down]
        at_up, at_down = at_up + n_up, at_down + n_down
    for k in range(PZ):
        up[at_up + 2 * k : at_up + 2 * k + 2] = pt[k, 6:]
        down[at_down + 2 * k : at_down + 2 * k + 2] = pt[k, :2]


def pack_x(own, pt, below, above, main, msg_even, msg_odd):
    at_up = at_down = 0
    rows = {r[0]: r[1:] for r in y_rows()}
    for p in range(PLANES):
        rest = jnp.full((8, X), 1.0 if S0 <= p < M0 else 0.0, F32)
        main[4 * p] = rest
        main[4 * p + 1] = own[p, :8]
        main[4 * p + 2] = own[p, 8:]
        main[4 * p + 3] = rest
        n_up, n_down = rows.get(p, (0, 0))
        if n_up:
            main[4 * p, 8 - n_up :] = below[at_up : at_up + n_up]
            main[4 * p + 3, :n_down] = above[at_down : at_down + n_down]
        at_up, at_down = at_up + n_up, at_down + n_down
    for k in range(PZ):
        for t in (0, 2):
            main[VT + 3 * k + t] = jnp.zeros((8, X), F32)
        main[VT + 3 * k, 6:] = below[at_up + 2 * k : at_up + 2 * k + 2]
        main[VT + 3 * k + 1] = pt[k]
        main[VT + 3 * k + 2, :2] = above[at_down + 2 * k : at_down + 2 * k + 2]
    lane = lanes()
    for k in range(PZ):
        for t in range(3):
            tile = main[VT + 3 * k + t]
            turned = pltpu.roll(tile, 64, axis=1)
            main[VT + 3 * k + t] = jnp.where(lane < 64, tile, turned)
            main[VT + 12 + 3 * k + t] = jnp.where(lane < 64, turned, tile)
    even = parity("gx") == 0
    for i in range(PACKED):
        turned = main[16 * i : 16 * i + 16].reshape(X, X).T
        low, high = turned[:8], turned[X - 8 :]
        msg_even[i] = jnp.where(even, high, low)
        msg_odd[i] = jnp.where(even, low, high)


def lanes():
    return lax.broadcasted_iota(jnp.int32, (8, X), 1)


def coefficients(bounds):
    low = jnp.full((8, X), bounds[0], F32)
    high = jnp.full((8, X), bounds[1], F32)
    centre = (high + low) / 2.0
    spread = (high - low) / 2.0
    sigma = centre / spread
    rho0 = 1.0 / sigma
    rho1 = 1.0 / (2.0 * sigma - rho0)
    rho2 = 1.0 / (2.0 * sigma - rho1)
    return 1.0 / centre, rho1 * rho0, 2.0 * rho1 / spread, rho2 * rho1, 2.0 * rho2 / spread


def tall(coef, rows):
    return jnp.concatenate([coef] * (rows // 8), axis=0)


def restriction():
    table = np.zeros((4, X, X), np.float32)
    for half in range(2):
        for l in range(X):
            x = l if half == 0 else (X + l if l < 8 else l - X)
            if half and 8 <= l < 120:
                continue
            for node in range(-2, PX + 2):
                o = x - 2 * node
                table[half, l, node + 2] = {-1: 0.25, 0: 0.5, 1: 0.25}.get(o, 0.0)
                table[2 + half, l, node + 2] = {-2: -0.125, -1: -0.25, 1: 0.25, 2: 0.125}.get(o, 0.0)
    return table.reshape(4 * X, X).astype(ml_dtypes.bfloat16)


SMOOTH_Z = {-1: (), 0: ((0, 0.5), (1, 0.25)), 4: ((7, 0.25),)}
DERIVE_Z = {
    -1: ((0, 0.125),),
    0: ((1, 0.25), (2, 0.125)),
    1: ((0, -0.125), (1, -0.25), (3, 0.25), (4, 0.125)),
    2: ((2, -0.125), (3, -0.25), (5, 0.25), (6, 0.125)),
    3: ((4, -0.125), (5, -0.25), (7, 0.25)),
    4: ((6, -0.125), (7, -0.25)),
}
for _k in (1, 2, 3):
    SMOOTH_Z[_k] = ((2 * _k - 1, 0.25), (2 * _k, 0.5), (2 * _k + 1, 0.25))


def smoothing():
    ring = np.eye(2 * X, dtype=np.float32)
    ring += 0.5 * (np.roll(ring, 1, axis=0) + np.roll(ring, -1, axis=0))
    return np.concatenate([ring[:X], ring[:X], ring[X:], ring[X:]]).astype(ml_dtypes.bfloat16)


def split(value, parts):
    out = []
    for _ in range(parts):
        out.append(value.astype(jnp.bfloat16))
        value = value - out[-1].astype(F32)
    return out


def dot(a, b):
    return lax.dot_general(a, b, (((1,), (0,)), ((), ())), preferred_element_type=F32)


def planes(ref, p):
    return ref[pl.ds(4 * p, 4)].reshape(32, X)


def loop(start, count, body, each=1):
    for z in range(start, start + count, each):
        body(list(range(z, min(z + each, start + count))))


def weigh(src, w):
    def body(zs):
        for z in zs:
            visc = planes(src, S0 + z)
            for c in range(3):
                w[c, z] = visc * planes(src, c * ZW + z)

    loop(0, ZW, body, 3)


def sum_rows(chains, t, lhs, z0, count):
    def body(zs):
        work = [(z, *chain) for z in zs for chain in chains]
        first = []
        for i, (z, c, w, col) in enumerate(work):
            v = w[z] + 0.5 * (w[z - 1] + w[z + 1])
            t[i, 8:40] = v
            first.append(v)
        for i, (z, c, w, col) in enumerate(work):
            v = first[i] + 0.5 * (t[i, 7:39] + t[i, 9:41])
            at = pl.ds((c * count + z - z0) * 32, 32)
            for part, value in enumerate(split(v, 2)):
                lhs[at, col + part * X : col + (part + 1) * X] = value

    loop(z0, count, body, 6 // len(chains))


def first_sums(main, ring, sums, w, t, lhs):
    t[...] = jnp.zeros_like(t)
    weigh(main, w)
    sum_rows([(c, w.at[c], 0) for c in range(3)], t, lhs, 1, Z + 2)
    sums[...] = dot(lhs[...], ring[: 2 * X])


def velocity_step(
    main, got_even, got_odd, table, ring, sums, coefs, vel, coupled, pscale, msg_even, msg_odd,
    halo, w, d, r, u, t, lhs, s, g, q, ptmp,
):
    lane = lanes()
    gap = jnp.zeros((X - 16, X), F32)
    even = parity("gx") == 0
    for i in range(PACKED):
        a, b = got_even[i], got_odd[i]
        strips = jnp.concatenate([jnp.where(even, a, b), gap, jnp.where(even, b, a)], axis=0)
        halo[16 * i : 16 * i + 16] = strips.T.reshape(16, 8, X)

    inv, a1, g1, a2, g2 = (tall(coefs[i], 32) for i in range(5))
    t[...] = jnp.zeros_like(t)
    both = (main, halo)

    weigh(halo, w.at[1])
    sum_rows([(c, w.at[1, c], 2 * X) for c in range(3)], t, lhs, 1, Z + 2)
    s[...] = dot(lhs[:, 2 * X :], ring[2 * X :])

    def sweep1(zs):
        (z,) = zs
        for h, src in enumerate(both):
            visc, mass = planes(src, S0 + z), planes(src, M0 + z - 1)
            cols = slice(h * X, (h + 1) * X)
            for c in range(3):
                at = pl.ds((c * (Z + 2) + z - 1) * 32, 32)
                b = planes(src, c * ZW + z)
                d0 = b * inv
                lap = 16.0 * (visc * d0) - (2.0 * inv) * (sums[at, cols] + s[at, cols])
                res = b - (visc * lap + mass * d0)
                d1 = a1 * d0 + g1 * res
                r[h, c, z] = res
                d[h, c, z] = d1
                w[h, c, z] = visc * d1

    loop(1, Z + 2, sweep1)

    for c in range(3):
        sum_rows([(c, w.at[h, c], 2 * h * X) for h in range(2)], t, lhs, 2, Z)
        at = slice(c * Z * 32, (c + 1) * Z * 32)
        s[at] = dot(lhs[at], ring[...])

    def sweep2(zs):
        (z,) = zs
        for h, src in enumerate(both):
            visc, mass = planes(src, S0 + z), planes(src, M0 + z - 1)
            for c in range(3):
                at = pl.ds((c * Z + z - 2) * 32, 32)
                d1 = d[h, c, z]
                lap = 16.0 * w[h, c, z] - 2.0 * s[at, h * X : (h + 1) * X]
                res = r[h, c, z] - (visc * lap + mass * d1)
                value = planes(src, c * ZW + z) * inv + d1 + (a2 * d1 + g2 * res)
                u[c, h, z - 2] = value
                if h == 0:
                    vel[c, z - 2] = value[8:24]

    loop(2, Z, sweep2)

    q[...] = jnp.zeros_like(q)
    for node in range(-1, 5):
        rows = slice(16 * (node + 1), 16 * (node + 1) + 12)

        def along_z(c, h, weights):
            acc = None
            for z, f in weights:
                term = f * u[c, h, z]
                acc = term if acc is None else acc + term
            return acc

        def at(k, start):
            return g[k, pl.ds(start, 12, stride=2), :]

        for h in range(2):
            cols = slice(X * h, X * (h + 1))
            g[2] = along_z(2, h, DERIVE_Z[node])
            total = 0.25 * (at(2, 3) + at(2, 5)) + 0.5 * at(2, 4)
            if SMOOTH_Z[node]:
                g[0] = along_z(0, h, SMOOTH_Z[node])
                g[1] = along_z(1, h, SMOOTH_Z[node])
                total = total + 0.25 * (at(1, 5) - at(1, 3)) + 0.125 * (at(1, 6) - at(1, 2))
                q[rows, 2 * X + X * h : 3 * X + X * h] = 0.25 * (at(0, 3) + at(0, 5)) + 0.5 * at(0, 4)
            q[rows, cols] = total

    div = sum(dot(v, table[...]) for v in reversed(split(q[...], 3)))

    def nodes(base, k):
        for i in range(3):
            own = pltpu.roll(main[base + 3 * k + i], 2, axis=1)
            side = halo[base + 3 * k + i]
            left = pltpu.roll(side, 2, axis=1)
            right = pltpu.roll(side, 66, axis=1)
            value = jnp.where(lane < 66, own, jnp.where(lane < 68, right, 0.0))
            ptmp[8 * i : 8 * i + 8] = jnp.where(lane < 2, left, value)
        return ptmp[6:18]

    coupled[...] = -div.reshape(6, 16, X)
    pscale[...] = jnp.zeros_like(pscale)
    for k in range(PZ):
        pscale[k, :12] = nodes(VT, k)
        coupled[k + 1, :12] = nodes(VT + 12, k) - div[16 * (k + 1) : 16 * (k + 1) + 12]
    par = parity("gz")
    for out, up in ((msg_even, 1 - par), (msg_odd, par)):
        parts = (
            coupled[2 + up] * pscale[1 + up], coupled[1 + 3 * up], coupled[5 * up], pscale[3 * up],
        )
        for j, part in enumerate(parts):
            out[12 * j : 12 * j + 12] = part[:12]


def pressure_step(coupled, pscale, got_even, got_odd, coefs, out, halo):
    even = parity("gz") == 0
    halo[...] = jnp.zeros_like(halo)
    for i in range(4):
        rows = slice(12 * i, 12 * i + 12)
        a, b = got_even[rows], got_odd[rows]
        halo[0, i, :12] = jnp.where(even, b, a)
        halo[1, i, :12] = jnp.where(even, a, b)
    b = [
        halo[0, 0], halo[0, 1] + coupled[0], halo[0, 2] + coupled[1], coupled[2],
        coupled[3], coupled[4] + halo[1, 2], coupled[5] + halo[1, 1], halo[1, 0],
    ]
    one = jnp.ones((16, X), F32)
    s = [one, halo[0, 3], pscale[0], pscale[1], pscale[2], pscale[3], halo[1, 3], one]
    inv, a1, g1, a2, g2 = (tall(coefs[5 + i], 16) for i in range(5))

    def operator(w, z):
        v = (1.0 / 6.0) * (w[z - 1] + w[z + 1]) + (2.0 / 3.0) * w[z]
        v = (1.0 / 6.0) * (pltpu.roll(v, 1, axis=0) + pltpu.roll(v, 15, axis=0)) + (2.0 / 3.0) * v
        v = (1.0 / 6.0) * (pltpu.roll(v, 1, axis=1) + pltpu.roll(v, X - 1, axis=1)) + (2.0 / 3.0) * v
        return s[z] * v

    d0 = [v * inv for v in b]
    w = [x * y for x, y in zip(s, d0)]
    r1, d1, w1 = [None] * 8, [None] * 8, [None] * 8
    for z in range(1, 7):
        r1[z] = b[z] - operator(w, z)
        d1[z] = a1 * d0[z] + g1 * r1[z]
        w1[z] = s[z] * d1[z]
    for z in range(2, 6):
        res = r1[z] - operator(w1, z)
        total = d0[z] + d1[z] + (a2 * d1[z] + g2 * res)
        total = pltpu.roll(pltpu.roll(total, 14, axis=0), X - 2, axis=1)
        out[z - 2] = total[:PY, :PX]


def per_device(rhs, prhs, visc, mass, pscale, vbounds, pbounds):
    plane, tile = (Y, X), (8, X)
    msg_even, msg_odd = call(
        pack_z,
        [(8, *plane)] * 2,
        scratch=[pltpu.VMEM((2, 4, *plane), F32), pltpu.SemaphoreType.DMA((10,))],
        hbm=(0, 1, 2),
    )(rhs, visc, mass)
    z_halos = swap_neighbours("gz", msg_even, msg_odd)
    (coefs,) = call(scalars, [(10, *tile)], smem=(0, 1))(vbounds, pbounds)
    (pt,) = call(pack_nodes, [(PZ, *tile)])(pscale, prhs)
    own, up, down = call(
        pack_y, [(PLANES, *plane), (padded(UP_ROWS + 8), X), (padded(DOWN_ROWS + 8), X)]
    )(rhs, visc, mass, *z_halos, pt)
    below, above = both_neighbours("gy", up, down)
    main, msg_even, msg_odd = call(pack_x, [(TILES, *tile), (PACKED, *tile), (PACKED, *tile)])(
        own, pt, below, above
    )
    below, above = swap_neighbours("gx", msg_even, msg_odd)
    ring = jnp.asarray(smoothing())
    rows = 3 * (Z + 2) * 32
    (sums,) = call(
        first_sums,
        [(rows, 2 * X)],
        scratch=[
            pltpu.VMEM((3, ZW, 32, X), F32),
            pltpu.VMEM((6, 48, X), F32),
            pltpu.VMEM((rows, 2 * X), jnp.bfloat16),
        ],
    )(main, ring)
    vel, coupled, scale, msg_even, msg_odd = call(
        velocity_step,
        [(3, Z, Y, X), (6, *plane), (PZ, *plane), (48, X), (48, X)],
        vmem=(0,),
        scratch=[
            pltpu.VMEM((TILES, 8, X), F32),
            pltpu.VMEM((2, 3, ZW, 32, X), F32),
            pltpu.VMEM((2, 3, ZW, 32, X), F32),
            pltpu.VMEM((2, 3, ZW, 32, X), F32),
            pltpu.VMEM((3, 2, Z, 32, X), F32),
            pltpu.VMEM((6, 48, X), F32),
            pltpu.VMEM((rows, 4 * X), jnp.bfloat16),
            pltpu.VMEM((rows, 2 * X), F32),
            pltpu.VMEM((3, 32, X), F32),
            pltpu.VMEM((96, 4 * X), F32),
            pltpu.VMEM((24, X), F32),
        ],
    )(main, below, above, jnp.asarray(restriction()), ring, sums, coefs)
    z_halos = swap_neighbours("gz", msg_even, msg_odd)
    (pressure,) = call(
        pressure_step, [(PZ, PY, PX)], scratch=[pltpu.VMEM((2, 4, *plane), F32)]
    )(coupled, scale, *z_halos, coefs)
    return vel, pressure


def solution(mesh):
    block = P("gz", "gy", "gx")
    field = P(None, "gz", "gy", "gx")
    return jax.shard_map(
        per_device,
        mesh=mesh,
        in_specs=(field, block, block, block, block, P(), P()),
        out_specs=(field, block),
        check_vma=False,
    )
```

```python
import jax
import jax.numpy as jnp
import ml_dtypes
import numpy as np
from jax import lax
from jax.experimental import pallas as pl
from jax.experimental.pallas import tpu as pltpu
from jax.sharding import PartitionSpec as P


Z, Y, X = 8, 16, 128
PZ, PY, PX = 4, 8, 64
F32 = jnp.float32
VMEM_LIMIT = 16 * 2**20

ZW = Z + 4
PLANES = 4 * ZW + Z + 2
S0, M0 = 3 * ZW, 4 * ZW
VT = 4 * PLANES
TILES = VT + 24
PACKED = TILES // 16


def parity(axis):
    return lax.rem(lax.axis_index(axis), 2)


def swap_neighbours(axis, first, second):
    size = lax.axis_size(axis)
    even = [(i, i ^ 1) for i in range(size)]
    odd = [(i, ((i + 1) ^ 1) - 1) for i in range(1, size - 1)]
    inner = lax.ppermute(first, axis, even)
    outer = lax.ppermute(second, axis, odd)
    return inner, outer


def call(body, outs, scratch=(), smem=(), hbm=(), vmem=()):
    def run(*args):
        space = {i: pltpu.SMEM for i in smem} | {i: pltpu.HBM for i in hbm}
        args = [
            pltpu.with_memory_space_constraint(x, pltpu.HBM) if i in hbm else x
            for i, x in enumerate(args)
        ]
        return pl.pallas_call(
            body,
            in_specs=[
                pl.BlockSpec(memory_space=space.get(i, pltpu.VMEM)) for i in range(len(args))
            ],
            out_specs=[pl.BlockSpec(memory_space=pltpu.VMEM) for _ in outs],
            out_shape=[
                pltpu.VMEM(o, F32) if i in vmem else jax.ShapeDtypeStruct(o, F32)
                for i, o in enumerate(outs)
            ],
            scratch_shapes=list(scratch),
            compiler_params=pltpu.CompilerParams(vmem_limit_bytes=VMEM_LIMIT),
        )(*args)

    return run


def pack_z(rhs, visc, mass, msg_even, msg_odd, far, sems):
    par = parity("gz")
    copies = []
    for i, (out, up) in enumerate(((msg_even, 1 - par), (msg_odd, par))):
        near, deep = 7 * up, 1 + 5 * up
        copies += [
            (rhs.at[:, near], out.at[3:6]),
            (visc.at[near], out.at[6]),
            (mass.at[near], out.at[7]),
            (rhs.at[:, deep], far.at[i, :3]),
            (visc.at[deep], far.at[i, 3]),
        ]
    copies = [pltpu.make_async_copy(*c, sems.at[i]) for i, c in enumerate(copies)]
    for c in copies:
        c.start()
    for c in copies:
        c.wait()
    for i, out in enumerate((msg_even, msg_odd)):
        for c in range(3):
            out[c] = far[i, c] * far[i, 3]


def scalars(vbounds, pbounds, coefs):
    for i, bounds in enumerate((vbounds, pbounds)):
        for j, value in enumerate(coefficients(bounds)):
            coefs[5 * i + j] = value


def z_halo(got_even, got_odd, i):
    even = parity("gz") == 0
    a, b = got_even[i], got_odd[i]
    return jnp.where(even, b, a), jnp.where(even, a, b)


def y_rows():
    out = []
    for p in range(PLANES):
        if p not in (S0, S0 + ZW - 1):
            out.append((p, 8, 7) if p // ZW == 1 else (p, 7, 6))
    return out


UP_ROWS = sum(r[1] for r in y_rows())
DOWN_ROWS = sum(r[2] for r in y_rows())


Y_ROWS = -(-(max(UP_ROWS, DOWN_ROWS) + 8) // 8) * 8


def pack_nodes(pscale, prhs, pt):
    for k in range(PZ):
        pt[k] = jnp.concatenate([pscale[k], prhs[k]], axis=1)


def pack_y(rhs, visc, mass, got_even, got_odd, pt, own, msg_even, msg_odd, up, down):
    for z in range(Z):
        for c in range(3):
            own[c * ZW + 2 + z] = rhs[c, z]
        own[S0 + 2 + z] = visc[z]
        own[M0 + 1 + z] = mass[z]
    for side, (deep, near) in enumerate(((0, 1), (ZW - 1, ZW - 2))):
        for c in range(3):
            own[c * ZW + deep] = z_halo(got_even, got_odd, c)[side]
            own[c * ZW + near] = z_halo(got_even, got_odd, 3 + c)[side]
        own[S0 + deep] = jnp.ones((Y, X), F32)
        own[S0 + near] = z_halo(got_even, got_odd, 6)[side]
        own[M0 + near - 1] = z_halo(got_even, got_odd, 7)[side]
    up[Y_ROWS - 8 :] = jnp.zeros((8, X), F32)
    unused = DOWN_ROWS // 8 * 8
    down[unused:] = jnp.zeros((Y_ROWS - unused, X), F32)
    row = lax.broadcasted_iota(jnp.int32, (8, X), 0)
    at_up = at_down = 0
    for p, n_up, n_down in y_rows():
        if p // ZW == 1:
            z = p - ZW
            up[at_up : at_up + 8] = own[p, 8:] * jnp.where(row == 0, own[S0 + z, 8:], 1.0)
            part = own[p, :8] * jnp.where(row == 6, own[S0 + z, :8], 1.0)
            down[at_down : at_down + 7] = part[:7]
        else:
            up[at_up : at_up + n_up] = own[p, Y - n_up :]
            down[at_down : at_down + n_down] = own[p, :n_down]
        at_up, at_down = at_up + n_up, at_down + n_down
    for k in range(PZ):
        up[at_up + 2 * k : at_up + 2 * k + 2] = pt[k, 6:]
        down[at_down + 2 * k : at_down + 2 * k + 2] = pt[k, :2]
    even = parity("gy") == 0
    for i in range(0, Y_ROWS, 8):
        tile = slice(i, i + 8)
        a, b = up[tile], down[tile]
        msg_even[tile] = jnp.where(even, a, b)
        msg_odd[tile] = jnp.where(even, b, a)


def pack_x(own, pt, got_even, got_odd, main, msg_even, msg_odd, below, above):
    even = parity("gy") == 0
    for i in range(0, Y_ROWS, 8):
        tile = slice(i, i + 8)
        a, b = got_even[tile], got_odd[tile]
        below[tile] = jnp.where(even, b, a)
        above[tile] = jnp.where(even, a, b)
    at_up = at_down = 0
    rows = {r[0]: r[1:] for r in y_rows()}
    for p in range(PLANES):
        rest = jnp.full((8, X), 1.0 if S0 <= p < M0 else 0.0, F32)
        main[4 * p] = rest
        main[4 * p + 1] = own[p, :8]
        main[4 * p + 2] = own[p, 8:]
        main[4 * p + 3] = rest
        n_up, n_down = rows.get(p, (0, 0))
        if n_up:
            main[4 * p, 8 - n_up :] = below[at_up : at_up + n_up]
            main[4 * p + 3, :n_down] = above[at_down : at_down + n_down]
        at_up, at_down = at_up + n_up, at_down + n_down
    for k in range(PZ):
        for t in (0, 2):
            main[VT + 3 * k + t] = jnp.zeros((8, X), F32)
        main[VT + 3 * k, 6:] = below[at_up + 2 * k : at_up + 2 * k + 2]
        main[VT + 3 * k + 1] = pt[k]
        main[VT + 3 * k + 2, :2] = above[at_down + 2 * k : at_down + 2 * k + 2]
    lane = lanes()
    for k in range(PZ):
        for t in range(3):
            tile = main[VT + 3 * k + t]
            turned = pltpu.roll(tile, 64, axis=1)
            main[VT + 3 * k + t] = jnp.where(lane < 64, tile, turned)
            main[VT + 12 + 3 * k + t] = jnp.where(lane < 64, turned, tile)
    even = parity("gx") == 0
    for i in range(PACKED):
        turned = main[16 * i : 16 * i + 16].reshape(X, X).T
        low, high = turned[:8], turned[X - 8 :]
        msg_even[i] = jnp.where(even, high, low)
        msg_odd[i] = jnp.where(even, low, high)


def lanes():
    return lax.broadcasted_iota(jnp.int32, (8, X), 1)


def coefficients(bounds):
    low = jnp.full((8, X), bounds[0], F32)
    high = jnp.full((8, X), bounds[1], F32)
    centre = (high + low) / 2.0
    spread = (high - low) / 2.0
    sigma = centre / spread
    rho0 = 1.0 / sigma
    rho1 = 1.0 / (2.0 * sigma - rho0)
    rho2 = 1.0 / (2.0 * sigma - rho1)
    return 1.0 / centre, rho1 * rho0, 2.0 * rho1 / spread, rho2 * rho1, 2.0 * rho2 / spread


def tall(coef, rows):
    return jnp.concatenate([coef] * (rows // 8), axis=0)


def restriction():
    table = np.zeros((4, X, X), np.float32)
    for half in range(2):
        for l in range(X):
            x = l if half == 0 else (X + l if l < 8 else l - X)
            if half and 8 <= l < 120:
                continue
            for node in range(-2, PX + 2):
                o = x - 2 * node
                table[half, l, node + 2] = {-1: 0.25, 0: 0.5, 1: 0.25}.get(o, 0.0)
                table[2 + half, l, node + 2] = {-2: -0.125, -1: -0.25, 1: 0.25, 2: 0.125}.get(o, 0.0)
    return table.reshape(4 * X, X).astype(ml_dtypes.bfloat16)


SMOOTH_Z = {-1: (), 0: ((0, 0.5), (1, 0.25)), 4: ((7, 0.25),)}
DERIVE_Z = {
    -1: ((0, 0.125),),
    0: ((1, 0.25), (2, 0.125)),
    1: ((0, -0.125), (1, -0.25), (3, 0.25), (4, 0.125)),
    2: ((2, -0.125), (3, -0.25), (5, 0.25), (6, 0.125)),
    3: ((4, -0.125), (5, -0.25), (7, 0.25)),
    4: ((6, -0.125), (7, -0.25)),
}
for _k in (1, 2, 3):
    SMOOTH_Z[_k] = ((2 * _k - 1, 0.25), (2 * _k, 0.5), (2 * _k + 1, 0.25))


def smoothing():
    ring = np.eye(2 * X, dtype=np.float32)
    ring += 0.5 * (np.roll(ring, 1, axis=0) + np.roll(ring, -1, axis=0))
    return np.concatenate([ring[:X], ring[:X], ring[X:], ring[X:]]).astype(ml_dtypes.bfloat16)


def split(value, parts):
    out = []
    for _ in range(parts):
        out.append(value.astype(jnp.bfloat16))
        value = value - out[-1].astype(F32)
    return out


def dot(a, b):
    return lax.dot_general(a, b, (((1,), (0,)), ((), ())), preferred_element_type=F32)


def planes(ref, p):
    return ref[pl.ds(4 * p, 4)].reshape(32, X)


def loop(start, count, body, each=1):
    for z in range(start, start + count, each):
        body(list(range(z, min(z + each, start + count))))


def weigh(src, w):
    def body(zs):
        for z in zs:
            visc = planes(src, S0 + z)
            for c in range(3):
                w[c, z] = visc * planes(src, c * ZW + z)

    loop(0, ZW, body, 3)


def sum_rows(chains, t, lhs, z0, count):
    def body(zs):
        work = [(z, *chain) for z in zs for chain in chains]
        first = []
        for i, (z, c, w, col) in enumerate(work):
            v = w[z] + 0.5 * (w[z - 1] + w[z + 1])
            t[i, 8:40] = v
            first.append(v)
        for i, (z, c, w, col) in enumerate(work):
            v = first[i] + 0.5 * (t[i, 7:39] + t[i, 9:41])
            at = pl.ds((c * count + z - z0) * 32, 32)
            for part, value in enumerate(split(v, 2)):
                lhs[at, col + part * X : col + (part + 1) * X] = value

    loop(z0, count, body, 6 // len(chains))


def first_sums(main, ring, sums, w, t, lhs):
    t[...] = jnp.zeros_like(t)
    weigh(main, w)
    sum_rows([(c, w.at[c], 0) for c in range(3)], t, lhs, 1, Z + 2)
    sums[...] = dot(lhs[...], ring[: 2 * X])


def velocity_step(
    main, got_even, got_odd, table, ring, sums, coefs, vel, coupled, pscale, msg_even, msg_odd,
    halo, w, d, r, u, t, lhs, s, g, q, ptmp,
):
    lane = lanes()
    gap = jnp.zeros((X - 16, X), F32)
    even = parity("gx") == 0
    for i in range(PACKED):
        a, b = got_even[i], got_odd[i]
        strips = jnp.concatenate([jnp.where(even, a, b), gap, jnp.where(even, b, a)], axis=0)
        halo[16 * i : 16 * i + 16] = strips.T.reshape(16, 8, X)

    inv, a1, g1, a2, g2 = (tall(coefs[i], 32) for i in range(5))
    t[...] = jnp.zeros_like(t)
    both = (main, halo)

    weigh(halo, w.at[1])
    sum_rows([(c, w.at[1, c], 2 * X) for c in range(3)], t, lhs, 1, Z + 2)
    s[...] = dot(lhs[:, 2 * X :], ring[2 * X :])

    def sweep1(zs):
        (z,) = zs
        for h, src in enumerate(both):
            visc, mass = planes(src, S0 + z), planes(src, M0 + z - 1)
            cols = slice(h * X, (h + 1) * X)
            for c in range(3):
                at = pl.ds((c * (Z + 2) + z - 1) * 32, 32)
                b = planes(src, c * ZW + z)
                d0 = b * inv
                lap = 16.0 * (visc * d0) - (2.0 * inv) * (sums[at, cols] + s[at, cols])
                res = b - (visc * lap + mass * d0)
                d1 = a1 * d0 + g1 * res
                r[h, c, z] = res
                d[h, c, z] = d1
                w[h, c, z] = visc * d1

    loop(1, Z + 2, sweep1)

    for c in range(3):
        sum_rows([(c, w.at[h, c], 2 * h * X) for h in range(2)], t, lhs, 2, Z)
        at = slice(c * Z * 32, (c + 1) * Z * 32)
        s[at] = dot(lhs[at], ring[...])

    def sweep2(zs):
        (z,) = zs
        for h, src in enumerate(both):
            visc, mass = planes(src, S0 + z), planes(src, M0 + z - 1)
            for c in range(3):
                at = pl.ds((c * Z + z - 2) * 32, 32)
                d1 = d[h, c, z]
                lap = 16.0 * w[h, c, z] - 2.0 * s[at, h * X : (h + 1) * X]
                res = r[h, c, z] - (visc * lap + mass * d1)
                value = planes(src, c * ZW + z) * inv + d1 + (a2 * d1 + g2 * res)
                u[c, h, z - 2] = value
                if h == 0:
                    vel[c, z - 2] = value[8:24]

    loop(2, Z, sweep2)

    q[...] = jnp.zeros_like(q)
    for node in range(-1, 5):
        rows = slice(16 * (node + 1), 16 * (node + 1) + 12)

        def along_z(c, h, weights):
            acc = None
            for z, f in weights:
                term = f * u[c, h, z]
                acc = term if acc is None else acc + term
            return acc

        def at(k, start):
            return g[k, pl.ds(start, 12, stride=2), :]

        for h in range(2):
            cols = slice(X * h, X * (h + 1))
            g[2] = along_z(2, h, DERIVE_Z[node])
            total = 0.25 * (at(2, 3) + at(2, 5)) + 0.5 * at(2, 4)
            if SMOOTH_Z[node]:
                g[0] = along_z(0, h, SMOOTH_Z[node])
                g[1] = along_z(1, h, SMOOTH_Z[node])
                total = total + 0.25 * (at(1, 5) - at(1, 3)) + 0.125 * (at(1, 6) - at(1, 2))
                q[rows, 2 * X + X * h : 3 * X + X * h] = 0.25 * (at(0, 3) + at(0, 5)) + 0.5 * at(0, 4)
            q[rows, cols] = total

    div = sum(dot(v, table[...]) for v in reversed(split(q[...], 3)))

    def nodes(base, k):
        for i in range(3):
            own = pltpu.roll(main[base + 3 * k + i], 2, axis=1)
            side = halo[base + 3 * k + i]
            left = pltpu.roll(side, 2, axis=1)
            right = pltpu.roll(side, 66, axis=1)
            value = jnp.where(lane < 66, own, jnp.where(lane < 68, right, 0.0))
            ptmp[8 * i : 8 * i + 8] = jnp.where(lane < 2, left, value)
        return ptmp[6:18]

    coupled[...] = -div.reshape(6, 16, X)
    pscale[...] = jnp.zeros_like(pscale)
    for k in range(PZ):
        pscale[k, :12] = nodes(VT, k)
        coupled[k + 1, :12] = nodes(VT + 12, k) - div[16 * (k + 1) : 16 * (k + 1) + 12]
    par = parity("gz")
    for out, up in ((msg_even, 1 - par), (msg_odd, par)):
        parts = (
            coupled[2 + up] * pscale[1 + up], coupled[1 + 3 * up], coupled[5 * up], pscale[3 * up],
        )
        for j, part in enumerate(parts):
            out[12 * j : 12 * j + 12] = part[:12]


def pressure_step(coupled, pscale, got_even, got_odd, coefs, out, halo):
    even = parity("gz") == 0
    halo[...] = jnp.zeros_like(halo)
    for i in range(4):
        rows = slice(12 * i, 12 * i + 12)
        a, b = got_even[rows], got_odd[rows]
        halo[0, i, :12] = jnp.where(even, b, a)
        halo[1, i, :12] = jnp.where(even, a, b)
    b = [
        halo[0, 0], halo[0, 1] + coupled[0], halo[0, 2] + coupled[1], coupled[2],
        coupled[3], coupled[4] + halo[1, 2], coupled[5] + halo[1, 1], halo[1, 0],
    ]
    one = jnp.ones((16, X), F32)
    s = [one, halo[0, 3], pscale[0], pscale[1], pscale[2], pscale[3], halo[1, 3], one]
    inv, a1, g1, a2, g2 = (tall(coefs[5 + i], 16) for i in range(5))

    def operator(w, z):
        v = (1.0 / 6.0) * (w[z - 1] + w[z + 1]) + (2.0 / 3.0) * w[z]
        v = (1.0 / 6.0) * (pltpu.roll(v, 1, axis=0) + pltpu.roll(v, 15, axis=0)) + (2.0 / 3.0) * v
        v = (1.0 / 6.0) * (pltpu.roll(v, 1, axis=1) + pltpu.roll(v, X - 1, axis=1)) + (2.0 / 3.0) * v
        return s[z] * v

    d0 = [v * inv for v in b]
    w = [x * y for x, y in zip(s, d0)]
    r1, d1, w1 = [None] * 8, [None] * 8, [None] * 8
    for z in range(1, 7):
        r1[z] = b[z] - operator(w, z)
        d1[z] = a1 * d0[z] + g1 * r1[z]
        w1[z] = s[z] * d1[z]
    for z in range(2, 6):
        res = r1[z] - operator(w1, z)
        total = d0[z] + d1[z] + (a2 * d1[z] + g2 * res)
        total = pltpu.roll(pltpu.roll(total, 14, axis=0), X - 2, axis=1)
        out[z - 2] = total[:PY, :PX]


def per_device(rhs, prhs, visc, mass, pscale, vbounds, pbounds):
    plane, tile = (Y, X), (8, X)
    msg_even, msg_odd = call(
        pack_z,
        [(8, *plane)] * 2,
        scratch=[pltpu.VMEM((2, 4, *plane), F32), pltpu.SemaphoreType.DMA((10,))],
        hbm=(0, 1, 2),
    )(rhs, visc, mass)
    z_halos = swap_neighbours("gz", msg_even, msg_odd)
    (coefs,) = call(scalars, [(10, *tile)], smem=(0, 1))(vbounds, pbounds)
    (pt,) = call(pack_nodes, [(PZ, *tile)])(pscale, prhs)
    y_message = (Y_ROWS, X)
    two = [pltpu.VMEM(y_message, F32)] * 2
    own, msg_even, msg_odd = call(
        pack_y, [(PLANES, *plane), y_message, y_message], scratch=two
    )(rhs, visc, mass, *z_halos, pt)
    y_halos = swap_neighbours("gy", msg_even, msg_odd)
    main, msg_even, msg_odd = call(
        pack_x, [(TILES, *tile), (PACKED, *tile), (PACKED, *tile)], scratch=two
    )(own, pt, *y_halos)
    below, above = swap_neighbours("gx", msg_even, msg_odd)
    ring = jnp.asarray(smoothing())
    rows = 3 * (Z + 2) * 32
    (sums,) = call(
        first_sums,
        [(rows, 2 * X)],
        scratch=[
            pltpu.VMEM((3, ZW, 32, X), F32),
            pltpu.VMEM((6, 48, X), F32),
            pltpu.VMEM((rows, 2 * X), jnp.bfloat16),
        ],
    )(main, ring)
    vel, coupled, scale, msg_even, msg_odd = call(
        velocity_step,
        [(3, Z, Y, X), (6, *plane), (PZ, *plane), (48, X), (48, X)],
        vmem=(0,),
        scratch=[
            pltpu.VMEM((TILES, 8, X), F32),
            pltpu.VMEM((2, 3, ZW, 32, X), F32),
            pltpu.VMEM((2, 3, ZW, 32, X), F32),
            pltpu.VMEM((2, 3, ZW, 32, X), F32),
            pltpu.VMEM((3, 2, Z, 32, X), F32),
            pltpu.VMEM((6, 48, X), F32),
            pltpu.VMEM((rows, 4 * X), jnp.bfloat16),
            pltpu.VMEM((rows, 2 * X), F32),
            pltpu.VMEM((3, 32, X), F32),
            pltpu.VMEM((96, 4 * X), F32),
            pltpu.VMEM((24, X), F32),
        ],
    )(main, below, above, jnp.asarray(restriction()), ring, sums, coefs)
    z_halos = swap_neighbours("gz", msg_even, msg_odd)
    (pressure,) = call(
        pressure_step, [(PZ, PY, PX)], scratch=[pltpu.VMEM((2, 4, *plane), F32)]
    )(coupled, scale, *z_halos, coefs)
    return vel, pressure


def solution(mesh):
    block = P("gz", "gy", "gx")
    field = P(None, "gz", "gy", "gx")
    return jax.shard_map(
        per_device,
        mesh=mesh,
        in_specs=(field, block, block, block, block, P(), P()),
        out_specs=(field, block),
        check_vma=False,
    )
```
